32 devices in a mesh: rows: 16 (over z, x, core), cols: 2 (over y).
Axes of the slice: x: 2, y: 2, z: 4, core: 2. Of those that a mesh axis runs over, the one named last changes fastest.
Arguments:
- kets: float32 [16, 4, 32], P('rows', 'cols'), may hold values from -3 to 3
- left_maps: float32 [2, 16, 4, 96, 384], P(None, 'rows', 'cols'), may hold values from -0.3125 to 0.3125
- right_maps: float32 [2, 16, 4, 96, 384], P(None, 'rows', 'cols'), may hold values from -0.3125 to 0.3125
- top_edge: float32 [4, 96, 384], P('cols'), may hold values from -6 to 6
- bottom_edge: float32 [4, 96, 384], P('cols'), may hold values from -6 to 6
- left_edge: float32 [16, 96, 384], P('rows'), may hold values from -6 to 6
- right_edge: float32 [16, 96, 384], P('rows'), may hold values from -6 to 6
- term_rows: int32 [16], replicated, may hold values from 0 to 15
- term_bonds: int32 [16], replicated, may hold values from 0 to 2
- term_ops: int32 [16], replicated, may hold values from 0 to 3
- operators: float32 [4, 16], replicated, may hold values from -6 to 6
Outputs:
- top_out: float32 [16, 4, 96, 384], P('rows', 'cols')
- bottom_out: float32 [16, 4, 96, 384], P('rows', 'cols')
- energies: float32 [16], replicated
The draws below stay inside these ranges and needn't reach their ends.
Inputs may be any that keep to these rules, and one draw needn't show every extreme that they name: Term t acts on the bond between columns term_bonds[t] and term_bonds[t] + 1 of row term_rows[t].
All inputs are finite; a program needn't handle non-finite values.
Results may differ from the reference program's by a relative error of at most 0.0003.
Values sent between devices are 32-bit elements; how exact they have to be, the bound alone decides.
A program may use at most 64 MiB of HBM per device.

```python
import jax
import jax.numpy as jnp
from jax import lax

D = 2
D2 = 4
PHYS = 2
CHI = 96
OPS = 4
TERMS = 16
NR = 16
NC = 4


def set_ends(array, rng, least, top_value):
    index_at = [jax.random.randint(jax.random.fold_in(rng, axis), (), 0, length) for axis, length in enumerate(array.shape)]
    widest = array.shape.index(max(array.shape))
    beside = index_at[:widest] + [(index_at[widest] + 1) % array.shape[widest]] + index_at[widest + 1:]
    return array.at[tuple(index_at)].set(least).at[tuple(beside)].set(top_value)


def levels(stream_key, shape, pieces, least, largest):
    factor_of = 1.0
    for axis_at, parts in pieces:
        draws = jax.random.uniform(jax.random.fold_in(jax.random.fold_in(stream_key, 6), axis_at), (parts,), jnp.float32, least / len(pieces), largest / len(pieces))
        factor_of = factor_of * jnp.repeat(jnp.exp(draws), shape[axis_at] // parts).reshape((-1,) + (1,) * (len(shape) - 1 - axis_at))
    return factor_of


def gaussian(key, dims, scale, most, shards=(), kind=jnp.bfloat16):
    entries = jax.random.normal(key, dims, jnp.float32) * scale
    if len(shards) > 0:
        entries = levels(key, dims, shards, -0.22, 0.18) * entries
    return jnp.clip(entries, min=-most, max=most).astype(kind)


def setup_inputs(seed: int = 0) -> dict:
    key_list = jax.random.split(jax.random.key(seed), 12)
    kets = gaussian(key_list[0], (NR, NC, PHYS * D**4), 0.5, 3.0, ((0, 16), (1, 2)), jnp.float32)
    left_maps = gaussian(key_list[1], (2, NR, NC, CHI, CHI * D2), (CHI * D2) ** -0.5, 0.3125, ((1, 16), (2, 2)), jnp.float32)
    right_maps = gaussian(key_list[2], (2, NR, NC, CHI, CHI * D2), (CHI * D2) ** -0.5, 0.3125, ((1, 16), (2, 2)), jnp.float32)
    top_edge = gaussian(key_list[3], (NC, CHI, D2 * CHI), 1.0, 6.0, ((0, 2),), jnp.float32)
    bottom_edge = gaussian(key_list[4], (NC, CHI, D2 * CHI), 1.0, 6.0, ((0, 2),), jnp.float32)
    left_edge = gaussian(key_list[5], (NR, CHI, D2 * CHI), 1.0, 6.0, ((0, 16),), jnp.float32)
    right_edge = gaussian(key_list[6], (NR, CHI, D2 * CHI), 1.0, 6.0, ((0, 16),), jnp.float32)
    term_rows = set_ends(jax.random.randint(key_list[7], (TERMS,), 0, NR), jax.random.fold_in(key_list[7], 1), 0, NR - 1).astype(jnp.int32)
    term_bonds = set_ends(jax.random.randint(key_list[8], (TERMS,), 0, NC - 1), jax.random.fold_in(key_list[8], 1), 0, (NC - 1) - 1).astype(jnp.int32)
    term_ops = set_ends(jax.random.randint(key_list[9], (TERMS,), 0, OPS), jax.random.fold_in(key_list[9], 1), 0, OPS - 1).astype(jnp.int32)
    operators = gaussian(key_list[10], (OPS, PHYS**4), 1.0, 6.0, (), jnp.float32)
    return dict(kets=kets, left_maps=left_maps, right_maps=right_maps, top_edge=top_edge, bottom_edge=bottom_edge, left_edge=left_edge, right_edge=right_edge, term_rows=term_rows, term_bonds=term_bonds, term_ops=term_ops, operators=operators)


EPSILON = 1e-06
PRECISION_HIGH = lax.Precision.HIGHEST

def product(pattern, former, latter):
    return jnp.einsum(pattern, former, latter, precision=PRECISION_HIGH, preferred_element_type=jnp.float32)

def normalize(values):
    return values / jnp.sqrt(jnp.mean(values * values) + EPSILON)

def select_at(values, position):
    return lax.dynamic_index_in_dim(values, position, 0, keepdims=False)

def pair_layers(ket_flat):
    tensor = ket_flat.reshape(PHYS, D, D, D, D)
    doubled = product('pabcd,pefgh->aebfcgdh', tensor, tensor)
    return doubled.reshape(D2, D2, D2, D2)

def open_layers(ket_flat):
    tensor = ket_flat.reshape(PHYS, D, D, D, D)
    doubled = product('pabcd,qefgh->pqaebfcgdh', tensor, tensor)
    return doubled.reshape(PHYS * PHYS, D2, D2, D2, D2)

def pair_diagonal():
    matched = jnp.arange(PHYS)[:, None] == jnp.arange(PHYS)[None, :]
    return jnp.where(matched, 1.0, 0.0).astype(jnp.float32).reshape(PHYS * PHYS)

def absorb_down(boundary, layers, left_map, right_map):
    above_col = boundary.reshape(CHI, D2, CHI)
    left_three = left_map.reshape(CHI, CHI, D2)
    right_three = right_map.reshape(CHI, CHI, D2)
    joined = product('aub,cbr->aurc', above_col, right_three)
    through = product('aurc,uldr->aldc', joined, layers)
    renewed = product('xal,aldc->xdc', left_three, through)
    return normalize(renewed.reshape(CHI, D2 * CHI))

def absorb_up(boundary, layers, left_map, right_map):
    below_col = boundary.reshape(CHI, D2, CHI)
    left_three = left_map.reshape(CHI, CHI, D2)
    right_three = right_map.reshape(CHI, CHI, D2)
    joined = product('adb,cbr->adrc', below_col, right_three)
    through = product('adrc,uldr->aluc', joined, layers)
    renewed = product('xal,aluc->xuc', left_three, through)
    return normalize(renewed.reshape(CHI, D2 * CHI))

def left_core(environ, layers, above_col, below_col):
    env_three = environ.reshape(CHI, D2, CHI)
    upper_three = above_col.reshape(CHI, D2, CHI)
    lower_three = below_col.reshape(CHI, D2, CHI)
    step_one = product('alb,aux->lbux', env_three, upper_three)
    step_two = product('lbux,uldr->bxdr', step_one, layers)
    return product('bxdr,bdy->xry', step_two, lower_three).reshape(CHI, D2 * CHI)

def right_core(environ, layers, above_col, below_col):
    env_three = environ.reshape(CHI, D2, CHI)
    upper_three = above_col.reshape(CHI, D2, CHI)
    lower_three = below_col.reshape(CHI, D2, CHI)
    step_one = product('xry,aux->ryau', env_three, upper_three)
    step_two = product('ryau,uldr->yald', step_one, layers)
    return product('yald,bdy->alb', step_two, lower_three).reshape(CHI, D2 * CHI)

def reference(kets, left_maps, right_maps, top_edge, bottom_edge, left_edge, right_edge, term_rows, term_bonds, term_ops, operators):
    layers = jax.vmap(jax.vmap(pair_layers))(kets)

    def down_row(carried, inputs):
        renewed = jax.vmap(absorb_down)(carried, inputs[0], inputs[1], inputs[2])
        return (renewed, renewed)

    def up_row(carried, inputs):
        renewed = jax.vmap(absorb_up)(carried, inputs[0], inputs[1], inputs[2])
        return (renewed, renewed)
    unused_top, top_out = lax.scan(down_row, top_edge, (layers, left_maps[0], right_maps[0]))
    unused_bottom, bottom_out = lax.scan(up_row, bottom_edge, (layers, left_maps[1], right_maps[1]), reverse=True)
    above = jnp.concatenate([top_edge[None], top_out[:-1]], axis=0)
    below = jnp.concatenate([bottom_out[1:], bottom_edge[None]], axis=0)
    diagonal = pair_diagonal()
    weights = jnp.outer(diagonal, diagonal).reshape(-1)

    def one_term(term_index):
        term_row = select_at(term_rows, term_index).astype(jnp.int32)
        term_bond = select_at(term_bonds, term_index).astype(jnp.int32)
        row_layers = select_at(layers, term_row)
        row_kets = select_at(kets, term_row)
        row_above = select_at(above, term_row)
        row_below = select_at(below, term_row)

        def left_walk(column, environ):
            return normalize(left_core(environ, select_at(row_layers, column), select_at(row_above, column), select_at(row_below, column)))

        def right_walk(step_count, environ):
            column = (NC - 1 - step_count).astype(jnp.int32)
            return normalize(right_core(environ, select_at(row_layers, column), select_at(row_above, column), select_at(row_below, column)))
        left_env = lax.fori_loop(0, term_bond, left_walk, select_at(left_edge, term_row))
        right_env = lax.fori_loop(0, NC - 2 - term_bond, right_walk, select_at(right_edge, term_row))
        right_col = (term_bond + 1).astype(jnp.int32)
        open_left = lax.map(lambda single: left_core(left_env, single, select_at(row_above, term_bond), select_at(row_below, term_bond)), open_layers(select_at(row_kets, term_bond)))
        open_right = lax.map(lambda single: right_core(right_env, single, select_at(row_above, right_col), select_at(row_below, right_col)), open_layers(select_at(row_kets, right_col)))
        density = product('pz,qz->pq', open_left.reshape(PHYS * PHYS, -1), open_right.reshape(PHYS * PHYS, -1)).reshape(-1)
        trace_value = jnp.sum(density * weights)
        spread = jnp.sqrt(jnp.sum(density * density))
        denominator = jnp.maximum(jnp.abs(trace_value), 0.25 * spread)
        chosen_op = select_at(operators, select_at(term_ops, term_index).astype(jnp.int32))
        return jnp.sum(density * chosen_op) / denominator
    energies = lax.map(one_term, jnp.arange(TERMS, dtype=jnp.int32))
    return (top_out, bottom_out, energies)
```

```python
import functools

import jax
import jax.numpy as jnp
from jax import lax
from jax.experimental import pallas as pl
from jax.experimental.pallas import tpu as pltpu
from jax.sharding import PartitionSpec as P

D = 2
D2 = 4
PHYS = 2
EPSILON = 1e-06
LANES = 128


def unpack_lanes(tiles, chi):
    rolled = {}
    lane = lax.broadcasted_iota(jnp.int32, tiles[0].shape, 1)
    blocks = []
    for block in range(D2):
        total = jnp.zeros_like(tiles[0])
        for place, tile in enumerate(tiles):
            low = max(chi * block, LANES * place)
            high = min(chi * (block + 1), LANES * (place + 1))
            if low >= high:
                continue
            shift = (LANES * place - chi * block) % LANES
            if (place, shift) not in rolled:
                rolled[place, shift] = tile if shift == 0 else pltpu.roll(tile, shift, 1)
            inside = (lane >= low - chi * block) & (lane < high - chi * block)
            total = jnp.where(inside, rolled[place, shift], total)
        blocks.append(total)
    return blocks


def pack_lanes(blocks, chi):
    lane = lax.broadcasted_iota(jnp.int32, blocks[0].shape, 1)
    rolled = {}
    tiles = []
    for place in range(chi * D2 // LANES):
        total = jnp.zeros_like(blocks[0])
        for block, values in enumerate(blocks):
            low = max(chi * block, LANES * place)
            high = min(chi * (block + 1), LANES * (place + 1))
            if low >= high:
                continue
            shift = (chi * block - LANES * place) % LANES
            if (block, shift) not in rolled:
                rolled[block, shift] = values if shift == 0 else pltpu.roll(values, shift, 1)
            inside = (lane >= low - LANES * place) & (lane < high - LANES * place)
            total = jnp.where(inside, rolled[block, shift], total)
        tiles.append(total)
    return tiles


def halves(values):
    high = values.astype(jnp.bfloat16)
    low = (values - high.astype(jnp.float32)).astype(jnp.bfloat16)
    return high, low


def dot32(former, latter):
    return jnp.dot(former, latter, preferred_element_type=jnp.float32)


def dot_last(former, latter):
    return lax.dot_general(
        former, latter, (((1,), (1,)), ((), ())), preferred_element_type=jnp.float32
    )


def load_tiles(ref, at, width):
    return [ref[at, :, LANES * t : LANES * (t + 1)] for t in range(width // LANES)]


def window_kernel(
    row_count,
    col_count,
    kets_ref,
    left_maps_ref,
    right_maps_ref,
    top_ref,
    bottom_ref,
    left_ref,
    right_ref,
    rows_ref,
    bonds_ref,
    ops_ref,
    table_ref,
    out_ref,
    energy_ref,
    kets,
    kets_env,
    maps,
    edges,
    sides,
    env_ref,
    pbuf,
    qbuf,
    kbuf,
    xbuf,
    ebuf,
    pick,
    pboth,
    qhi,
    qlo,
    x32,
    jbuf,
    thi,
    tlo,
    near,
    far,
    vbuf,
    opens,
    hop_out,
    hop_in,
    half_out,
    half_in,
    shares,
    row_share,
    token,
    load_sem,
    map_send,
    map_recv,
    env_send,
    env_recv,
    out_send,
    out_recv,
    chain_send,
    chain_recv,
    hop_send,
    hop_recv,
    half_send,
    half_recv,
    share_send,
    share_recv,
):
    local_cols = kets.shape[1]
    chi, width = maps.shape[3], maps.shape[4]
    half = chi // 2
    wide = D2 * LANES
    pairs = PHYS * PHYS
    terms = rows_ref.shape[1]
    tall = shares.shape[1:]
    group = 2 * local_cols
    groups = row_count // group
    place = lax.axis_index("rows")
    cols_at = lax.axis_index("cols")
    has_left = cols_at > 0
    has_right = cols_at < col_count - 1
    mine = place // group
    me = place % group
    column = me // 2
    way = me % 2
    base = mine * group
    before = mine - 1 + 2 * way
    after = mine + 1 - 2 * way
    has_before = (before >= 0) & (before < groups)
    has_after = (after >= 0) & (after < groups)

    barrier = pltpu.get_barrier_semaphore()
    for other in range(group):

        @pl.when(me != other)
        def _():
            pl.semaphore_signal(barrier, inc=1, device_id={"rows": base + other})

    has_lower = mine > 0
    has_upper = mine < groups - 1

    @pl.when(has_lower)
    def _():
        pl.semaphore_signal(barrier, inc=1, device_id={"rows": place - group})

    @pl.when(has_upper)
    def _():
        pl.semaphore_signal(barrier, inc=1, device_id={"rows": place + group})

    for other in range(col_count):

        @pl.when(cols_at != other)
        def _():
            pl.semaphore_signal(barrier, inc=1, device_id={"cols": other})

    loads = [
        pltpu.make_async_copy(source, target, load_sem.at[at])
        for at, (source, target) in enumerate(
            (
                (right_maps_ref.at[:, 0], maps.at[0]),
                (left_maps_ref.at[:, 0], maps.at[1]),
                (top_ref, edges.at[0]),
                (bottom_ref, edges.at[1]),
                (left_ref, sides.at[pl.ds(0, 1)]),
                (right_ref, sides.at[pl.ds(1, 1)]),
            )
        )
    ]
    for load in loads:
        load.start()

    count = kets_ref.shape[2]
    spot = lax.broadcasted_iota(jnp.int32, (count, count), 0)
    from_lane = lax.broadcasted_iota(jnp.int32, (count, count), 1)

    def exchanged(high, low):
        top, bottom = (spot // high) % 2, (spot // low) % 2
        return spot + (bottom - top) * high + (top - bottom) * low

    for order, target in ((spot, 0), (exchanged(8, 2), 1), (exchanged(4, 1), 2)):
        for at in range(local_cols):
            values = jnp.broadcast_to(kets_ref[0, at : at + 1, :], (count, count))
            tallest = jnp.sum(
                jnp.where(order == from_lane, values, 0.0), axis=1, keepdims=True
            )
            filled = jnp.broadcast_to(tallest, (count, LANES))
            if target < 2:
                kets[target, at] = filled
            if target != 1:
                kets_env[target // 2, at] = filled

    chosen = lax.broadcasted_iota(jnp.int32, (wide, width), 0)
    entry = lax.broadcasted_iota(jnp.int32, (wide, width), 1)
    wanted = (chosen % LANES) * D2 + chosen // LANES
    live = (chosen % LANES) < chi
    pick[...] = jnp.where((wanted == entry) & live, 1.0, 0.0).astype(jnp.bfloat16)
    thi[...] = jnp.zeros_like(thi)
    tlo[...] = jnp.zeros_like(tlo)
    for load in loads:
        load.wait()
    greeted = jnp.where(has_lower, 1, 0) + jnp.where(has_upper, 1, 0)
    pl.semaphore_wait(barrier, group - 1 + col_count - 1 + greeted)

    def pass_token(way_at):
        pl.semaphore_signal(
            token.at[way_at], inc=1, device_id={"rows": place + (group, -group)[way_at]}
        )

    @pl.when(has_upper & jnp.logical_not(has_lower))
    def _():
        pass_token(0)

    @pl.when(has_lower & jnp.logical_not(has_upper))
    def _():
        pass_token(1)

    def map_copies(target_way, target_col, target, local):
        made = []
        for kind, (source, buffer) in enumerate(
            ((kets, kbuf), (maps.at[0], qbuf), (maps.at[1], pbuf))
        ):
            origin, landing = source.at[target_way, target_col], buffer.at[me]
            if local:
                made.append(pltpu.make_async_copy(origin, landing, map_recv.at[kind, me]))
            else:
                made.append(
                    pltpu.make_async_remote_copy(
                        origin,
                        landing,
                        map_send.at[kind, target],
                        map_recv.at[kind, me],
                        device_id={"rows": base + target},
                    )
                )
        return made

    low_half = jnp.where(mine >= groups // 2, 1, 0)
    for turn in range(group):
        target_way = (low_half + turn // local_cols) % 2
        target_col = turn % local_cols
        target = target_col * 2 + target_way

        @pl.when(target != me)
        def _():
            for copy in map_copies(target_way, target_col, target, False):
                copy.start()

        @pl.when(target == me)
        def _():
            for copy in map_copies(target_way, target_col, target, True):
                copy.start()

    def prepare(step, unused):
        slot = step + way * (group - 1 - 2 * step)
        for kind, buffer in enumerate((kbuf, qbuf, pbuf)):
            pltpu.make_async_copy(
                buffer.at[slot], buffer.at[slot], map_recv.at[kind, slot]
            ).wait()
        ket = kbuf[slot]
        half = ket.shape[0] // PHYS
        for i in range(half):
            total = ket[i : i + 1] * ket[0:half]
            for p in range(1, PHYS):
                total += ket[p * half + i : p * half + i + 1] * ket[p * half : (p + 1) * half]
            ebuf[step, i * half : (i + 1) * half] = total
        values = pick[...]
        for source, high_ref, low_ref, right in (
            (qbuf, qhi, qlo, True),
            (pbuf, pboth, pboth, False),
        ):
            for at, (part, ref) in enumerate(zip(halves(source[slot]), (high_ref, low_ref))):
                if right:
                    fill = jnp.zeros((LANES - chi, width), jnp.bfloat16)
                    tall = dot_last(values, jnp.concatenate([part, fill], axis=0))
                    for w in range(D2):
                        ref[step, :, w * LANES : (w + 1) * LANES] = tall[
                            w * LANES : (w + 1) * LANES
                        ].astype(jnp.bfloat16)
                else:
                    spread_map = dot_last(part, values).astype(jnp.bfloat16)
                    ref[step, at * chi : (at + 1) * chi] = spread_map
        return unused

    def row_copy(source, landing, send, recv, slot):
        remote = pltpu.make_async_remote_copy(
            source, landing, send, recv, device_id={"rows": base + slot}
        )
        return remote, pltpu.make_async_copy(source, landing, recv)

    def send_row(source, landing, send, recv, slot):
        remote, local = row_copy(source, landing, send, recv, slot)

        @pl.when(slot != me)
        def _():
            remote.start()

        @pl.when(slot == me)
        def _():
            local.start()

    chain_hop = pltpu.make_async_remote_copy(
        xbuf.at[group],
        xbuf.at[0],
        chain_send,
        chain_recv,
        device_id={"rows": after * group + me},
    )

    start_slot = way * (group - 1)
    crossing = jnp.logical_not(has_before) & ((start_slot // local_cols) != (me // local_cols))
    ahead = jnp.where(has_before, group, jnp.where(crossing, group - local_cols + 1, 1))
    turned_by = jnp.where(crossing, local_cols, 0)

    def prepare_ahead(turn, unused):
        return prepare((turn + turned_by) % group, unused)

    lax.fori_loop(0, ahead, prepare_ahead, 0)

    @pl.when(has_lower & has_upper)
    def _():
        for way_at in range(2):
            pl.semaphore_wait(token.at[way_at], 1)
            pass_token(way_at)

    @pl.when(has_before)
    def _():
        pltpu.make_async_copy(xbuf.at[0], xbuf.at[0], chain_recv).wait()

    @pl.when(jnp.logical_not(has_before) & (way == 0))
    def _():
        xbuf[0] = edges[0, column]

    @pl.when(jnp.logical_not(has_before) & (way == 1))
    def _():
        xbuf[0] = edges[1, column]

    for u, block in enumerate(unpack_lanes(load_tiles(xbuf, 0, width), chi)):
        x32[u * chi : (u + 1) * chi] = block

    def absorb(step, unused):
        slot = step + way * (group - 1 - 2 * step)

        pending = (step >= 1) & jnp.logical_not(crossing & (step >= local_cols))

        @pl.when(pending & jnp.logical_not(has_before))
        def _():
            prepare(step, 0)

        send_row(
            xbuf.at[step], env_ref.at[way, column], env_send.at[step], env_recv.at[way, column], slot
        )
        x_high, x_low = halves(x32[...])
        q_high = qhi[step]
        jbuf[...] = dot32(x_high, q_high) + (dot32(x_high, qlo[step]) + dot32(x_low, q_high))
        chunk = 16

        def through(at, unused):
            start = pl.multiple_of(at * chunk, chunk)
            for l in range(D2):
                for d in range(D2):
                    total = None
                    for u in range(D2):
                        for w in range(D2):
                            ket_at = (u // D) * 8 + (l // D) * 4 + (d // D) * 2 + w // D
                            bra_at = (u % D) * 8 + (l % D) * 4 + (d % D) * 2 + w % D
                            spot = ket_at * 16 + bra_at
                            term = (
                                ebuf[step, spot : spot + 1, :]
                                * jbuf[
                                    pl.ds(u * chi + start, chunk), w * LANES : (w + 1) * LANES
                                ]
                            )
                            total = term if total is None else total + term
                    high, low = halves(total)
                    rows = pl.ds(l * LANES + start, chunk)
                    thi[rows, d * LANES : (d + 1) * LANES] = high
                    tlo[rows, d * LANES : (d + 1) * LANES] = low
            return unused

        lax.fori_loop(0, chi // chunk, through, 0, unroll=True)
        both = pboth[step]
        large = dot32(both, thi[:, 0:wide])
        renewed = large[:chi] + (large[chi:] + dot32(both[:chi], tlo[:, 0:wide]))
        square = jnp.sum(jnp.sum(renewed * renewed, axis=1, keepdims=True), axis=0, keepdims=True)
        renewed = renewed * (1.0 / jnp.sqrt(square / (chi * width) + EPSILON))
        blocks = [renewed[:, d * LANES : (d + 1) * LANES] for d in range(D2)]
        for d, block in enumerate(blocks):
            x32[d * chi : (d + 1) * chi] = block
        for t, tile in enumerate(pack_lanes(blocks, chi)):
            xbuf[step + 1, :, t * LANES : (t + 1) * LANES] = tile

        @pl.when((step == group - 1) & has_after)
        def _():
            chain_hop.start()

        send_row(
            xbuf.at[step + 1],
            out_ref.at[way, column],
            out_send.at[step],
            out_recv.at[way, column],
            slot,
        )
        return unused

    lax.fori_loop(0, group, absorb, 0)

    unit = jnp.where(
        lax.broadcasted_iota(jnp.int32, (LANES, LANES), 0)
        == lax.broadcasted_iota(jnp.int32, (LANES, LANES), 1),
        1.0,
        0.0,
    ).astype(jnp.bfloat16)
    fill = jnp.zeros((LANES - chi, LANES), jnp.bfloat16)

    def take_boundary(kind):
        for column in range(local_cols):
            landed = env_ref.at[kind, column]
            pltpu.make_async_copy(landed, landed, env_recv.at[kind, column]).wait()
            blocks = unpack_lanes(load_tiles(env_ref.at[kind], column, width), chi)
            for at, block in enumerate(blocks):
                lanes = slice(at * LANES, (at + 1) * LANES)
                for part, values in enumerate(halves(block)):
                    tall_block = jnp.concatenate([values, fill], axis=0)
                    turned = dot_last(unit, tall_block).astype(jnp.bfloat16)
                    if kind == 0:
                        rows = slice(part * chi, (part + 1) * chi)
                        near[0, column, rows, lanes] = turned[:chi]
                        near[1, column, rows, lanes] = values
                    else:
                        far[1, column, part, :, lanes] = turned
                        far[0, column, part, :, lanes] = tall_block

    for turn in range(2):
        for kind in range(2):

            @pl.when((turn + low_half) % 2 == kind)
            def _():
                take_boundary(kind)

    spot_row = lax.broadcasted_iota(jnp.int32, (terms, terms), 0)
    spot_lane = lax.broadcasted_iota(jnp.int32, (terms, terms), 1)

    def stand(ref):
        values = jnp.broadcast_to(ref[...].astype(jnp.float32), (terms, terms))
        return jnp.sum(jnp.where(spot_row == spot_lane, values, 0.0), axis=1, keepdims=True)

    term_row = stand(rows_ref).astype(jnp.int32)
    term_bond = stand(bonds_ref).astype(jnp.int32)
    term_op = stand(ops_ref).astype(jnp.int32)
    term_weights = jnp.zeros((terms, table_ref.shape[1]), jnp.float32)
    for op in range(table_ref.shape[0]):
        term_weights = jnp.where(term_op == op, table_ref[op : op + 1, :], term_weights)

    late = jnp.where(cols_at >= col_count // 2, 1, 0)

    def hop(side, step):
        return pltpu.make_async_remote_copy(
            hop_out.at[side],
            hop_in.at[side],
            hop_send.at[side],
            hop_recv.at[side],
            device_id={"cols": cols_at + step},
        )

    def half_copy(side):
        step = (1, -1)[side]
        return pltpu.make_async_remote_copy(
            half_out.at[side],
            half_in.at[side],
            half_send.at[side],
            half_recv.at[side],
            device_id={"cols": cols_at + step},
        )

    def put_environ(blocks):
        for at, block in enumerate(blocks):
            vbuf[at * chi : (at + 1) * chi] = block

    def walk(turn, unused):
        side = (turn // local_cols + late) % 2
        order = turn % local_cols
        column = order + side * (local_cols - 1 - 2 * order)
        first = ((side == 0) & (cols_at == 0)) | ((side == 1) & (cols_at == col_count - 1))
        final = ((side == 1) & (cols_at == 0)) | ((side == 0) & (cols_at == col_count - 1))
        ending = order == local_cols - 1

        @pl.when((order == 0) & jnp.logical_not(first))
        def _():
            pltpu.make_async_copy(hop_in.at[side], hop_in.at[side], hop_recv.at[side]).wait()
            put_environ(unpack_lanes(load_tiles(hop_in, side, width), chi))

        for at in range(2):

            @pl.when((order == 0) & first & (side == at))
            def _():
                put_environ(unpack_lanes(load_tiles(sides, at, width), chi))

        @pl.when(jnp.logical_not(ending & final))
        def _():
            v_high, v_low = halves(vbuf[...])
            f_high = far[side, column, 0]
            jbuf[...] = dot32(v_high, f_high) + (
                dot32(v_high, far[side, column, 1]) + dot32(v_low, f_high)
            )
            chunk = 16

            def ket(p, u, i, d, o):
                at = p * 16 + u * 8 + i * 4 + d * 2 + o
                return kets_env[side, column, at : at + 1, :]

            def through(at, unused):
                start = pl.multiple_of(at * chunk, chunk)

                def joined(i, d):
                    return jbuf[pl.ds(i * chi + start, chunk), d * LANES : (d + 1) * LANES]

                for p in range(PHYS):
                    for u in range(D):
                        for o in range(D):
                            part = {}
                            for i2 in range(D):
                                for d2 in range(D):
                                    total = None
                                    for i in range(D):
                                        for d in range(D):
                                            term = ket(p, u, i, d, o) * joined(
                                                i * D + i2, d * D + d2
                                            )
                                            total = term if total is None else total + term
                                    part[i2, d2] = total
                            for q in range(PHYS):
                                for u2 in range(D):
                                    for o2 in range(D):
                                        total = None
                                        for i2 in range(D):
                                            for d2 in range(D):
                                                term = ket(q, u2, i2, d2, o2) * part[i2, d2]
                                                total = term if total is None else total + term
                                        high, low = halves(total)
                                        rows = pl.ds((u * D + u2) * LANES + start, chunk)
                                        spot = (p * PHYS + q) * D2 + o * D + o2
                                        lanes = slice(spot * LANES, (spot + 1) * LANES)
                                        thi[rows, lanes] = high
                                        tlo[rows, lanes] = low
                return unused

            lax.fori_loop(0, chi // chunk, through, 0)
            both = near[side, column]
            wide = D2 * LANES
            closed = None
            for pair in range(pairs):
                lanes = slice(pair * wide, (pair + 1) * wide)
                large = dot32(both, thi[:, lanes])
                value = large[:chi] + (large[chi:] + dot32(both[:chi], tlo[:, lanes]))
                opens[side, column, pair] = value
                if pair // PHYS == pair % PHYS:
                    closed = value if closed is None else closed + value
            square = jnp.sum(
                jnp.sum(closed * closed, axis=1, keepdims=True), axis=0, keepdims=True
            )
            closed = closed * (1.0 / jnp.sqrt(square / (chi * width) + EPSILON))
            blocks = [closed[:, d * LANES : (d + 1) * LANES] for d in range(D2)]
            put_environ(blocks)

            @pl.when(ending)
            def _():
                for t, tile in enumerate(pack_lanes(blocks, chi)):
                    hop_out[side, :, t * LANES : (t + 1) * LANES] = tile

            for at, step in enumerate((1, -1)):

                @pl.when(ending & (side == at))
                def _():
                    hop(at, step).start()
                    rows = slice((1 - at) * half, (2 - at) * half)
                    for pair in range(pairs):
                        lanes = [
                            opens[side, column, pair, rows, d * LANES : (d + 1) * LANES]
                            for d in range(D2)
                        ]
                        for t, tile in enumerate(pack_lanes(lanes, chi)):
                            half_out[at, pair, :, t * LANES : (t + 1) * LANES] = tile
                    half_copy(at).start()

        return unused

    lax.fori_loop(0, 2 * local_cols, walk, 0)

    lane = lax.broadcasted_iota(jnp.int32, tall, 1)

    def density(former, latter):
        total = jnp.zeros(tall, jnp.float32)
        for p in range(pairs):
            first = former(p)
            for q in range(pairs):
                value = jnp.sum(
                    jnp.sum(first * latter(q), axis=0, keepdims=True), axis=1, keepdims=True
                )
                total = jnp.where(lane == p * pairs + q, value, total)
        return total

    def share(bond, values):
        hit = (term_row == place) & (term_bond == bond)
        return jnp.where(hit, values, 0.0)

    held = shares.at[cols_at]
    held[...] = jnp.zeros(tall, jnp.float32)
    for column in range(local_cols - 1):
        held[...] += share(
            cols_at * local_cols + column,
            density(lambda p: opens[0, column, p], lambda q: opens[1, column + 1, q]),
        )

    def arrived(side):
        known = {}

        def take(pair):
            if pair not in known:
                known[pair] = jnp.concatenate(
                    unpack_lanes(load_tiles(half_in.at[side], pair, width), chi), axis=1
                )
            return known[pair]

        return take

    def land(side):
        pltpu.make_async_copy(half_in.at[side], half_in.at[side], half_recv.at[side]).wait()

    @pl.when(has_right)
    def _():
        land(1)
        held[...] += share(
            cols_at * local_cols + local_cols - 1,
            density(lambda p: opens[0, local_cols - 1, p, :half], arrived(1)),
        )

    @pl.when(has_left)
    def _():
        land(0)
        held[...] += share(
            cols_at * local_cols - 1,
            density(arrived(0), lambda q: opens[1, 0, q, half:]),
        )

    def spread(buffer, stage, axis, at, count):
        def copies(other):
            return pltpu.make_async_remote_copy(
                buffer.at[at],
                buffer.at[at],
                share_send.at[stage, other],
                share_recv.at[stage, at],
                device_id={axis: other},
            )

        for other in range(count):

            @pl.when(at != other)
            def _():
                copies(other).start()

        for other in range(count):

            @pl.when(at != other)
            def _():
                pltpu.make_async_copy(
                    buffer.at[other], buffer.at[other], share_recv.at[stage, other]
                ).wait()

        total = buffer[0]
        for other in range(1, count):
            total += buffer[other]

        def finish():
            for other in range(count):

                @pl.when(at != other)
                def _():
                    copies(other).wait_send()

        return total, finish

    total, finish_cols = spread(shares, 0, "cols", cols_at, col_count)
    picked = jnp.sum(total[:, : pairs * pairs] * term_weights, axis=1, keepdims=True)
    bra, ket_at = lane % pairs, lane // pairs
    diagonal = (bra // PHYS == bra % PHYS) & (ket_at // PHYS == ket_at % PHYS)
    trace = jnp.sum(
        jnp.where(diagonal & (lane < pairs * pairs), total, 0.0), axis=1, keepdims=True
    )
    size = jnp.sqrt(jnp.sum(total * total, axis=1, keepdims=True))
    energy = picked / jnp.maximum(jnp.abs(trace), 0.25 * size)
    same = lax.broadcasted_iota(jnp.int32, tall, 0) == lane
    row_share[place] = jnp.sum(
        jnp.where(same & (term_row == place), energy, 0.0), axis=0, keepdims=True
    )

    @pl.when(has_lower & jnp.logical_not(has_upper))
    def _():
        pl.semaphore_wait(token.at[0], 1)

    @pl.when(has_upper & jnp.logical_not(has_lower))
    def _():
        pl.semaphore_wait(token.at[1], 1)

    total, finish_rows = spread(row_share, 1, "rows", place, row_count)
    energy_ref[...] = total[:, :terms]
    finish_cols()
    finish_rows()

    @pl.when(has_right)
    def _():
        hop(0, 1).wait_send()
        half_copy(0).wait_send()

    @pl.when(has_left)
    def _():
        hop(1, -1).wait_send()
        half_copy(1).wait_send()

    for step in range(group):
        slot = step + way * (group - 1 - 2 * step)

        @pl.when(slot != me)
        def _():
            row_copy(
                xbuf.at[step],
                env_ref.at[way, column],
                env_send.at[step],
                env_recv.at[way, column],
                slot,
            )[0].wait_send()
            row_copy(
                xbuf.at[step + 1],
                out_ref.at[way, column],
                out_send.at[step],
                out_recv.at[way, column],
                slot,
            )[0].wait_send()

    for target in range(group):

        @pl.when(target != me)
        def _():
            for copy in map_copies(target % 2, target // 2, target, False):
                copy.wait_send()

    @pl.when(has_after)
    def _():
        chain_hop.wait_send()

    for a in range(2):
        for b in range(local_cols):
            pltpu.make_async_copy(out_ref.at[a, b], out_ref.at[a, b], out_recv.at[a, b]).wait()


def window(row_count, col_count, args):
    local_cols = args[0].shape[1]
    chi, width = args[1].shape[-2:]
    terms = args[7].shape[0]
    group = 2 * local_cols
    wide = D2 * LANES
    pairs = PHYS * PHYS
    most = max(row_count, col_count)
    entries = args[0].shape[2]
    vmem = pl.BlockSpec(memory_space=pltpu.VMEM)
    stay = pl.BlockSpec(memory_space=pltpu.HBM)
    dma = pltpu.SemaphoreType.DMA

    def f32(*shape):
        return pltpu.VMEM(shape, jnp.float32)

    def bf16(*shape):
        return pltpu.VMEM(shape, jnp.bfloat16)

    return pl.pallas_call(
        functools.partial(window_kernel, row_count, col_count),
        out_shape=(
            jax.ShapeDtypeStruct((2, local_cols, chi, width), jnp.float32),
            jax.ShapeDtypeStruct((1, terms), jnp.float32),
        ),
        in_specs=[vmem] + [stay] * 6 + [vmem] * 4,
        out_specs=(vmem, vmem),
        scratch_shapes=[
            f32(2, local_cols, entries, LANES),
            f32(2, local_cols, entries, LANES),
            f32(2, 2, local_cols, chi, width),
            f32(2, local_cols, chi, width),
            f32(2, chi, width),
            f32(2, local_cols, chi, width),
            f32(group, chi, width),
            f32(group, chi, width),
            f32(group, entries, LANES),
            f32(group + 1, chi, width),
            f32(group, D2**4, LANES),
            bf16(wide, width),
            bf16(group, 2 * chi, wide),
            bf16(group, LANES, wide),
            bf16(group, LANES, wide),
            f32(D2 * chi, LANES),
            f32(D2 * chi, wide),
            bf16(wide, pairs * wide),
            bf16(wide, pairs * wide),
            bf16(2, local_cols, 2 * chi, wide),
            bf16(2, local_cols, 2, LANES, wide),
            f32(D2 * chi, LANES),
            f32(2, local_cols, pairs, chi, wide),
            f32(2, chi, width),
            f32(2, chi, width),
            f32(2, pairs, chi // 2, width),
            f32(2, pairs, chi // 2, width),
            f32(col_count, terms, LANES),
            f32(row_count, 1, LANES),
            pltpu.SemaphoreType.REGULAR((2,)),
            dma((6,)),
            dma((3, group)),
            dma((3, group)),
            dma((group,)),
            dma((2, local_cols)),
            dma((group,)),
            dma((2, local_cols)),
            dma,
            dma,
            dma((2,)),
            dma((2,)),
            dma((2,)),
            dma((2,)),
            dma((2, most)),
            dma((2, most)),
        ],
        compiler_params=pltpu.CompilerParams(
            collective_id=0, has_side_effects=True, vmem_limit_bytes=56 * 1024 * 1024
        ),
        name="window",
    )(*args[:7], *(index[None] for index in args[7:10]), args[10])


def shards(*args):
    outs, energies = window(lax.axis_size("rows"), lax.axis_size("cols"), args)
    return (outs[0][None], outs[1][None], energies[0])


def solution(mesh):
    placed = (
        P("rows", "cols", None),
        P(None, "rows", "cols", None, None),
        P(None, "rows", "cols", None, None),
        P("cols", None, None),
        P("cols", None, None),
        P("rows", None, None),
        P("rows", None, None),
        P(),
        P(),
        P(),
        P(),
    )
    return jax.shard_map(
        shards,
        mesh=mesh,
        in_specs=placed,
        out_specs=(P("rows", "cols", None, None), P("rows", "cols", None, None), P()),
        check_vma=False,
    )
```

```python
import functools

import jax
import jax.numpy as jnp
from jax import lax
from jax.experimental import pallas as pl
from jax.experimental.pallas import tpu as pltpu
from jax.sharding import PartitionSpec as P

D = 2
D2 = 4
PHYS = 2
EPSILON = 1e-06
LANES = 128


def unpack_lanes(tiles, chi):
    rolled = {}
    lane = lax.broadcasted_iota(jnp.int32, tiles[0].shape, 1)
    blocks = []
    for block in range(D2):
        total = jnp.zeros_like(tiles[0])
        for place, tile in enumerate(tiles):
            low = max(chi * block, LANES * place)
            high = min(chi * (block + 1), LANES * (place + 1))
            if low >= high:
                continue
            shift = (LANES * place - chi * block) % LANES
            if (place, shift) not in rolled:
                rolled[place, shift] = tile if shift == 0 else pltpu.roll(tile, shift, 1)
            inside = (lane >= low - chi * block) & (lane < high - chi * block)
            total = jnp.where(inside, rolled[place, shift], total)
        blocks.append(total)
    return blocks


def pack_lanes(blocks, chi):
    lane = lax.broadcasted_iota(jnp.int32, blocks[0].shape, 1)
    rolled = {}
    tiles = []
    for place in range(chi * D2 // LANES):
        total = jnp.zeros_like(blocks[0])
        for block, values in enumerate(blocks):
            low = max(chi * block, LANES * place)
            high = min(chi * (block + 1), LANES * (place + 1))
            if low >= high:
                continue
            shift = (chi * block - LANES * place) % LANES
            if (block, shift) not in rolled:
                rolled[block, shift] = values if shift == 0 else pltpu.roll(values, shift, 1)
            inside = (lane >= low - LANES * place) & (lane < high - LANES * place)
            total = jnp.where(inside, rolled[block, shift], total)
        tiles.append(total)
    return tiles


def halves(values):
    high = values.astype(jnp.bfloat16)
    low = (values - high.astype(jnp.float32)).astype(jnp.bfloat16)
    return high, low


def dot32(former, latter):
    return jnp.dot(former, latter, preferred_element_type=jnp.float32)


def dot_last(former, latter):
    return lax.dot_general(
        former, latter, (((1,), (1,)), ((), ())), preferred_element_type=jnp.float32
    )


def load_tiles(ref, at, width):
    return [ref[at, :, LANES * t : LANES * (t + 1)] for t in range(width // LANES)]


def window_kernel(
    row_count,
    col_count,
    kets_ref,
    left_maps_ref,
    right_maps_ref,
    top_ref,
    bottom_ref,
    left_ref,
    right_ref,
    rows_ref,
    bonds_ref,
    ops_ref,
    table_ref,
    out_ref,
    energy_ref,
    kets,
    kets_near,
    maps,
    edges,
    sides,
    env_ref,
    pbuf,
    qbuf,
    kbuf,
    xbuf,
    ebuf,
    pick,
    turn_pick,
    pmap,
    rbuf,
    fold,
    xw,
    jbuf,
    thi,
    tlo,
    near,
    far,
    vbuf,
    opens,
    hop_out,
    hop_in,
    share,
    shared,
    token,
    load_sem,
    map_send,
    map_recv,
    env_send,
    side_send,
    env_recv,
    out_send,
    out_recv,
    chain_send,
    chain_recv,
    hop_send,
    hop_recv,
    share_send,
    share_recv,
    ket_send,
    ket_recv,
):
    local_cols = kets.shape[1]
    chi, width = maps.shape[3], maps.shape[4]
    wide = D2 * LANES
    pairs = PHYS * PHYS
    terms = rows_ref.shape[1]
    group = 2 * local_cols
    groups = row_count // group
    place = lax.axis_index("rows")
    cols_at = lax.axis_index("cols")
    has_left = cols_at > 0
    has_right = cols_at < col_count - 1
    mine = place // group
    me = place % group
    column = me // 2
    way = me % 2
    base = mine * group
    before = mine - 1 + 2 * way
    after = mine + 1 - 2 * way
    has_before = (before >= 0) & (before < groups)
    has_after = (after >= 0) & (after < groups)
    low_half = jnp.where(mine >= groups // 2, 1, 0)
    early, late = low_half, 1 - low_half
    has_lower = mine > 0
    has_upper = mine < groups - 1

    barrier = pltpu.get_barrier_semaphore()
    for at in range(col_count):
        for other in range(group):

            @pl.when((me != other) | (cols_at != at))
            def _():
                pl.semaphore_signal(
                    barrier, inc=1, device_id={"rows": base + other, "cols": at}
                )

    @pl.when(has_lower)
    def _():
        pl.semaphore_signal(barrier, inc=1, device_id={"rows": place - group})

    @pl.when(has_upper)
    def _():
        pl.semaphore_signal(barrier, inc=1, device_id={"rows": place + group})

    loads = [
        pltpu.make_async_copy(source, target, load_sem.at[at])
        for at, (source, target) in enumerate(
            (
                (right_maps_ref.at[:, 0], maps.at[0]),
                (left_maps_ref.at[:, 0], maps.at[1]),
                (top_ref, edges.at[0]),
                (bottom_ref, edges.at[1]),
                (left_ref, sides.at[pl.ds(0, 1)]),
                (right_ref, sides.at[pl.ds(1, 1)]),
            )
        )
    ]
    for load in loads:
        load.start()

    count = kets_ref.shape[2]
    spot = lax.broadcasted_iota(jnp.int32, (count, count), 0)
    from_lane = lax.broadcasted_iota(jnp.int32, (count, count), 1)

    def exchanged(high, low):
        top, bottom = (spot // high) % 2, (spot // low) % 2
        return spot + (bottom - top) * high + (top - bottom) * low

    def led(out, into):
        rest = (spot // 8) % 2 * 16 + (spot // 2) % 2 * 4 + spot % 2
        return rest + spot // 16 * out + (spot // 4) % 2 * into

    for order, ref, target in (
        (led(2, 8), kets, 0),
        (led(8, 2), kets, 1),
        (spot + (exchanged(8, 2) - spot) * late, kets_near, 0),
        (spot + (exchanged(8, 2) - spot) * late + (exchanged(4, 1) - spot), kets_near, 1),
    ):
        for at in range(local_cols):
            values = jnp.broadcast_to(kets_ref[0, at : at + 1, :], (count, count))
            tallest = jnp.sum(
                jnp.where(order == from_lane, values, 0.0), axis=1, keepdims=True
            )
            filled = jnp.broadcast_to(tallest, (count, LANES))
            if ref is kets:
                kets[target, at] = filled
            else:
                kets_near[at + 1, target] = filled

    chosen = lax.broadcasted_iota(jnp.int32, (wide, width), 0)
    entry = lax.broadcasted_iota(jnp.int32, (wide, width), 1)
    wanted = (chosen % LANES) * D2 + chosen // LANES
    live = (chosen % LANES) < chi
    pick[...] = jnp.where((wanted == entry) & live, 1.0, 0.0).astype(jnp.bfloat16)
    chosen = lax.broadcasted_iota(jnp.int32, (width, width), 0)
    entry = lax.broadcasted_iota(jnp.int32, (width, width), 1)
    wanted = (chosen % chi) * D2 + chosen // chi
    turn_pick[...] = jnp.where(wanted == entry, 1.0, 0.0).astype(jnp.bfloat16)
    xw[...] = jnp.zeros_like(xw)
    thi[...] = jnp.zeros_like(thi)
    tlo[...] = jnp.zeros_like(tlo)
    for load in loads:
        load.wait()
    greeted = jnp.where(has_lower, 1, 0) + jnp.where(has_upper, 1, 0)
    pl.semaphore_wait(barrier, group * col_count - 1 + greeted)

    def pass_token(way_at):
        pl.semaphore_signal(
            token.at[way_at], inc=1, device_id={"rows": place + (group, -group)[way_at]}
        )

    @pl.when(has_upper & jnp.logical_not(has_lower))
    def _():
        pass_token(0)

    @pl.when(has_lower & jnp.logical_not(has_upper))
    def _():
        pass_token(1)

    ket_copy = pltpu.make_async_remote_copy(
        kets_near.at[local_cols],
        kets_near.at[0],
        ket_send,
        ket_recv,
        device_id={"cols": cols_at + 1},
    )

    @pl.when(has_right)
    def _():
        ket_copy.start()

    def map_copies(target_way, target_col, target, local):
        made = []
        for kind, (source, buffer) in enumerate(
            ((kets, kbuf), (maps.at[0], qbuf), (maps.at[1], pbuf))
        ):
            origin, landing = source.at[target_way, target_col], buffer.at[me]
            if local:
                made.append(pltpu.make_async_copy(origin, landing, map_recv.at[kind, me]))
            else:
                made.append(
                    pltpu.make_async_remote_copy(
                        origin,
                        landing,
                        map_send.at[kind, target],
                        map_recv.at[kind, me],
                        device_id={"rows": base + target},
                    )
                )
        return made

    for turn in range(group):
        target_way = (low_half + turn // local_cols) % 2
        target_col = turn % local_cols
        target = target_col * 2 + target_way

        @pl.when(target != me)
        def _():
            for copy in map_copies(target_way, target_col, target, False):
                copy.start()

        @pl.when(target == me)
        def _():
            for copy in map_copies(target_way, target_col, target, True):
                copy.start()

    lane_pair = lax.broadcasted_iota(jnp.int32, (count // 2, width), 1) // chi

    def folded_kets(values):
        former, latter = (
            jnp.concatenate([part] * (width // LANES), axis=1)
            for part in (values[: count // 2], values[count // 2 :])
        )
        ket = jnp.where(lane_pair // D == 0, former, latter)
        bra = jnp.where(lane_pair % D == 0, former, latter)
        legs = D**3
        for i in range(legs):
            total = ket[i : i + 1] * bra[:legs]
            for p in range(1, PHYS):
                total += ket[p * legs + i : p * legs + i + 1] * bra[p * legs : (p + 1) * legs]
            ebuf[i * legs : (i + 1) * legs] = total

    def fold_into(target):
        chunk = 16

        def through(at, unused):
            start = pl.multiple_of(at * chunk, chunk)
            tiles = [rbuf[pl.ds(c * chi + start, chunk), :] for c in range(D2)]
            for g in range(D2):
                for h in range(D2):
                    total = None
                    for c, tile in enumerate(tiles):
                        ket_at = (h // D) * 4 + (g // D) * 2 + c // D
                        bra_at = (h % D) * 4 + (g % D) * 2 + c % D
                        spot = ket_at * D**3 + bra_at
                        term = ebuf[spot : spot + 1, :] * tile
                        total = term if total is None else total + term
                    high, low = halves(total)
                    rows = pl.ds((g * D2 + h) * chi + start, chunk)
                    target[rows, :width] = high
                    target[rows, width:] = low
            return unused

        lax.fori_loop(0, chi // chunk, through, 0)

    def put_right(values):
        high, low = halves(values)
        xw[:chi] = high
        xw[LANES : LANES + chi] = low

    def joined_with(high, low):
        return dot32(jnp.concatenate([high, high], axis=1), xw[...]) + dot32(low, xw[:LANES])

    def absorbed(joined, folded):
        rows = []
        for part in halves(joined):
            rows.append(
                jnp.concatenate([part[g * chi : (g + 1) * chi] for g in range(D2)], axis=1)
            )
        large = dot32(jnp.concatenate(rows, axis=0), folded)
        high, low = large[:, :width], large[:, width:]
        return high[:chi] + ((high[chi:] + low[:chi]) + low[chi:])

    def normalized(values):
        square = jnp.sum(jnp.sum(values * values, axis=1, keepdims=True), axis=0, keepdims=True)
        return values * (1.0 / jnp.sqrt(square / (chi * width) + EPSILON))

    def prepare(step, unused):
        slot = step + way * (group - 1 - 2 * step)
        for kind, buffer in enumerate((kbuf, qbuf, pbuf)):
            pltpu.make_async_copy(
                buffer.at[slot], buffer.at[slot], map_recv.at[kind, slot]
            ).wait()
        folded_kets(kbuf[slot])
        for at, part in enumerate(halves(pbuf[slot])):
            spread_map = dot_last(part, pick[...]).astype(jnp.bfloat16)
            for l in range(D2):
                pmap[step, at, l * chi : (l + 1) * chi] = spread_map[
                    :, l * LANES : (l + 1) * LANES
                ]
        high, low = (
            dot_last(turn_pick[...], jnp.concatenate([part] * D2, axis=0))
            for part in halves(qbuf[slot])
        )
        rbuf[...] = high + low
        fold_into(fold.at[step])
        return unused

    def row_copy(source, landing, send, recv, slot):
        remote = pltpu.make_async_remote_copy(
            source, landing, send, recv, device_id={"rows": base + slot}
        )
        return remote, pltpu.make_async_copy(source, landing, recv)

    def send_row(source, landing, send, recv, slot):
        remote, local = row_copy(source, landing, send, recv, slot)

        @pl.when(slot != me)
        def _():
            remote.start()

        @pl.when(slot == me)
        def _():
            local.start()

    chain_hop = pltpu.make_async_remote_copy(
        xbuf.at[group],
        xbuf.at[0],
        chain_send,
        chain_recv,
        device_id={"rows": after * group + me},
    )

    start_slot = way * (group - 1)
    crossing = jnp.logical_not(has_before) & ((start_slot // local_cols) != (me // local_cols))
    ahead = jnp.where(has_before, group, jnp.where(crossing, group - local_cols + 1, 1))
    turned_by = jnp.where(crossing, local_cols, 0)

    def prepare_ahead(turn, unused):
        return prepare((turn + turned_by) % group, unused)

    lax.fori_loop(0, ahead, prepare_ahead, 0)

    @pl.when(has_lower & has_upper)
    def _():
        for way_at in range(2):
            pl.semaphore_wait(token.at[way_at], 1)
            pass_token(way_at)

    def side_copy(step, slot):
        return pltpu.make_async_remote_copy(
            xbuf.at[step],
            env_ref.at[way, 0],
            side_send.at[step],
            env_recv.at[way, 0],
            device_id={"rows": base + slot, "cols": cols_at + 1},
        )

    def absorb(step, unused):
        slot = step + way * (group - 1 - 2 * step)

        pending = (step >= 1) & jnp.logical_not(crossing & (step >= local_cols))

        @pl.when(pending & jnp.logical_not(has_before))
        def _():
            prepare(step, 0)

        send_row(
            xbuf.at[step],
            env_ref.at[way, column + 1],
            env_send.at[step],
            env_recv.at[way, column + 1],
            slot,
        )

        @pl.when(has_right & (column == local_cols - 1))
        def _():
            side_copy(step, slot).start()

        joined = joined_with(pmap[step, 0], pmap[step, 1])
        renewed = normalized(absorbed(joined, fold[step]))
        xbuf[step + 1] = renewed
        put_right(renewed)

        @pl.when((step == group - 1) & has_after)
        def _():
            chain_hop.start()

        return unused

    def run_chain():
        @pl.when(has_before)
        def _():
            pltpu.make_async_copy(xbuf.at[0], xbuf.at[0], chain_recv).wait()

        @pl.when(jnp.logical_not(has_before) & (way == 0))
        def _():
            xbuf[0] = edges[0, column]

        @pl.when(jnp.logical_not(has_before) & (way == 1))
        def _():
            xbuf[0] = edges[1, column]

        put_right(xbuf[0])
        lax.fori_loop(0, group, absorb, 0)

        for step in range(group):
            send_row(
                xbuf.at[step + 1],
                out_ref.at[way, column],
                out_send.at[step],
                out_recv.at[way, column],
                step + way * (group - 1 - 2 * step),
            )

    unit = jnp.where(
        lax.broadcasted_iota(jnp.int32, (LANES, LANES), 0)
        == lax.broadcasted_iota(jnp.int32, (LANES, LANES), 1),
        1.0,
        0.0,
    ).astype(jnp.bfloat16)
    fill = jnp.zeros((LANES - chi, LANES), jnp.bfloat16)

    def take_blocks(kind, at):
        landed = env_ref.at[kind, at]
        pltpu.make_async_copy(landed, landed, env_recv.at[kind, at]).wait()
        blocks = unpack_lanes(load_tiles(env_ref.at[kind], at, width), chi)
        for d, block in enumerate(blocks):
            lanes = slice(d * LANES, (d + 1) * LANES)
            for part, values in enumerate(halves(block)):
                tall_block = jnp.concatenate([values, fill], axis=0)
                turned = dot_last(unit, tall_block).astype(jnp.bfloat16)
                yield lanes, part, values, tall_block, turned

    def take_far(at):
        for lanes, part, values, tall_block, turned in take_blocks(early, at):
            far[1, at, part, :, lanes] = turned
            far[0, at, part, :, lanes] = tall_block

    def take_near(at):
        for lanes, part, values, tall_block, turned in take_blocks(late, at):
            rows = slice(part * chi, (part + 1) * chi)
            near[0, at, rows, lanes] = turned[:chi]
            near[1, at, rows, lanes] = values

    def for_columns(take):
        for at in range(1, local_cols + 1):
            take(at)

        @pl.when(has_left)
        def _():
            take(0)

    second = jnp.where(cols_at >= col_count // 2, 1, 0)

    def hop(side, step):
        return pltpu.make_async_remote_copy(
            hop_out.at[side],
            hop_in.at[side],
            hop_send.at[side],
            hop_recv.at[side],
            device_id={"cols": cols_at + step},
        )

    def put_environ(blocks):
        for at, block in enumerate(blocks):
            vbuf[at * chi : (at + 1) * chi] = block

    def put_edge(side):
        blocks = unpack_lanes(load_tiles(sides, side, width), chi)

        @pl.when(late == 0)
        def _():
            put_environ(blocks)

        @pl.when(late == 1)
        def _():
            empty = jnp.zeros((LANES - chi, LANES), jnp.float32)
            put_environ([jnp.concatenate([block, empty], axis=0).T[:chi] for block in blocks])

    def place_of(side, order):
        return order + side * (local_cols - 2 * order)

    def open_up(side, at_column):
        v_high, v_low = halves(vbuf[...])
        f_high = far[side, at_column, 0]
        jbuf[...] = dot32(v_high, f_high) + (
            dot32(v_high, far[side, at_column, 1]) + dot32(v_low, f_high)
        )
        chunk = 16

        def ket(p, u, i, d, o):
            at = p * 16 + u * 8 + i * 4 + d * 2 + o
            return kets_near[at_column, side, at : at + 1, :]

        def through(at, unused):
            start = pl.multiple_of(at * chunk, chunk)

            def joined(i, d):
                return jbuf[pl.ds(i * chi + start, chunk), d * LANES : (d + 1) * LANES]

            for p in range(PHYS):
                for u in range(D):
                    for o in range(D):
                        part = {}
                        for i2 in range(D):
                            for d2 in range(D):
                                total = None
                                for i in range(D):
                                    for d in range(D):
                                        term = ket(p, u, i, d, o) * joined(
                                            i * D + i2, d * D + d2
                                        )
                                        total = term if total is None else total + term
                                part[i2, d2] = total
                        for q in range(PHYS):
                            for u2 in range(D):
                                for o2 in range(D):
                                    total = None
                                    for i2 in range(D):
                                        for d2 in range(D):
                                            term = ket(q, u2, i2, d2, o2) * part[i2, d2]
                                            total = term if total is None else total + term
                                    high, low = halves(total)
                                    rows = pl.ds((u * D + u2) * LANES + start, chunk)
                                    spot = (p * PHYS + q) * D2 + o * D + o2
                                    lanes = slice(spot * LANES, (spot + 1) * LANES)
                                    thi[rows, lanes] = high
                                    tlo[rows, lanes] = low
            return unused

        lax.fori_loop(0, chi // chunk, through, 0)

    def first_order(side):
        return jnp.where((side == 0) & (cols_at == 0), 1, 0)

    def is_edge(side):
        return ((side == 0) & (cols_at == 0)) | ((side == 1) & (cols_at == col_count - 1))

    def early_work():
        @pl.when(has_left)
        def _():
            pltpu.make_async_copy(kets_near.at[0], kets_near.at[0], ket_recv).wait()

        for_columns(take_far)
        for side in range(2):

            @pl.when(is_edge(side))
            def _():
                put_edge(side)

        @pl.when(is_edge(second))
        def _():
            open_up(second, place_of(second, first_order(second)))

    early_first = (way != low_half) & (mine != groups // 2) & (mine != groups // 2 - 1)
    early_at = jnp.where(early_first, 0, 1)

    def phase(at, unused):
        @pl.when(at == early_at)
        def _():
            early_work()

        @pl.when(at != early_at)
        def _():
            run_chain()

        return unused

    lax.fori_loop(0, 2, phase, 0)
    for_columns(take_near)

    spot_row = lax.broadcasted_iota(jnp.int32, (terms, terms), 0)
    spot_lane = lax.broadcasted_iota(jnp.int32, (terms, terms), 1)

    def stand(ref):
        values = jnp.broadcast_to(ref[...].astype(jnp.float32), (terms, terms))
        return jnp.sum(jnp.where(spot_row == spot_lane, values, 0.0), axis=1, keepdims=True)

    term_row = stand(rows_ref).astype(jnp.int32)
    term_bond = stand(bonds_ref).astype(jnp.int32)
    term_op = stand(ops_ref).astype(jnp.int32)
    term_weights = jnp.zeros((terms, table_ref.shape[1]), jnp.float32)
    for op in range(table_ref.shape[0]):
        term_weights = jnp.where(term_op == op, table_ref[op : op + 1, :], term_weights)

    def walk(turn, unused):
        side = (turn // local_cols + second) % 2
        order = turn % local_cols
        at_column = place_of(side, order)
        absent = (cols_at == 0) & (at_column == side)
        opening = order == first_order(side)
        ending = order == local_cols - 1

        @pl.when((order == 0) & jnp.logical_not(is_edge(side)))
        def _():
            pltpu.make_async_copy(hop_in.at[side], hop_in.at[side], hop_recv.at[side]).wait()
            put_environ(unpack_lanes(load_tiles(hop_in, side, width), chi))

        @pl.when(jnp.logical_not(absent) & jnp.logical_not(opening & is_edge(side)))
        def _():
            open_up(side, at_column)

        @pl.when(jnp.logical_not(absent))
        def _():
            both = near[side, at_column]
            closed = None
            for pair in range(pairs):
                lanes = slice(pair * wide, (pair + 1) * wide)
                large = dot32(both, thi[:, lanes])
                value = large[:chi] + (large[chi:] + dot32(both[:chi], tlo[:, lanes]))
                opens[side, at_column - side, pair] = value
                if pair // PHYS == pair % PHYS:
                    closed = value if closed is None else closed + value
            square = jnp.sum(
                jnp.sum(closed * closed, axis=1, keepdims=True), axis=0, keepdims=True
            )
            closed = closed * (1.0 / jnp.sqrt(square / (chi * width) + EPSILON))
            blocks = [closed[:, d * LANES : (d + 1) * LANES] for d in range(D2)]
            put_environ(blocks)

            @pl.when(ending)
            def _():
                for t, tile in enumerate(pack_lanes(blocks, chi)):
                    hop_out[side, :, t * LANES : (t + 1) * LANES] = tile

        @pl.when(ending & (side == 0) & has_right)
        def _():
            hop(0, 1).start()

        @pl.when(ending & (side == 1) & has_left)
        def _():
            hop(1, -1).start()

        return unused

    lax.fori_loop(0, 2 * local_cols, walk, 0)

    tall = (terms, LANES)
    lane = lax.broadcasted_iota(jnp.int32, tall, 1)
    held = shared.at[0]
    held[...] = jnp.zeros(tall, jnp.float32)
    here = jnp.zeros((terms, 1), jnp.int32)
    for k in range(local_cols):
        bond = cols_at * local_cols + k - 1
        hit = (term_row == place) & (term_bond == bond)
        here = jnp.where(hit, 1, here)

        def add_bond(k=k, hit=hit):
            values = jnp.zeros(tall, jnp.float32)
            for p in range(pairs):
                former = opens[0, k, p]
                for q in range(pairs):
                    value = jnp.sum(
                        jnp.sum(former * opens[1, k, q], axis=0, keepdims=True),
                        axis=1,
                        keepdims=True,
                    )
                    values = jnp.where(lane == p * pairs + q, value, values)
            held[...] += jnp.where(hit, values, 0.0)

        if k:
            add_bond()
        else:
            pl.when(has_left)(add_bond)

    total = held[...]
    picked = jnp.sum(total[:, : pairs * pairs] * term_weights, axis=1, keepdims=True)
    bra, ket_at = lane % pairs, lane // pairs
    diagonal = (bra // PHYS == bra % PHYS) & (ket_at // PHYS == ket_at % PHYS)
    trace = jnp.sum(
        jnp.where(diagonal & (lane < pairs * pairs), total, 0.0), axis=1, keepdims=True
    )
    size = jnp.sqrt(jnp.sum(total * total, axis=1, keepdims=True))
    energy = picked / jnp.maximum(jnp.abs(trace), 0.25 * size)
    same = lax.broadcasted_iota(jnp.int32, tall, 0) == lane
    devices = row_count * col_count
    spot_mine = place * col_count + cols_at
    own = share.at[devices]
    own[...] = jnp.sum(jnp.where(same & (here == 1), energy, 0.0), axis=0, keepdims=True)

    @pl.when(has_lower & jnp.logical_not(has_upper))
    def _():
        pl.semaphore_wait(token.at[0], 1)

    @pl.when(has_upper & jnp.logical_not(has_lower))
    def _():
        pl.semaphore_wait(token.at[1], 1)

    def tell(other, unused):
        @pl.when(other != spot_mine)
        def _():
            pltpu.make_async_remote_copy(
                own,
                share.at[spot_mine],
                share_send,
                share_recv,
                device_id={"rows": other // col_count, "cols": other % col_count},
            ).start()

        return unused

    lax.fori_loop(0, devices, tell, 0)
    pltpu.make_async_copy(own, share.at[spot_mine], share_recv).start()
    everyone = share.at[pl.ds(0, devices)]
    pltpu.make_async_copy(everyone, everyone, share_recv).wait()
    energy_ref[...] = jnp.sum(share[:devices], axis=0)[:, :terms]
    others = share.at[pl.ds(0, devices - 1)]
    pltpu.make_async_copy(others, others, share_send).wait()

    @pl.when(has_right)
    def _():
        hop(0, 1).wait_send()
        ket_copy.wait_send()

    @pl.when(has_left)
    def _():
        hop(1, -1).wait_send()

    for step in range(group):
        slot = step + way * (group - 1 - 2 * step)

        @pl.when(slot != me)
        def _():
            row_copy(
                xbuf.at[step],
                env_ref.at[way, column + 1],
                env_send.at[step],
                env_recv.at[way, column + 1],
                slot,
            )[0].wait_send()
            row_copy(
                xbuf.at[step + 1],
                out_ref.at[way, column],
                out_send.at[step],
                out_recv.at[way, column],
                slot,
            )[0].wait_send()

        @pl.when(has_right & (column == local_cols - 1))
        def _():
            side_copy(step, slot).wait_send()

    for target in range(group):

        @pl.when(target != me)
        def _():
            for copy in map_copies(target % 2, target // 2, target, False):
                copy.wait_send()

    @pl.when(has_after)
    def _():
        chain_hop.wait_send()

    for a in range(2):
        for b in range(local_cols):
            pltpu.make_async_copy(out_ref.at[a, b], out_ref.at[a, b], out_recv.at[a, b]).wait()


def window(row_count, col_count, args):
    local_cols = args[0].shape[1]
    chi, width = args[1].shape[-2:]
    terms = args[7].shape[0]
    group = 2 * local_cols
    wide = D2 * LANES
    pairs = PHYS * PHYS
    entries = args[0].shape[2]
    vmem = pl.BlockSpec(memory_space=pltpu.VMEM)
    stay = pl.BlockSpec(memory_space=pltpu.HBM)
    dma = pltpu.SemaphoreType.DMA

    def f32(*shape):
        return pltpu.VMEM(shape, jnp.float32)

    def bf16(*shape):
        return pltpu.VMEM(shape, jnp.bfloat16)

    return pl.pallas_call(
        functools.partial(window_kernel, row_count, col_count),
        out_shape=(
            jax.ShapeDtypeStruct((2, local_cols, chi, width), jnp.float32),
            jax.ShapeDtypeStruct((1, terms), jnp.float32),
        ),
        in_specs=[vmem] + [stay] * 6 + [vmem] * 4,
        out_specs=(vmem, vmem),
        scratch_shapes=[
            f32(2, local_cols, entries, LANES),
            f32(local_cols + 1, 2, entries, LANES),
            f32(2, 2, local_cols, chi, width),
            f32(2, local_cols, chi, width),
            f32(2, chi, width),
            f32(2, local_cols + 1, chi, width),
            f32(group, chi, width),
            f32(group, chi, width),
            f32(group, entries, LANES),
            f32(group + 1, chi, width),
            f32(D2**3, width),
            bf16(wide, width),
            bf16(width, width),
            bf16(group, 2, width, LANES),
            f32(width, width),
            bf16(group, D2 * width, 2 * width),
            bf16(2 * LANES, width),
            f32(D2 * chi, wide),
            bf16(wide, pairs * wide),
            bf16(wide, pairs * wide),
            bf16(2, local_cols + 1, 2 * chi, wide),
            bf16(2, local_cols + 1, 2, LANES, wide),
            f32(D2 * chi, LANES),
            f32(2, local_cols, pairs, chi, wide),
            f32(2, chi, width),
            f32(2, chi, width),
            f32(row_count * col_count + 1, 1, LANES),
            f32(1, terms, LANES),
            pltpu.SemaphoreType.REGULAR((2,)),
            dma((6,)),
            dma((3, group)),
            dma((3, group)),
            dma((group,)),
            dma((group,)),
            dma((2, local_cols + 1)),
            dma((group,)),
            dma((2, local_cols)),
            dma,
            dma,
            dma((2,)),
            dma((2,)),
            dma,
            dma,
            dma,
            dma,
        ],
        compiler_params=pltpu.CompilerParams(
            collective_id=0, has_side_effects=True, vmem_limit_bytes=56 * 1024 * 1024
        ),
        name="window",
    )(*args[:7], *(index[None] for index in args[7:10]), args[10])


def shards(*args):
    outs, energies = window(lax.axis_size("rows"), lax.axis_size("cols"), args)
    return (outs[0][None], outs[1][None], energies[0])


def solution(mesh):
    placed = (
        P("rows", "cols", None),
        P(None, "rows", "cols", None, None),
        P(None, "rows", "cols", None, None),
        P("cols", None, None),
        P("cols", None, None),
        P("rows", None, None),
        P("rows", None, None),
        P(),
        P(),
        P(),
        P(),
    )
    return jax.shard_map(
        shards,
        mesh=mesh,
        in_specs=placed,
        out_specs=(P("rows", "cols", None, None), P("rows", "cols", None, None), P()),
        check_vma=False,
    )
```

```python
import functools

import jax
import jax.numpy as jnp
from jax import lax
from jax.experimental import pallas as pl
from jax.experimental.pallas import tpu as pltpu
from jax.sharding import PartitionSpec as P

D = 2
D2 = 4
PHYS = 2
EPSILON = 1e-06
LANES = 128
PACE = 9


def unpack_lanes(tiles, chi):
    rolled = {}
    lane = lax.broadcasted_iota(jnp.int32, tiles[0].shape, 1)
    blocks = []
    for block in range(D2):
        total = jnp.zeros_like(tiles[0])
        for place, tile in enumerate(tiles):
            low = max(chi * block, LANES * place)
            high = min(chi * (block + 1), LANES * (place + 1))
            if low >= high:
                continue
            shift = (LANES * place - chi * block) % LANES
            if (place, shift) not in rolled:
                rolled[place, shift] = tile if shift == 0 else pltpu.roll(tile, shift, 1)
            inside = (lane >= low - chi * block) & (lane < high - chi * block)
            total = jnp.where(inside, rolled[place, shift], total)
        blocks.append(total)
    return blocks


def pack_lanes(blocks, chi):
    lane = lax.broadcasted_iota(jnp.int32, blocks[0].shape, 1)
    rolled = {}
    tiles = []
    for place in range(chi * D2 // LANES):
        total = jnp.zeros_like(blocks[0])
        for block, values in enumerate(blocks):
            low = max(chi * block, LANES * place)
            high = min(chi * (block + 1), LANES * (place + 1))
            if low >= high:
                continue
            shift = (chi * block - LANES * place) % LANES
            if (block, shift) not in rolled:
                rolled[block, shift] = values if shift == 0 else pltpu.roll(values, shift, 1)
            inside = (lane >= low - LANES * place) & (lane < high - LANES * place)
            total = jnp.where(inside, rolled[block, shift], total)
        tiles.append(total)
    return tiles


def halves(values):
    high = values.astype(jnp.bfloat16)
    low = (values - high.astype(jnp.float32)).astype(jnp.bfloat16)
    return high, low


def dot32(former, latter):
    return jnp.dot(former, latter, preferred_element_type=jnp.float32)


def dot_last(former, latter):
    return lax.dot_general(
        former, latter, (((1,), (1,)), ((), ())), preferred_element_type=jnp.float32
    )


def load_tiles(ref, at, width):
    return [ref[at, :, LANES * t : LANES * (t + 1)] for t in range(width // LANES)]


def window_kernel(
    row_count,
    col_count,
    kets_ref,
    left_maps_ref,
    right_maps_ref,
    top_ref,
    bottom_ref,
    left_ref,
    right_ref,
    rows_ref,
    bonds_ref,
    ops_ref,
    table_ref,
    out_ref,
    energy_ref,
    kets,
    kets_near,
    maps,
    edges,
    sides,
    env_ref,
    pbuf,
    qbuf,
    kbuf,
    xbuf,
    ebuf,
    pick,
    turn_pick,
    pmap,
    rbuf,
    fold,
    xw,
    jbuf,
    thi,
    tlo,
    near,
    far,
    vbuf,
    opens,
    hop_out,
    hop_in,
    share,
    shared,
    token,
    load_sem,
    map_send,
    map_recv,
    env_send,
    side_send,
    env_recv,
    out_send,
    out_recv,
    chain_send,
    chain_recv,
    hop_send,
    hop_recv,
    share_send,
    share_recv,
    ket_send,
    ket_recv,
):
    local_cols = kets.shape[1]
    chi, width = maps.shape[3], maps.shape[4]
    wide = D2 * LANES
    pairs = PHYS * PHYS
    terms = rows_ref.shape[1]
    group = 2 * local_cols
    groups = row_count // group
    place = lax.axis_index("rows")
    cols_at = lax.axis_index("cols")
    mine = place // group
    me = place % group
    column = me // 2
    way = me % 2
    base = mine * group
    before = mine - 1 + 2 * way
    after = mine + 1 - 2 * way
    has_before = (before >= 0) & (before < groups)
    has_after = (after >= 0) & (after < groups)
    low_half = jnp.where(mine >= groups // 2, 1, 0)
    early, late = low_half, 1 - low_half
    onward = 1 - 2 * late
    rank = cols_at + late * (col_count - 1 - 2 * cols_at)
    has_prev = rank > 0
    has_next = rank < col_count - 1
    edge_col = low_half * (local_cols - 1)

    def spot_of(at):
        return at + 1 + late * (local_cols - 1 - 2 * at)

    def true_side(side):
        return side + late * (1 - 2 * side)
    has_lower = mine > 0
    has_upper = mine < groups - 1

    barrier = pltpu.get_barrier_semaphore()
    for at in range(col_count):
        for other in range(group):

            @pl.when((me != other) | (cols_at != at))
            def _():
                pl.semaphore_signal(
                    barrier, inc=1, device_id={"rows": base + other, "cols": at}
                )

    @pl.when(has_lower)
    def _():
        pl.semaphore_signal(barrier, inc=1, device_id={"rows": place - group})

    @pl.when(has_upper)
    def _():
        pl.semaphore_signal(barrier, inc=1, device_id={"rows": place + group})

    loads = [
        pltpu.make_async_copy(source, target, load_sem.at[at])
        for at, (source, target) in enumerate(
            (
                (right_maps_ref.at[:, 0], maps.at[0]),
                (left_maps_ref.at[:, 0], maps.at[1]),
                (top_ref, edges.at[0]),
                (bottom_ref, edges.at[1]),
                (left_ref, sides.at[pl.ds(0, 1)]),
                (right_ref, sides.at[pl.ds(1, 1)]),
            )
        )
    ]
    for load in loads:
        load.start()

    count = kets_ref.shape[2]
    spot = lax.broadcasted_iota(jnp.int32, (count, count), 0)
    from_lane = lax.broadcasted_iota(jnp.int32, (count, count), 1)

    def exchanged(high, low):
        top, bottom = (spot // high) % 2, (spot // low) % 2
        return spot + (bottom - top) * high + (top - bottom) * low

    def led(out, into):
        rest = (spot // 8) % 2 * 16 + (spot // 2) % 2 * 4 + spot % 2
        return rest + spot // 16 * out + (spot // 4) % 2 * into

    for order, ref, target in (
        (led(2, 8), kets, 0),
        (led(8, 2), kets, 1),
        (spot + (exchanged(8, 2) - spot) * late, kets_near, 0),
        (spot + (exchanged(8, 2) - spot) * late + (exchanged(4, 1) - spot), kets_near, 1),
    ):
        for at in range(local_cols):
            values = jnp.broadcast_to(kets_ref[0, at : at + 1, :], (count, count))
            tallest = jnp.sum(
                jnp.where(order == from_lane, values, 0.0), axis=1, keepdims=True
            )
            filled = jnp.broadcast_to(tallest, (count, LANES))
            if ref is kets:
                kets[target, at] = filled
            else:
                kets_near[spot_of(at), target] = filled

    chosen = lax.broadcasted_iota(jnp.int32, (width, wide), 1)
    entry = lax.broadcasted_iota(jnp.int32, (width, wide), 0)
    wanted = (chosen % LANES) * D2 + chosen // LANES
    live = (chosen % LANES) < chi
    pick[...] = jnp.where((wanted == entry) & live, 1.0, 0.0).astype(jnp.bfloat16)
    chosen = lax.broadcasted_iota(jnp.int32, (width, width), 0)
    entry = lax.broadcasted_iota(jnp.int32, (width, width), 1)
    wanted = (chosen % chi) * D2 + chosen // chi
    turn_pick[...] = jnp.where(wanted == entry, 1.0, 0.0).astype(jnp.bfloat16)
    xw[...] = jnp.zeros_like(xw)
    for load in loads:
        load.wait()
    greeted = jnp.where(has_lower, 1, 0) + jnp.where(has_upper, 1, 0)
    pl.semaphore_wait(barrier, group * col_count - 1 + greeted)

    def pass_token(way_at):
        pl.semaphore_signal(
            token.at[way_at], inc=1, device_id={"rows": place + (group, -group)[way_at]}
        )

    @pl.when(has_upper & jnp.logical_not(has_lower))
    def _():
        pass_token(0)

    @pl.when(has_lower & jnp.logical_not(has_upper))
    def _():
        pass_token(1)

    ket_copy = pltpu.make_async_remote_copy(
        kets_near.at[local_cols],
        kets_near.at[0],
        ket_send,
        ket_recv,
        device_id={"cols": cols_at + onward},
    )

    @pl.when(has_next)
    def _():
        ket_copy.start()

    def map_copies(target_way, target_col, target, local):
        made = []
        for kind, (source, buffer) in enumerate(
            ((kets, kbuf), (maps.at[0], qbuf), (maps.at[1], pbuf))
        ):
            origin, landing = source.at[target_way, target_col], buffer.at[me]
            if local:
                made.append(pltpu.make_async_copy(origin, landing, map_recv.at[kind, me]))
            else:
                made.append(
                    pltpu.make_async_remote_copy(
                        origin,
                        landing,
                        map_send.at[kind, target],
                        map_recv.at[kind, me],
                        device_id={"rows": base + target},
                    )
                )
        return made

    def each_map(target_way, cross, act):
        for target_col in range(local_cols):
            target = target_col * 2 + target_way
            wanted = (target_col != column) if cross else (target_col == column)

            @pl.when(wanted & (target != me))
            def _():
                for copy in map_copies(target_way, target_col, target, False):
                    act(copy, False)

            @pl.when(wanted & (target == me))
            def _():
                for copy in map_copies(target_way, target_col, target, True):
                    act(copy, True)

    def start(copy, local):
        copy.start()

    def finish(copy, local):
        if not local:
            copy.wait_send()

    opening_chain = jnp.logical_not(has_before)

    def start_later_maps():
        for cross in (True, False):
            each_map(late, cross, start)

    each_map(low_half, False, start)
    leading = me % 2 == low_half

    @pl.when(leading)
    def _():
        each_map(low_half, True, start)

    def clear(at, unused):
        thi[...] = jnp.zeros_like(thi)
        tlo[...] = jnp.zeros_like(tlo)
        return unused

    lax.fori_loop(0, jnp.where(leading, 1, PACE), clear, 0)

    @pl.when(jnp.logical_not(leading))
    def _():
        each_map(low_half, True, start)

    @pl.when(has_before)
    def _():
        each_map(low_half, True, finish)
        start_later_maps()

    lane_pair = lax.broadcasted_iota(jnp.int32, (count // 2, width), 1) // chi

    def folded_kets(values):
        former, latter = (
            jnp.concatenate([part] * (width // LANES), axis=1)
            for part in (values[: count // 2], values[count // 2 :])
        )
        ket = jnp.where(lane_pair // D == 0, former, latter)
        bra = jnp.where(lane_pair % D == 0, former, latter)
        legs = D**3
        for i in range(legs):
            total = ket[i : i + 1] * bra[:legs]
            for p in range(1, PHYS):
                total += ket[p * legs + i : p * legs + i + 1] * bra[p * legs : (p + 1) * legs]
            ebuf[i * legs : (i + 1) * legs] = total

    def fold_into(target):
        chunk = 16
        full = width // (2 * LANES) * 2 * LANES

        def through(at, unused):
            start = pl.multiple_of(at * chunk, chunk)
            tiles = [rbuf[pl.ds(c * chi + start, chunk), :] for c in range(D2)]
            for g in range(D2):
                for h in range(D2):
                    total = None
                    for c, tile in enumerate(tiles):
                        ket_at = (h // D) * 4 + (g // D) * 2 + c // D
                        bra_at = (h % D) * 4 + (g % D) * 2 + c % D
                        spot = ket_at * D**3 + bra_at
                        term = ebuf[spot : spot + 1, :] * tile
                        total = term if total is None else total + term
                    high, low = halves(total)
                    rows = pl.ds((g * D2 + h) * chi + start, chunk)
                    target[rows, :width] = high
                    target[rows, width : 2 * width - full] = low[:, full:]
                    target[rows, 2 * width - full :] = low[:, :full]
            return unused

        lax.fori_loop(0, chi // chunk, through, 0)

    def put_right(values):
        high, low = halves(values)
        xw[:chi] = high
        xw[LANES : LANES + chi] = low

    def joined_with(high, low):
        return dot32(jnp.concatenate([high, high], axis=1), xw[...]) + dot32(low, xw[:LANES])

    def absorbed(at_step):
        full = width // (2 * LANES) * 2 * LANES
        part = D2 * chi // 2
        joined = [
            joined_with(pmap[at_step, 0, at : at + part], pmap[at_step, 1, at : at + part])
            for at in (0, part)
        ]
        total = None
        for at, piece in enumerate(joined):
            rows = [
                jnp.concatenate([half[g * chi : (g + 1) * chi] for g in range(D2 // 2)], axis=1)
                for half in halves(piece)
            ]
            depth = slice(at * D2 // 2 * width, (at + 1) * D2 // 2 * width)
            large = dot32(jnp.concatenate(rows, axis=0), fold[at_step, depth, : 2 * width - full])
            front = large[:chi, :width] + large[chi:, :width]
            rest = large[:chi, width:] + large[chi:, width:]
            small = dot32(rows[0], fold[at_step, depth, 2 * width - full :])
            value = jnp.concatenate([front[:, :full] + small, front[:, full:] + rest], axis=1)
            total = value if total is None else total + value
        return total

    def normalized(values):
        square = jnp.sum(jnp.sum(values * values, axis=1, keepdims=True), axis=0, keepdims=True)
        return values * (1.0 / jnp.sqrt(square / (chi * width) + EPSILON))

    def prepare(step, unused):
        slot = step + way * (group - 1 - 2 * step)
        for kind, buffer in enumerate((kbuf, qbuf, pbuf)):
            pltpu.make_async_copy(
                buffer.at[slot], buffer.at[slot], map_recv.at[kind, slot]
            ).wait()
        folded_kets(kbuf[slot])
        gap = jnp.zeros((LANES - chi, width), jnp.bfloat16)
        high, low = halves(qbuf[slot])
        turned = dot_last(turn_pick[...], jnp.concatenate([high, gap, low, gap], axis=0))
        turned = turned[:, :LANES] + turned[:, LANES:]
        for t, tile in enumerate(pack_lanes([turned] * D2, chi)):
            rbuf[:, t * LANES : (t + 1) * LANES] = tile
        spread_map = dot32(
            jnp.concatenate(halves(pbuf[slot]), axis=0), pick[...]
        ).astype(jnp.bfloat16)
        for at in range(2):
            for l in range(D2):
                pmap[step, at, l * chi : (l + 1) * chi] = spread_map[
                    at * chi : (at + 1) * chi, l * LANES : (l + 1) * LANES
                ]
        fold_into(fold.at[step])
        return unused

    def row_copy(source, landing, send, recv, slot):
        remote = pltpu.make_async_remote_copy(
            source, landing, send, recv, device_id={"rows": base + slot}
        )
        return remote, pltpu.make_async_copy(source, landing, recv)

    def send_row(source, landing, send, recv, slot):
        remote, local = row_copy(source, landing, send, recv, slot)

        @pl.when(slot != me)
        def _():
            remote.start()

        @pl.when(slot == me)
        def _():
            local.start()

    chain_hop = pltpu.make_async_remote_copy(
        xbuf.at[group],
        xbuf.at[0],
        chain_send,
        chain_recv,
        device_id={"rows": after * group + me},
    )

    start_slot = way * (group - 1)
    crossing = jnp.logical_not(has_before) & ((start_slot // local_cols) != (me // local_cols))
    ahead = jnp.where(has_before, group, jnp.where(crossing, group - local_cols + 1, 1))
    turned_by = jnp.where(crossing, local_cols, 0)

    def prepare_ahead(turn, unused):
        return prepare((turn + turned_by) % group, unused)


    @pl.when(has_lower & has_upper)
    def _():
        for way_at in range(2):
            pl.semaphore_wait(token.at[way_at], 1)
            pass_token(way_at)

    def side_copy(step, slot):
        return pltpu.make_async_remote_copy(
            xbuf.at[step],
            env_ref.at[way, 0],
            side_send.at[step],
            env_recv.at[way, 0],
            device_id={"rows": base + slot, "cols": cols_at + onward},
        )

    def absorb(step, unused):
        slot = step + way * (group - 1 - 2 * step)

        @pl.when(opening_chain & (step == local_cols))
        def _():
            start_later_maps()

        pending = (step >= 1) & jnp.logical_not(crossing & (step >= local_cols))

        @pl.when(pending & jnp.logical_not(has_before))
        def _():
            prepare(step, 0)

        send_row(
            xbuf.at[step],
            env_ref.at[way, spot_of(column)],
            env_send.at[step],
            env_recv.at[way, spot_of(column)],
            slot,
        )

        @pl.when(has_next & (column == edge_col))
        def _():
            side_copy(step, slot).start()

        renewed = normalized(absorbed(step))
        xbuf[step + 1] = renewed
        put_right(renewed)

        @pl.when((step == group - 1) & has_after)
        def _():
            chain_hop.start()

        return unused

    def run_chain():
        lax.fori_loop(0, ahead, prepare_ahead, 0)

        @pl.when(has_before)
        def _():
            pltpu.make_async_copy(xbuf.at[0], xbuf.at[0], chain_recv).wait()

        @pl.when(jnp.logical_not(has_before) & (way == 0))
        def _():
            xbuf[0] = edges[0, column]

        @pl.when(jnp.logical_not(has_before) & (way == 1))
        def _():
            xbuf[0] = edges[1, column]

        put_right(xbuf[0])
        lax.fori_loop(0, group, absorb, 0)

        for step in range(group):
            send_row(
                xbuf.at[step + 1],
                out_ref.at[way, column],
                out_send.at[step],
                out_recv.at[way, column],
                step + way * (group - 1 - 2 * step),
            )

    unit = jnp.where(
        lax.broadcasted_iota(jnp.int32, (LANES, LANES), 0)
        == lax.broadcasted_iota(jnp.int32, (LANES, LANES), 1),
        1.0,
        0.0,
    ).astype(jnp.bfloat16)
    fill = jnp.zeros((LANES - chi, LANES), jnp.bfloat16)

    def take_blocks(kind, at):
        landed = env_ref.at[kind, at]
        pltpu.make_async_copy(landed, landed, env_recv.at[kind, at]).wait()
        blocks = unpack_lanes(load_tiles(env_ref.at[kind], at, width), chi)
        for d, block in enumerate(blocks):
            lanes = slice(d * LANES, (d + 1) * LANES)
            for part, values in enumerate(halves(block)):
                tall_block = jnp.concatenate([values, fill], axis=0)
                turned = dot_last(unit, tall_block).astype(jnp.bfloat16)
                yield lanes, part, values, tall_block, turned

    def take_far(at):
        for lanes, part, values, tall_block, turned in take_blocks(early, at):
            far[1, at, part, :, lanes] = turned
            far[0, at, part, :, lanes] = tall_block

    def take_near(at):
        for lanes, part, values, tall_block, turned in take_blocks(late, at):
            rows = slice(part * chi, (part + 1) * chi)
            near[0, at, rows, lanes] = turned[:chi]
            near[1, at, rows, lanes] = values

    second = jnp.where(rank >= col_count // 2, 1, 0)

    def hop(side):
        return pltpu.make_async_remote_copy(
            hop_out.at[side],
            hop_in.at[side],
            hop_send.at[side],
            hop_recv.at[side],
            device_id={"cols": cols_at + onward * (1 - 2 * side)},
        )

    def put_environ(blocks):
        for at, block in enumerate(blocks):
            vbuf[at * chi : (at + 1) * chi] = block

    def put_edge(side):
        blocks = unpack_lanes(load_tiles(sides, true_side(side), width), chi)

        @pl.when(late == 0)
        def _():
            put_environ(blocks)

        @pl.when(late == 1)
        def _():
            empty = jnp.zeros((LANES - chi, LANES), jnp.float32)
            put_environ([jnp.concatenate([block, empty], axis=0).T[:chi] for block in blocks])

    def place_of(side, order):
        return order + side * (local_cols - 2 * order)

    def open_up(side, at_column):
        v_high, v_low = halves(vbuf[...])
        true = true_side(side)
        f_high = far[true, at_column, 0]
        jbuf[...] = dot32(v_high, f_high) + (
            dot32(v_high, far[true, at_column, 1]) + dot32(v_low, f_high)
        )
        chunk = 16

        def ket(p, u, i, d, o):
            at = p * 16 + u * 8 + i * 4 + d * 2 + o
            return kets_near[at_column, true, at : at + 1, :]

        def through(at, unused):
            start = pl.multiple_of(at * chunk, chunk)

            def joined(i, d):
                return jbuf[pl.ds(i * chi + start, chunk), d * LANES : (d + 1) * LANES]

            for p in range(PHYS):
                for u in range(D):
                    for o in range(D):
                        part = {}
                        for i2 in range(D):
                            for d2 in range(D):
                                total = None
                                for i in range(D):
                                    for d in range(D):
                                        term = ket(p, u, i, d, o) * joined(
                                            i * D + i2, d * D + d2
                                        )
                                        total = term if total is None else total + term
                                part[i2, d2] = total
                        for q in range(PHYS):
                            for u2 in range(D):
                                for o2 in range(D):
                                    total = None
                                    for i2 in range(D):
                                        for d2 in range(D):
                                            term = ket(q, u2, i2, d2, o2) * part[i2, d2]
                                            total = term if total is None else total + term
                                    high, low = halves(total)
                                    rows = pl.ds((u * D + u2) * LANES + start, chunk)
                                    spot = (p * PHYS + q) * D2 + o * D + o2
                                    lanes = slice(spot * LANES, (spot + 1) * LANES)
                                    thi[rows, lanes] = high
                                    tlo[rows, lanes] = low
            return unused

        lax.fori_loop(0, chi // chunk, through, 0)

    def first_order(side):
        return jnp.where((side == 0) & (rank == 0), 1, 0)

    def is_edge(side):
        return ((side == 0) & (rank == 0)) | ((side == 1) & (rank == col_count - 1))

    def early_work():
        @pl.when(has_prev)
        def _():
            pltpu.make_async_copy(kets_near.at[0], kets_near.at[0], ket_recv).wait()

        for at in range(1, local_cols + 1):
            take_far(at)

        @pl.when(has_prev)
        def _():
            take_far(0)

        for side in range(2):

            @pl.when(is_edge(side))
            def _():
                put_edge(side)

        @pl.when(is_edge(second))
        def _():
            open_up(second, place_of(second, first_order(second)))

    early_first = (way != low_half) & (mine != groups // 2) & (mine != groups // 2 - 1)
    early_at = jnp.where(early_first, 0, 1)

    def phase(at, unused):
        @pl.when(at == early_at)
        def _():
            early_work()

        @pl.when(at != early_at)
        def _():
            run_chain()

        return unused

    lax.fori_loop(0, 2, phase, 0)
    for at in range(1, local_cols + 1):
        take_near(at)

    spot_row = lax.broadcasted_iota(jnp.int32, (terms, terms), 0)
    spot_lane = lax.broadcasted_iota(jnp.int32, (terms, terms), 1)

    def stand(ref):
        values = jnp.broadcast_to(ref[...].astype(jnp.float32), (terms, terms))
        return jnp.sum(jnp.where(spot_row == spot_lane, values, 0.0), axis=1, keepdims=True)

    term_row = stand(rows_ref).astype(jnp.int32)
    term_bond = stand(bonds_ref).astype(jnp.int32)
    term_op = stand(ops_ref).astype(jnp.int32)
    term_weights = jnp.zeros((terms, table_ref.shape[1]), jnp.float32)
    for op in range(table_ref.shape[0]):
        term_weights = jnp.where(term_op == op, table_ref[op : op + 1, :], term_weights)

    def walk(turn, unused):
        side = (turn // local_cols + second) % 2
        order = turn % local_cols
        at_column = place_of(side, order)
        absent = (rank == 0) & (at_column == side)
        opening = order == first_order(side)
        ending = order == local_cols - 1

        @pl.when((order == 0) & jnp.logical_not(is_edge(side)))
        def _():
            pltpu.make_async_copy(hop_in.at[side], hop_in.at[side], hop_recv.at[side]).wait()
            put_environ(unpack_lanes(load_tiles(hop_in, side, width), chi))

        @pl.when(jnp.logical_not(absent) & jnp.logical_not(opening & is_edge(side)))
        def _():
            open_up(side, at_column)

        @pl.when(jnp.logical_not(absent) & (at_column == 0))
        def _():
            take_near(0)

        @pl.when(jnp.logical_not(absent))
        def _():
            both = near[true_side(side), at_column]
            closed = None
            for pair in range(pairs):
                lanes = slice(pair * wide, (pair + 1) * wide)
                large = dot32(both, thi[:, lanes])
                value = large[:chi] + (large[chi:] + dot32(both[:chi], tlo[:, lanes]))
                opens[true_side(side), at_column - side, pair] = value
                if pair // PHYS == pair % PHYS:
                    closed = value if closed is None else closed + value
            square = jnp.sum(
                jnp.sum(closed * closed, axis=1, keepdims=True), axis=0, keepdims=True
            )
            closed = closed * (1.0 / jnp.sqrt(square / (chi * width) + EPSILON))
            blocks = [closed[:, d * LANES : (d + 1) * LANES] for d in range(D2)]
            put_environ(blocks)

            @pl.when(ending)
            def _():
                for t, tile in enumerate(pack_lanes(blocks, chi)):
                    hop_out[side, :, t * LANES : (t + 1) * LANES] = tile

        @pl.when(ending & (side == 0) & has_next)
        def _():
            hop(0).start()

        @pl.when(ending & (side == 1) & has_prev)
        def _():
            hop(1).start()

        return unused

    lax.fori_loop(0, 2 * local_cols, walk, 0)

    tall = (terms, LANES)
    lane = lax.broadcasted_iota(jnp.int32, tall, 1)
    held = shared.at[0]
    held[...] = jnp.zeros(tall, jnp.float32)
    here = jnp.zeros((terms, 1), jnp.int32)
    for k in range(local_cols):
        bond = cols_at * local_cols + k - 1 + late * (local_cols - 2 * k)
        hit = (term_row == place) & (term_bond == bond)
        here = jnp.where(hit, 1, here)

        def add_bond(k=k, hit=hit):
            values = jnp.zeros(tall, jnp.float32)
            for p in range(pairs):
                former = opens[0, k, p]
                for q in range(pairs):
                    value = jnp.sum(
                        jnp.sum(former * opens[1, k, q], axis=0, keepdims=True),
                        axis=1,
                        keepdims=True,
                    )
                    values = jnp.where(lane == p * pairs + q, value, values)
            held[...] += jnp.where(hit, values, 0.0)

        if k:
            add_bond()
        else:
            pl.when(has_prev)(add_bond)

    total = held[...]
    picked = jnp.sum(total[:, : pairs * pairs] * term_weights, axis=1, keepdims=True)
    bra, ket_at = lane % pairs, lane // pairs
    diagonal = (bra // PHYS == bra % PHYS) & (ket_at // PHYS == ket_at % PHYS)
    trace = jnp.sum(
        jnp.where(diagonal & (lane < pairs * pairs), total, 0.0), axis=1, keepdims=True
    )
    size = jnp.sqrt(jnp.sum(total * total, axis=1, keepdims=True))
    energy = picked / jnp.maximum(jnp.abs(trace), 0.25 * size)
    same = lax.broadcasted_iota(jnp.int32, tall, 0) == lane
    devices = row_count * col_count
    spot_mine = place * col_count + cols_at
    own = share.at[devices]
    own[...] = jnp.sum(jnp.where(same & (here == 1), energy, 0.0), axis=0, keepdims=True)

    @pl.when(has_lower & jnp.logical_not(has_upper))
    def _():
        pl.semaphore_wait(token.at[0], 1)

    @pl.when(has_upper & jnp.logical_not(has_lower))
    def _():
        pl.semaphore_wait(token.at[1], 1)

    def tell(turn, unused):
        row = turn + late * (row_count - 1 - 2 * turn)
        for col in range(col_count):

            @pl.when((row != place) | (col != cols_at))
            def _():
                pltpu.make_async_remote_copy(
                    own,
                    share.at[spot_mine],
                    share_send,
                    share_recv,
                    device_id={"rows": row, "cols": col},
                ).start()

        return unused

    lax.fori_loop(0, row_count, tell, 0)
    pltpu.make_async_copy(own, share.at[spot_mine], share_recv).start()
    everyone = share.at[pl.ds(0, devices)]
    pltpu.make_async_copy(everyone, everyone, share_recv).wait()
    energy_ref[...] = jnp.sum(share[:devices], axis=0)[:, :terms]
    others = share.at[pl.ds(0, devices - 1)]
    pltpu.make_async_copy(others, others, share_send).wait()

    @pl.when(has_next)
    def _():
        hop(0).wait_send()
        ket_copy.wait_send()

    @pl.when(has_prev)
    def _():
        hop(1).wait_send()

    for step in range(group):
        slot = step + way * (group - 1 - 2 * step)

        @pl.when(slot != me)
        def _():
            row_copy(
                xbuf.at[step],
                env_ref.at[way, spot_of(column)],
                env_send.at[step],
                env_recv.at[way, spot_of(column)],
                slot,
            )[0].wait_send()
            row_copy(
                xbuf.at[step + 1],
                out_ref.at[way, column],
                out_send.at[step],
                out_recv.at[way, column],
                slot,
            )[0].wait_send()

        @pl.when(has_next & (column == edge_col))
        def _():
            side_copy(step, slot).wait_send()

    @pl.when(opening_chain)
    def _():
        each_map(low_half, True, finish)

    each_map(low_half, False, finish)
    for cross in (True, False):
        each_map(late, cross, finish)

    @pl.when(has_after)
    def _():
        chain_hop.wait_send()

    for a in range(2):
        for b in range(local_cols):
            pltpu.make_async_copy(out_ref.at[a, b], out_ref.at[a, b], out_recv.at[a, b]).wait()


def window(row_count, col_count, args):
    local_cols = args[0].shape[1]
    chi, width = args[1].shape[-2:]
    terms = args[7].shape[0]
    group = 2 * local_cols
    wide = D2 * LANES
    pairs = PHYS * PHYS
    entries = args[0].shape[2]
    vmem = pl.BlockSpec(memory_space=pltpu.VMEM)
    stay = pl.BlockSpec(memory_space=pltpu.HBM)
    dma = pltpu.SemaphoreType.DMA

    def f32(*shape):
        return pltpu.VMEM(shape, jnp.float32)

    def bf16(*shape):
        return pltpu.VMEM(shape, jnp.bfloat16)

    return pl.pallas_call(
        functools.partial(window_kernel, row_count, col_count),
        out_shape=(
            jax.ShapeDtypeStruct((2, local_cols, chi, width), jnp.float32),
            jax.ShapeDtypeStruct((1, terms), jnp.float32),
        ),
        in_specs=[vmem] + [stay] * 6 + [vmem] * 4,
        out_specs=(stay, vmem),
        scratch_shapes=[
            f32(2, local_cols, entries, LANES),
            f32(local_cols + 1, 2, entries, LANES),
            f32(2, 2, local_cols, chi, width),
            f32(2, local_cols, chi, width),
            f32(2, chi, width),
            f32(2, local_cols + 1, chi, width),
            f32(group, chi, width),
            f32(group, chi, width),
            f32(group, entries, LANES),
            f32(group + 1, chi, width),
            f32(D2**3, width),
            bf16(width, wide),
            bf16(width, width),
            bf16(group, 2, width, LANES),
            f32(width, width),
            bf16(group, D2 * width, 2 * width),
            bf16(2 * LANES, width),
            f32(D2 * chi, wide),
            bf16(wide, pairs * wide),
            bf16(wide, pairs * wide),
            bf16(2, local_cols + 1, 2 * chi, wide),
            bf16(2, local_cols + 1, 2, LANES, wide),
            f32(D2 * chi, LANES),
            f32(2, local_cols, pairs, chi, wide),
            f32(2, chi, width),
            f32(2, chi, width),
            f32(row_count * col_count + 1, 1, LANES),
            f32(1, terms, LANES),
            pltpu.SemaphoreType.REGULAR((2,)),
            dma((6,)),
            dma((3, group)),
            dma((3, group)),
            dma((group,)),
            dma((group,)),
            dma((2, local_cols + 1)),
            dma((group,)),
            dma((2, local_cols)),
            dma,
            dma,
            dma((2,)),
            dma((2,)),
            dma,
            dma,
            dma,
            dma,
        ],
        compiler_params=pltpu.CompilerParams(
            collective_id=0, has_side_effects=True, vmem_limit_bytes=56 * 1024 * 1024
        ),
        name="window",
    )(*args[:7], *(index[None] for index in args[7:10]), args[10])


def shards(*args):
    outs, energies = window(lax.axis_size("rows"), lax.axis_size("cols"), args)
    return (outs[0][None], outs[1][None], energies[0])


def solution(mesh):
    placed = (
        P("rows", "cols", None),
        P(None, "rows", "cols", None, None),
        P(None, "rows", "cols", None, None),
        P("cols", None, None),
        P("cols", None, None),
        P("rows", None, None),
        P("rows", None, None),
        P(),
        P(),
        P(),
        P(),
    )
    return jax.shard_map(
        shards,
        mesh=mesh,
        in_specs=placed,
        out_specs=(P("rows", "cols", None, None), P("rows", "cols", None, None), P()),
        check_vma=False,
    )
```

```python
import functools

import jax
import jax.numpy as jnp
from jax import lax
from jax.experimental import pallas as pl
from jax.experimental.pallas import tpu as pltpu
from jax.sharding import PartitionSpec as P

D = 2
D2 = 4
PHYS = 2
EPSILON = 1e-06
LANES = 128
PACE = 9


def unpack_lanes(tiles, chi):
    rolled = {}
    lane = lax.broadcasted_iota(jnp.int32, tiles[0].shape, 1)
    blocks = []
    for block in range(D2):
        total = jnp.zeros_like(tiles[0])
        for place, tile in enumerate(tiles):
            low = max(chi * block, LANES * place)
            high = min(chi * (block + 1), LANES * (place + 1))
            if low >= high:
                continue
            shift = (LANES * place - chi * block) % LANES
            if (place, shift) not in rolled:
                rolled[place, shift] = tile if shift == 0 else pltpu.roll(tile, shift, 1)
            inside = (lane >= low - chi * block) & (lane < high - chi * block)
            total = jnp.where(inside, rolled[place, shift], total)
        blocks.append(total)
    return blocks


def pack_lanes(blocks, chi):
    lane = lax.broadcasted_iota(jnp.int32, blocks[0].shape, 1)
    rolled = {}
    tiles = []
    for place in range(chi * D2 // LANES):
        total = jnp.zeros_like(blocks[0])
        for block, values in enumerate(blocks):
            low = max(chi * block, LANES * place)
            high = min(chi * (block + 1), LANES * (place + 1))
            if low >= high:
                continue
            shift = (chi * block - LANES * place) % LANES
            if (block, shift) not in rolled:
                rolled[block, shift] = values if shift == 0 else pltpu.roll(values, shift, 1)
            inside = (lane >= low - LANES * place) & (lane < high - LANES * place)
            total = jnp.where(inside, rolled[block, shift], total)
        tiles.append(total)
    return tiles


def halves(values):
    high = values.astype(jnp.bfloat16)
    low = (values - high.astype(jnp.float32)).astype(jnp.bfloat16)
    return high, low


def dot32(former, latter):
    return jnp.dot(former, latter, preferred_element_type=jnp.float32)


def dot_last(former, latter):
    return lax.dot_general(
        former, latter, (((1,), (1,)), ((), ())), preferred_element_type=jnp.float32
    )


def load_tiles(ref, at, width):
    return [ref[at, :, LANES * t : LANES * (t + 1)] for t in range(width // LANES)]


def window_kernel(
    row_count,
    col_count,
    kets_ref,
    left_maps_ref,
    right_maps_ref,
    top_ref,
    bottom_ref,
    left_ref,
    right_ref,
    rows_ref,
    bonds_ref,
    ops_ref,
    table_ref,
    out_ref,
    share,
    kets,
    kets_near,
    maps,
    edges,
    sides,
    env_ref,
    pbuf,
    qbuf,
    kbuf,
    xbuf,
    ebuf,
    pick,
    turn_pick,
    pmap,
    rbuf,
    fold,
    xw,
    jbuf,
    thi,
    tlo,
    near,
    far,
    vbuf,
    opens,
    hop_out,
    hop_in,
    own_share,
    shared,
    token,
    load_sem,
    map_send,
    map_recv,
    env_send,
    side_send,
    env_recv,
    out_send,
    out_recv,
    chain_send,
    chain_recv,
    hop_send,
    hop_recv,
    share_send,
    share_recv,
    ket_send,
    ket_recv,
):
    local_cols = kets.shape[1]
    chi, width = maps.shape[3], maps.shape[4]
    wide = D2 * LANES
    pairs = PHYS * PHYS
    terms = rows_ref.shape[1]
    group = 2 * local_cols
    groups = row_count // group
    place = lax.axis_index("rows")
    cols_at = lax.axis_index("cols")
    mine = place // group
    me = place % group
    column = me // 2
    way = me % 2
    base = mine * group
    before = mine - 1 + 2 * way
    after = mine + 1 - 2 * way
    has_before = (before >= 0) & (before < groups)
    has_after = (after >= 0) & (after < groups)
    low_half = jnp.where(mine >= groups // 2, 1, 0)
    early, late = low_half, 1 - low_half
    onward = 1 - 2 * late
    rank = cols_at + late * (col_count - 1 - 2 * cols_at)
    has_prev = rank > 0
    has_next = rank < col_count - 1
    edge_col = low_half * (local_cols - 1)

    def spot_of(at):
        return at + 1 + late * (local_cols - 1 - 2 * at)

    def true_side(side):
        return side + late * (1 - 2 * side)
    has_lower = mine > 0
    has_upper = mine < groups - 1

    barrier = pltpu.get_barrier_semaphore()
    for at in range(col_count):
        for other in range(group):

            @pl.when((me != other) | (cols_at != at))
            def _():
                pl.semaphore_signal(
                    barrier, inc=1, device_id={"rows": base + other, "cols": at}
                )

    @pl.when(has_lower)
    def _():
        pl.semaphore_signal(barrier, inc=1, device_id={"rows": place - group})

    @pl.when(has_upper)
    def _():
        pl.semaphore_signal(barrier, inc=1, device_id={"rows": place + group})

    loads = [
        pltpu.make_async_copy(source, target, load_sem.at[at])
        for at, (source, target) in enumerate(
            (
                (right_maps_ref.at[:, 0], maps.at[0]),
                (left_maps_ref.at[:, 0], maps.at[1]),
                (top_ref, edges.at[0]),
                (bottom_ref, edges.at[1]),
                (left_ref, sides.at[pl.ds(0, 1)]),
                (right_ref, sides.at[pl.ds(1, 1)]),
            )
        )
    ]
    for load in loads:
        load.start()

    count = kets_ref.shape[2]
    spot = lax.broadcasted_iota(jnp.int32, (count, count), 0)
    from_lane = lax.broadcasted_iota(jnp.int32, (count, count), 1)

    def exchanged(high, low):
        top, bottom = (spot // high) % 2, (spot // low) % 2
        return spot + (bottom - top) * high + (top - bottom) * low

    def led(out, into):
        rest = (spot // 8) % 2 * 16 + (spot // 2) % 2 * 4 + spot % 2
        return rest + spot // 16 * out + (spot // 4) % 2 * into

    for order, ref, target in (
        (led(2, 8), kets, 0),
        (led(8, 2), kets, 1),
        (spot + (exchanged(8, 2) - spot) * late, kets_near, 0),
        (spot + (exchanged(8, 2) - spot) * late + (exchanged(4, 1) - spot), kets_near, 1),
    ):
        for at in range(local_cols):
            values = jnp.broadcast_to(kets_ref[0, at : at + 1, :], (count, count))
            tallest = jnp.sum(
                jnp.where(order == from_lane, values, 0.0), axis=1, keepdims=True
            )
            filled = jnp.broadcast_to(tallest, (count, LANES))
            if ref is kets:
                kets[target, at] = filled
            else:
                kets_near[spot_of(at), target] = filled

    chosen = lax.broadcasted_iota(jnp.int32, (width, wide), 1)
    entry = lax.broadcasted_iota(jnp.int32, (width, wide), 0)
    wanted = (chosen % LANES) * D2 + chosen // LANES
    live = (chosen % LANES) < chi
    pick[...] = jnp.where((wanted == entry) & live, 1.0, 0.0).astype(jnp.bfloat16)
    chosen = lax.broadcasted_iota(jnp.int32, (width, width), 0)
    entry = lax.broadcasted_iota(jnp.int32, (width, width), 1)
    wanted = (chosen % chi) * D2 + chosen // chi
    turn_pick[...] = jnp.where(wanted == entry, 1.0, 0.0).astype(jnp.bfloat16)
    xw[...] = jnp.zeros_like(xw)
    for load in loads:
        load.wait()
    greeted = jnp.where(has_lower, 1, 0) + jnp.where(has_upper, 1, 0)
    pl.semaphore_wait(barrier, group * col_count - 1 + greeted)

    def pass_token(way_at):
        pl.semaphore_signal(
            token.at[way_at], inc=1, device_id={"rows": place + (group, -group)[way_at]}
        )

    @pl.when(has_upper & jnp.logical_not(has_lower))
    def _():
        pass_token(0)

    @pl.when(has_lower & jnp.logical_not(has_upper))
    def _():
        pass_token(1)

    ket_copy = pltpu.make_async_remote_copy(
        kets_near.at[local_cols],
        kets_near.at[0],
        ket_send,
        ket_recv,
        device_id={"cols": cols_at + onward},
    )

    @pl.when(has_next)
    def _():
        ket_copy.start()

    def map_copies(target_way, target_col, target, local):
        made = []
        for kind, (source, buffer) in enumerate(
            ((kets, kbuf), (maps.at[0], qbuf), (maps.at[1], pbuf))
        ):
            origin, landing = source.at[target_way, target_col], buffer.at[me]
            if local:
                made.append(pltpu.make_async_copy(origin, landing, map_recv.at[kind, me]))
            else:
                made.append(
                    pltpu.make_async_remote_copy(
                        origin,
                        landing,
                        map_send.at[kind, target],
                        map_recv.at[kind, me],
                        device_id={"rows": base + target},
                    )
                )
        return made

    def each_map(target_way, cross, act):
        for target_col in range(local_cols):
            target = target_col * 2 + target_way
            wanted = (target_col != column) if cross else (target_col == column)

            @pl.when(wanted & (target != me))
            def _():
                for copy in map_copies(target_way, target_col, target, False):
                    act(copy, False)

            @pl.when(wanted & (target == me))
            def _():
                for copy in map_copies(target_way, target_col, target, True):
                    act(copy, True)

    def start(copy, local):
        copy.start()

    def finish(copy, local):
        if not local:
            copy.wait_send()

    opening_chain = jnp.logical_not(has_before)

    def start_later_maps():
        for cross in (True, False):
            each_map(late, cross, start)

    each_map(low_half, False, start)
    leading = me % 2 == low_half

    @pl.when(leading)
    def _():
        each_map(low_half, True, start)

    def clear(at, unused):
        thi[...] = jnp.zeros_like(thi)
        tlo[...] = jnp.zeros_like(tlo)
        return unused

    lax.fori_loop(0, jnp.where(leading, 1, PACE), clear, 0)

    @pl.when(jnp.logical_not(leading))
    def _():
        each_map(low_half, True, start)

    @pl.when(has_before)
    def _():
        each_map(low_half, True, finish)
        start_later_maps()

    lane_pair = lax.broadcasted_iota(jnp.int32, (count // 2, width), 1) // chi

    def folded_kets(values):
        former, latter = (
            jnp.concatenate([part] * (width // LANES), axis=1)
            for part in (values[: count // 2], values[count // 2 :])
        )
        ket = jnp.where(lane_pair // D == 0, former, latter)
        bra = jnp.where(lane_pair % D == 0, former, latter)
        legs = D**3
        for i in range(legs):
            total = ket[i : i + 1] * bra[:legs]
            for p in range(1, PHYS):
                total += ket[p * legs + i : p * legs + i + 1] * bra[p * legs : (p + 1) * legs]
            ebuf[i * legs : (i + 1) * legs] = total

    def fold_into(target):
        chunk = 16
        full = width // (2 * LANES) * 2 * LANES

        def through(at, unused):
            start = pl.multiple_of(at * chunk, chunk)
            tiles = [rbuf[pl.ds(c * chi + start, chunk), :] for c in range(D2)]
            for g in range(D2):
                for h in range(D2):
                    total = None
                    for c, tile in enumerate(tiles):
                        ket_at = (h // D) * 4 + (g // D) * 2 + c // D
                        bra_at = (h % D) * 4 + (g % D) * 2 + c % D
                        spot = ket_at * D**3 + bra_at
                        term = ebuf[spot : spot + 1, :] * tile
                        total = term if total is None else total + term
                    high, low = halves(total)
                    rows = pl.ds((g * D2 + h) * chi + start, chunk)
                    target[rows, :width] = high
                    target[rows, width : 2 * width - full] = low[:, full:]
                    target[rows, 2 * width - full :] = low[:, :full]
            return unused

        lax.fori_loop(0, chi // chunk, through, 0)

    def put_right(values):
        high, low = halves(values)
        xw[:chi, :width] = high
        xw[LANES : LANES + chi, :width] = high
        xw[:chi, width:] = low

    def joined_with(maps):
        both = dot32(maps, xw[...])
        return both[:, :width] + both[:, width:]

    def absorbed(at_step):
        full = width // (2 * LANES) * 2 * LANES
        part = D2 * chi // 2
        joined = [
            joined_with(pmap[at_step, at : at + part])
            for at in (0, part)
        ]
        total = None
        for at, piece in enumerate(joined):
            rows = [
                jnp.concatenate([half[g * chi : (g + 1) * chi] for g in range(D2 // 2)], axis=1)
                for half in halves(piece)
            ]
            depth = slice(at * D2 // 2 * width, (at + 1) * D2 // 2 * width)
            large = dot32(jnp.concatenate(rows, axis=0), fold[at_step, depth, : 2 * width - full])
            front = large[:chi, :width] + large[chi:, :width]
            rest = large[:chi, width:] + large[chi:, width:]
            small = dot32(rows[0], fold[at_step, depth, 2 * width - full :])
            value = jnp.concatenate([front[:, :full] + small, front[:, full:] + rest], axis=1)
            total = value if total is None else total + value
        return total

    def size_of(values):
        square = jnp.sum(jnp.sum(values * values, axis=1, keepdims=True), axis=0, keepdims=True)
        return square / (chi * width)

    def prepare(step, unused):
        slot = step + way * (group - 1 - 2 * step)
        for kind, buffer in enumerate((kbuf, qbuf, pbuf)):
            pltpu.make_async_copy(
                buffer.at[slot], buffer.at[slot], map_recv.at[kind, slot]
            ).wait()
        folded_kets(kbuf[slot])
        gap = jnp.zeros((LANES - chi, width), jnp.bfloat16)
        high, low = halves(qbuf[slot])
        turned = dot_last(turn_pick[...], jnp.concatenate([high, gap, low, gap], axis=0))
        turned = turned[:, :LANES] + turned[:, LANES:]
        for t, tile in enumerate(pack_lanes([turned] * D2, chi)):
            rbuf[:, t * LANES : (t + 1) * LANES] = tile
        spread_map = dot32(
            jnp.concatenate(halves(pbuf[slot]), axis=0), pick[...]
        ).astype(jnp.bfloat16)
        for at in range(2):
            for l in range(D2):
                lanes = slice(at * LANES, (at + 1) * LANES)
                pmap[step, l * chi : (l + 1) * chi, lanes] = spread_map[
                    at * chi : (at + 1) * chi, l * LANES : (l + 1) * LANES
                ]
        fold_into(fold.at[step])
        return unused

    def row_copy(source, landing, send, recv, slot):
        remote = pltpu.make_async_remote_copy(
            source, landing, send, recv, device_id={"rows": base + slot}
        )
        return remote, pltpu.make_async_copy(source, landing, recv)

    def send_row(source, landing, send, recv, slot):
        remote, local = row_copy(source, landing, send, recv, slot)

        @pl.when(slot != me)
        def _():
            remote.start()

        @pl.when(slot == me)
        def _():
            local.start()

    chain_hop = pltpu.make_async_remote_copy(
        xbuf.at[group],
        xbuf.at[0],
        chain_send,
        chain_recv,
        device_id={"rows": after * group + me},
    )

    start_slot = way * (group - 1)
    crossing = jnp.logical_not(has_before) & ((start_slot // local_cols) != (me // local_cols))
    ahead = jnp.where(has_before, group, jnp.where(crossing, group - local_cols + 1, 1))
    turned_by = jnp.where(crossing, local_cols, 0)

    def prepare_ahead(turn, unused):
        return prepare((turn + turned_by) % group, unused)


    @pl.when(has_lower & has_upper)
    def _():
        for way_at in range(2):
            pl.semaphore_wait(token.at[way_at], 1)
            pass_token(way_at)

    def side_copy(step, slot):
        return pltpu.make_async_remote_copy(
            xbuf.at[step],
            env_ref.at[way, 0],
            side_send.at[step],
            env_recv.at[way, 0],
            device_id={"rows": base + slot, "cols": cols_at + onward},
        )

    def absorb(step, carried):
        known, ratio = carried
        slot = step + way * (group - 1 - 2 * step)

        @pl.when(opening_chain & (step == local_cols))
        def _():
            start_later_maps()

        pending = (step >= 1) & jnp.logical_not(crossing & (step >= local_cols))

        @pl.when(pending & jnp.logical_not(has_before))
        def _():
            prepare(step, 0)

        send_row(
            xbuf.at[step],
            env_ref.at[way, spot_of(column)],
            env_send.at[step],
            env_recv.at[way, spot_of(column)],
            slot,
        )

        @pl.when(has_next & (column == edge_col))
        def _():
            side_copy(step, slot).start()

        renewed = absorbed(step)
        put_right(renewed * known)
        factor = ratio * lax.rsqrt(ratio * ratio * size_of(renewed) + EPSILON)
        xbuf[step + 1] = renewed * factor

        @pl.when((step == group - 1) & has_after)
        def _():
            chain_hop.start()

        return factor, factor / known

    def run_chain():
        lax.fori_loop(0, ahead, prepare_ahead, 0)

        @pl.when(has_before)
        def _():
            pltpu.make_async_copy(xbuf.at[0], xbuf.at[0], chain_recv).wait()

        @pl.when(jnp.logical_not(has_before) & (way == 0))
        def _():
            xbuf[0] = edges[0, column]

        @pl.when(jnp.logical_not(has_before) & (way == 1))
        def _():
            xbuf[0] = edges[1, column]

        put_right(xbuf[0])
        one = jnp.ones((1, 1), jnp.float32)
        lax.fori_loop(0, group, absorb, (one, one))

        for step in range(group):
            send_row(
                xbuf.at[step + 1],
                out_ref.at[way, column],
                out_send.at[step],
                out_recv.at[way, column],
                step + way * (group - 1 - 2 * step),
            )

    unit = jnp.where(
        lax.broadcasted_iota(jnp.int32, (LANES, LANES), 0)
        == lax.broadcasted_iota(jnp.int32, (LANES, LANES), 1),
        1.0,
        0.0,
    ).astype(jnp.bfloat16)
    fill = jnp.zeros((LANES - chi, LANES), jnp.bfloat16)

    def take_blocks(kind, at):
        landed = env_ref.at[kind, at]
        pltpu.make_async_copy(landed, landed, env_recv.at[kind, at]).wait()
        blocks = unpack_lanes(load_tiles(env_ref.at[kind], at, width), chi)
        for d, block in enumerate(blocks):
            lanes = slice(d * LANES, (d + 1) * LANES)
            for part, values in enumerate(halves(block)):
                tall_block = jnp.concatenate([values, fill], axis=0)
                turned = dot_last(unit, tall_block).astype(jnp.bfloat16)
                yield lanes, part, values, tall_block, turned

    def take_far(at):
        for lanes, part, values, tall_block, turned in take_blocks(early, at):
            for copy in (0, 1) if part == 0 else (2,):
                rows = slice(copy * LANES, (copy + 1) * LANES)
                far[1, at, rows, lanes] = turned
                far[0, at, rows, lanes] = tall_block

    def take_near(at):
        for lanes, part, values, tall_block, turned in take_blocks(late, at):
            rows = slice(part * chi, (part + 1) * chi)
            near[0, at, rows, lanes] = turned[:chi]
            near[1, at, rows, lanes] = values

    second = jnp.where(rank >= col_count // 2, 1, 0)

    def hop(side):
        return pltpu.make_async_remote_copy(
            hop_out.at[side],
            hop_in.at[side],
            hop_send.at[side],
            hop_recv.at[side],
            device_id={"cols": cols_at + onward * (1 - 2 * side)},
        )

    def put_environ(blocks):
        for at, block in enumerate(blocks):
            vbuf[at * chi : (at + 1) * chi] = block

    def put_edge(side):
        blocks = unpack_lanes(load_tiles(sides, true_side(side), width), chi)

        @pl.when(late == 0)
        def _():
            put_environ(blocks)

        @pl.when(late == 1)
        def _():
            empty = jnp.zeros((LANES - chi, LANES), jnp.float32)
            put_environ([jnp.concatenate([block, empty], axis=0).T[:chi] for block in blocks])

    def place_of(side, order):
        return order + side * (local_cols - 2 * order)

    def join(side, at_column):
        v_high, v_low = halves(vbuf[...])
        true = true_side(side)
        jbuf[...] = dot32(
            jnp.concatenate([v_high, v_low], axis=1), far[true, at_column, : 2 * LANES]
        ) + dot32(v_high, far[true, at_column, 2 * LANES :])

    chunk = 16

    def pass_through(side, at_column, p, start):
        true = true_side(side)

        def ket(p, u, i, d, o):
            at = p * 16 + u * 8 + i * 4 + d * 2 + o
            return kets_near[at_column, true, at : at + 1, :]

        def joined(i, d):
            return jbuf[pl.ds(i * chi + start, chunk), d * LANES : (d + 1) * LANES]

        for u in range(D):
            for o in range(D):
                part = {}
                for i2 in range(D):
                    for d2 in range(D):
                        total = None
                        for i in range(D):
                            for d in range(D):
                                term = ket(p, u, i, d, o) * joined(i * D + i2, d * D + d2)
                                total = term if total is None else total + term
                        part[i2, d2] = total
                for q in range(PHYS):
                    for u2 in range(D):
                        for o2 in range(D):
                            total = None
                            for i2 in range(D):
                                for d2 in range(D):
                                    term = ket(q, u2, i2, d2, o2) * part[i2, d2]
                                    total = term if total is None else total + term
                            high, low = halves(total)
                            rows = pl.ds((u * D + u2) * LANES + start, chunk)
                            spot = (p * PHYS + q) * D2 + o * D + o2
                            lanes = slice(spot * LANES, (spot + 1) * LANES)
                            thi[rows, lanes] = high
                            tlo[rows, lanes] = low

    def open_up(side, at_column):
        join(side, at_column)

        def through(at, unused):
            for p in range(PHYS):
                pass_through(side, at_column, p, pl.multiple_of(at * chunk, chunk))
            return unused

        lax.fori_loop(0, chi // chunk, through, 0)

    def close(side, at_column, pair):
        both = near[true_side(side), at_column]
        lanes = slice(pair * wide, (pair + 1) * wide)
        large = dot32(both, thi[:, lanes])
        opens[true_side(side), at_column - side, pair] = large[:chi] + (
            large[chi:] + dot32(both[:chi], tlo[:, lanes])
        )

    def first_order(side):
        return jnp.where((side == 0) & (rank == 0), 1, 0)

    def is_edge(side):
        return ((side == 0) & (rank == 0)) | ((side == 1) & (rank == col_count - 1))

    def early_work():
        @pl.when(has_prev)
        def _():
            pltpu.make_async_copy(kets_near.at[0], kets_near.at[0], ket_recv).wait()

        for at in range(1, local_cols + 1):
            take_far(at)

        @pl.when(has_prev)
        def _():
            take_far(0)

        for side in range(2):

            @pl.when(is_edge(side))
            def _():
                put_edge(side)

        @pl.when(is_edge(second))
        def _():
            open_up(second, place_of(second, first_order(second)))

    early_first = (way != low_half) & (mine != groups // 2) & (mine != groups // 2 - 1)
    early_at = jnp.where(early_first, 0, 1)

    def phase(at, unused):
        @pl.when(at == early_at)
        def _():
            early_work()

        @pl.when(at != early_at)
        def _():
            run_chain()

        return unused

    lax.fori_loop(0, 2, phase, 0)
    for at in range(1, local_cols + 1):
        take_near(at)

    spot_row = lax.broadcasted_iota(jnp.int32, (terms, terms), 0)
    spot_lane = lax.broadcasted_iota(jnp.int32, (terms, terms), 1)

    def stand(ref):
        values = jnp.broadcast_to(ref[...].astype(jnp.float32), (terms, terms))
        return jnp.sum(jnp.where(spot_row == spot_lane, values, 0.0), axis=1, keepdims=True)

    term_row = stand(rows_ref).astype(jnp.int32)
    term_bond = stand(bonds_ref).astype(jnp.int32)
    term_op = stand(ops_ref).astype(jnp.int32)
    term_weights = jnp.zeros((terms, table_ref.shape[1]), jnp.float32)
    for op in range(table_ref.shape[0]):
        term_weights = jnp.where(term_op == op, table_ref[op : op + 1, :], term_weights)

    def walk(turn, unused):
        side = (turn // local_cols + second) % 2
        order = turn % local_cols
        at_column = place_of(side, order)
        absent = (rank == 0) & (at_column == side)
        opening = order == first_order(side)
        ending = order == local_cols - 1

        @pl.when((order == 0) & jnp.logical_not(is_edge(side)))
        def _():
            pltpu.make_async_copy(hop_in.at[side], hop_in.at[side], hop_recv.at[side]).wait()
            put_environ(unpack_lanes(load_tiles(hop_in, side, width), chi))

        @pl.when(jnp.logical_not(absent) & (at_column == 0))
        def _():
            take_near(0)

        @pl.when(jnp.logical_not(absent) & opening & is_edge(side))
        def _():
            for pair in range(pairs):
                close(side, at_column, pair)

        @pl.when(jnp.logical_not(absent) & jnp.logical_not(opening & is_edge(side)))
        def _():
            join(side, at_column)
            for p in range(PHYS):
                for start in range(0, chi, chunk):
                    pass_through(side, at_column, p, start)
                for q in range(PHYS):
                    close(side, at_column, p * PHYS + q)

        @pl.when(jnp.logical_not(absent))
        def _():
            closed = opens[true_side(side), at_column - side, 0]
            for p in range(1, PHYS):
                closed += opens[true_side(side), at_column - side, p * PHYS + p]
            square = jnp.sum(
                jnp.sum(closed * closed, axis=1, keepdims=True), axis=0, keepdims=True
            )
            closed = closed * (1.0 / jnp.sqrt(square / (chi * width) + EPSILON))
            blocks = [closed[:, d * LANES : (d + 1) * LANES] for d in range(D2)]
            put_environ(blocks)

            @pl.when(ending)
            def _():
                for t, tile in enumerate(pack_lanes(blocks, chi)):
                    hop_out[side, :, t * LANES : (t + 1) * LANES] = tile

        @pl.when(ending & (side == 0) & has_next)
        def _():
            hop(0).start()

        @pl.when(ending & (side == 1) & has_prev)
        def _():
            hop(1).start()

        return unused

    lax.fori_loop(0, 2 * local_cols, walk, 0)

    tall = (terms, LANES)
    lane = lax.broadcasted_iota(jnp.int32, tall, 1)
    held = shared.at[0]
    held[...] = jnp.zeros(tall, jnp.float32)
    here = jnp.zeros((terms, 1), jnp.int32)
    for k in range(local_cols):
        bond = cols_at * local_cols + k - 1 + late * (local_cols - 2 * k)
        hit = (term_row == place) & (term_bond == bond)
        here = jnp.where(hit, 1, here)

        def add_bond(k=k, hit=hit):
            values = jnp.zeros(tall, jnp.float32)
            for p in range(pairs):
                former = opens[0, k, p]
                for q in range(pairs):
                    value = jnp.sum(
                        jnp.sum(former * opens[1, k, q], axis=0, keepdims=True),
                        axis=1,
                        keepdims=True,
                    )
                    values = jnp.where(lane == p * pairs + q, value, values)
            held[...] += jnp.where(hit, values, 0.0)

        if k:
            add_bond()
        else:
            pl.when(has_prev)(add_bond)

    total = held[...]
    picked = jnp.sum(total[:, : pairs * pairs] * term_weights, axis=1, keepdims=True)
    bra, ket_at = lane % pairs, lane // pairs
    diagonal = (bra // PHYS == bra % PHYS) & (ket_at // PHYS == ket_at % PHYS)
    trace = jnp.sum(
        jnp.where(diagonal & (lane < pairs * pairs), total, 0.0), axis=1, keepdims=True
    )
    size = jnp.sqrt(jnp.sum(total * total, axis=1, keepdims=True))
    energy = picked / jnp.maximum(jnp.abs(trace), 0.25 * size)
    same = lax.broadcasted_iota(jnp.int32, tall, 0) == lane
    devices = row_count * col_count
    spot_mine = place * col_count + cols_at
    own = own_share.at[0]
    own[...] = jnp.sum(jnp.where(same & (here == 1), energy, 0.0), axis=0, keepdims=True)

    @pl.when(has_lower & jnp.logical_not(has_upper))
    def _():
        pl.semaphore_wait(token.at[0], 1)

    @pl.when(has_upper & jnp.logical_not(has_lower))
    def _():
        pl.semaphore_wait(token.at[1], 1)

    def tell(turn, unused):
        row = turn + late * (row_count - 1 - 2 * turn)
        for col in range(col_count):

            @pl.when((row != place) | (col != cols_at))
            def _():
                pltpu.make_async_remote_copy(
                    own,
                    share.at[spot_mine],
                    share_send,
                    share_recv,
                    device_id={"rows": row, "cols": col},
                ).start()

        return unused

    lax.fori_loop(0, row_count, tell, 0)
    pltpu.make_async_copy(own, share.at[spot_mine], share_recv).start()
    pltpu.make_async_copy(share, share, share_recv).wait()
    others = share.at[pl.ds(0, devices - 1)]
    pltpu.make_async_copy(others, others, share_send).wait()

    @pl.when(has_next)
    def _():
        hop(0).wait_send()
        ket_copy.wait_send()

    @pl.when(has_prev)
    def _():
        hop(1).wait_send()

    for step in range(group):
        slot = step + way * (group - 1 - 2 * step)

        @pl.when(slot != me)
        def _():
            row_copy(
                xbuf.at[step],
                env_ref.at[way, spot_of(column)],
                env_send.at[step],
                env_recv.at[way, spot_of(column)],
                slot,
            )[0].wait_send()
            row_copy(
                xbuf.at[step + 1],
                out_ref.at[way, column],
                out_send.at[step],
                out_recv.at[way, column],
                slot,
            )[0].wait_send()

        @pl.when(has_next & (column == edge_col))
        def _():
            side_copy(step, slot).wait_send()

    @pl.when(opening_chain)
    def _():
        each_map(low_half, True, finish)

    each_map(low_half, False, finish)
    for cross in (True, False):
        each_map(late, cross, finish)

    @pl.when(has_after)
    def _():
        chain_hop.wait_send()

    for a in range(2):
        for b in range(local_cols):
            pltpu.make_async_copy(out_ref.at[a, b], out_ref.at[a, b], out_recv.at[a, b]).wait()


def window(row_count, col_count, args):
    local_cols = args[0].shape[1]
    chi, width = args[1].shape[-2:]
    terms = args[7].shape[0]
    group = 2 * local_cols
    wide = D2 * LANES
    pairs = PHYS * PHYS
    entries = args[0].shape[2]
    vmem = pl.BlockSpec(memory_space=pltpu.VMEM)
    stay = pl.BlockSpec(memory_space=pltpu.HBM)
    dma = pltpu.SemaphoreType.DMA

    def f32(*shape):
        return pltpu.VMEM(shape, jnp.float32)

    def bf16(*shape):
        return pltpu.VMEM(shape, jnp.bfloat16)

    return pl.pallas_call(
        functools.partial(window_kernel, row_count, col_count),
        out_shape=(
            jax.ShapeDtypeStruct((2, local_cols, chi, width), jnp.float32),
            jax.ShapeDtypeStruct((row_count * col_count, 1, LANES), jnp.float32),
        ),
        in_specs=[vmem] + [stay] * 6 + [vmem] * 4,
        out_specs=(stay, stay),
        scratch_shapes=[
            f32(2, local_cols, entries, LANES),
            f32(local_cols + 1, 2, entries, LANES),
            f32(2, 2, local_cols, chi, width),
            f32(2, local_cols, chi, width),
            f32(2, chi, width),
            f32(2, local_cols + 1, chi, width),
            f32(group, chi, width),
            f32(group, chi, width),
            f32(group, entries, LANES),
            f32(group + 1, chi, width),
            f32(D2**3, width),
            bf16(width, wide),
            bf16(width, width),
            bf16(group, width, 2 * LANES),
            f32(width, width),
            bf16(group, D2 * width, 2 * width),
            bf16(2 * LANES, 2 * width),
            f32(D2 * chi, wide),
            bf16(wide, pairs * wide),
            bf16(wide, pairs * wide),
            bf16(2, local_cols + 1, 2 * chi, wide),
            bf16(2, local_cols + 1, 3 * LANES, wide),
            f32(D2 * chi, LANES),
            f32(2, local_cols, pairs, chi, wide),
            f32(2, chi, width),
            f32(2, chi, width),
            f32(1, 1, LANES),
            f32(1, terms, LANES),
            pltpu.SemaphoreType.REGULAR((2,)),
            dma((6,)),
            dma((3, group)),
            dma((3, group)),
            dma((group,)),
            dma((group,)),
            dma((2, local_cols + 1)),
            dma((group,)),
            dma((2, local_cols)),
            dma,
            dma,
            dma((2,)),
            dma((2,)),
            dma,
            dma,
            dma,
            dma,
        ],
        compiler_params=pltpu.CompilerParams(
            collective_id=0, has_side_effects=True, vmem_limit_bytes=56 * 1024 * 1024
        ),
        name="window",
    )(*args[:7], *(index[None] for index in args[7:10]), args[10])


def settle_kernel(
    outs_ref, share_ref, top_ref, bottom_ref, energies_ref, held, shares, line, sem
):
    gather = pltpu.make_async_copy(share_ref, shares, sem.at[0, 0])
    gather.start()
    parts = [
        (outs_ref.at[way, at], held.at[way, at], (top_ref, bottom_ref)[way].at[0, at])
        for way in range(2)
        for at in range(held.shape[1])
    ]
    for at, (source, middle, target) in enumerate(parts):
        pltpu.make_async_copy(source, middle, sem.at[0, at + 1]).start()
    gather.wait()
    line[...] = jnp.sum(shares[...], axis=0)[:, : line.shape[1]]
    put = pltpu.make_async_copy(line, energies_ref, sem.at[1, 0])
    put.start()
    for at, (source, middle, target) in enumerate(parts):
        pltpu.make_async_copy(source, middle, sem.at[0, at + 1]).wait()
        pltpu.make_async_copy(middle, target, sem.at[1, at + 1]).start()
    for at, (source, middle, target) in enumerate(parts):
        pltpu.make_async_copy(middle, target, sem.at[1, at + 1]).wait()
    put.wait()


def settle(outs, shares, terms):
    stay = pl.BlockSpec(memory_space=pltpu.HBM)
    half = jax.ShapeDtypeStruct((1,) + outs.shape[1:], outs.dtype)
    count = outs.shape[0] * outs.shape[1] + 1
    return pl.pallas_call(
        settle_kernel,
        out_shape=(half, half, jax.ShapeDtypeStruct((1, terms), shares.dtype)),
        in_specs=[stay] * 2,
        out_specs=(stay,) * 3,
        scratch_shapes=[
            pltpu.VMEM(outs.shape, outs.dtype),
            pltpu.VMEM(shares.shape, shares.dtype),
            pltpu.VMEM((1, terms), shares.dtype),
            pltpu.SemaphoreType.DMA((2, count)),
        ],
        name="settle",
    )(outs, shares)


def shards(*args):
    outs, shares = window(lax.axis_size("rows"), lax.axis_size("cols"), args)
    top, bottom, energies = settle(outs, shares, args[7].shape[0])
    return (top, bottom, energies[0])


def solution(mesh):
    placed = (
        P("rows", "cols", None),
        P(None, "rows", "cols", None, None),
        P(None, "rows", "cols", None, None),
        P("cols", None, None),
        P("cols", None, None),
        P("rows", None, None),
        P("rows", None, None),
        P(),
        P(),
        P(),
        P(),
    )
    return jax.shard_map(
        shards,
        mesh=mesh,
        in_specs=placed,
        out_specs=(P("rows", "cols", None, None), P("rows", "cols", None, None), P()),
        check_vma=False,
    )
```

```python
import functools

import jax
import jax.numpy as jnp
from jax import lax
from jax.experimental import pallas as pl
from jax.experimental.pallas import tpu as pltpu
from jax.sharding import PartitionSpec as P

D = 2
D2 = 4
PHYS = 2
EPSILON = 1e-06
LANES = 128
PACE = 9


def unpack_lanes(tiles, chi):
    rolled = {}
    lane = lax.broadcasted_iota(jnp.int32, tiles[0].shape, 1)
    blocks = []
    for block in range(D2):
        total = jnp.zeros_like(tiles[0])
        for place, tile in enumerate(tiles):
            low = max(chi * block, LANES * place)
            high = min(chi * (block + 1), LANES * (place + 1))
            if low >= high:
                continue
            shift = (LANES * place - chi * block) % LANES
            if (place, shift) not in rolled:
                rolled[place, shift] = tile if shift == 0 else pltpu.roll(tile, shift, 1)
            inside = (lane >= low - chi * block) & (lane < high - chi * block)
            total = jnp.where(inside, rolled[place, shift], total)
        blocks.append(total)
    return blocks


def pack_lanes(blocks, chi):
    lane = lax.broadcasted_iota(jnp.int32, blocks[0].shape, 1)
    rolled = {}
    tiles = []
    for place in range(chi * D2 // LANES):
        total = jnp.zeros_like(blocks[0])
        for block, values in enumerate(blocks):
            low = max(chi * block, LANES * place)
            high = min(chi * (block + 1), LANES * (place + 1))
            if low >= high:
                continue
            shift = (chi * block - LANES * place) % LANES
            if (block, shift) not in rolled:
                rolled[block, shift] = values if shift == 0 else pltpu.roll(values, shift, 1)
            inside = (lane >= low - LANES * place) & (lane < high - LANES * place)
            total = jnp.where(inside, rolled[block, shift], total)
        tiles.append(total)
    return tiles


def halves(values):
    high = values.astype(jnp.bfloat16)
    low = (values - high.astype(jnp.float32)).astype(jnp.bfloat16)
    return high, low


def dot32(former, latter):
    return jnp.dot(former, latter, preferred_element_type=jnp.float32)


def dot_last(former, latter):
    return lax.dot_general(
        former, latter, (((1,), (1,)), ((), ())), preferred_element_type=jnp.float32
    )


def load_tiles(ref, at, width):
    return [ref[at, :, LANES * t : LANES * (t + 1)] for t in range(width // LANES)]


def window_kernel(
    row_count,
    col_count,
    kets_ref,
    left_maps_ref,
    right_maps_ref,
    top_ref,
    bottom_ref,
    left_ref,
    right_ref,
    rows_ref,
    bonds_ref,
    ops_ref,
    table_ref,
    out_ref,
    share,
    kets,
    kets_near,
    maps,
    edges,
    sides,
    env_ref,
    pbuf,
    qbuf,
    kbuf,
    xbuf,
    ebuf,
    pick,
    turn_pick,
    pmap,
    rbuf,
    fold,
    xw,
    jbuf,
    thi,
    tlo,
    near,
    far,
    vbuf,
    opens,
    hop_out,
    hop_in,
    own_share,
    shared,
    token,
    load_sem,
    map_send,
    map_recv,
    env_send,
    side_send,
    env_recv,
    out_send,
    out_recv,
    chain_send,
    chain_recv,
    hop_send,
    hop_recv,
    share_send,
    share_recv,
    ket_send,
    ket_recv,
):
    local_cols = kets.shape[1]
    chi, width = maps.shape[3], maps.shape[4]
    wide = D2 * LANES
    pairs = PHYS * PHYS
    terms = rows_ref.shape[1]
    group = 2 * local_cols
    groups = row_count // group
    place = lax.axis_index("rows")
    cols_at = lax.axis_index("cols")
    mine = place // group
    me = place % group
    column = me // 2
    way = me % 2
    base = mine * group
    before = mine - 1 + 2 * way
    after = mine + 1 - 2 * way
    has_before = (before >= 0) & (before < groups)
    has_after = (after >= 0) & (after < groups)
    low_half = jnp.where(mine >= groups // 2, 1, 0)
    early, late = low_half, 1 - low_half
    onward = 1 - 2 * late
    rank = cols_at + late * (col_count - 1 - 2 * cols_at)
    has_prev = rank > 0
    has_next = rank < col_count - 1
    edge_col = low_half * (local_cols - 1)

    def spot_of(at):
        return at + 1 + late * (local_cols - 1 - 2 * at)

    def true_side(side):
        return side + late * (1 - 2 * side)
    has_lower = mine > 0
    has_upper = mine < groups - 1

    barrier = pltpu.get_barrier_semaphore()
    for at in range(col_count):
        for other in range(group):

            @pl.when((me != other) | (cols_at != at))
            def _():
                pl.semaphore_signal(
                    barrier, inc=1, device_id={"rows": base + other, "cols": at}
                )

    @pl.when(has_lower)
    def _():
        pl.semaphore_signal(barrier, inc=1, device_id={"rows": place - group})

    @pl.when(has_upper)
    def _():
        pl.semaphore_signal(barrier, inc=1, device_id={"rows": place + group})

    loads = [
        pltpu.make_async_copy(source, target, load_sem.at[at])
        for at, (source, target) in enumerate(
            (
                (right_maps_ref.at[:, 0], maps.at[0]),
                (left_maps_ref.at[:, 0], maps.at[1]),
                (top_ref, edges.at[0]),
                (bottom_ref, edges.at[1]),
                (left_ref, sides.at[pl.ds(0, 1)]),
                (right_ref, sides.at[pl.ds(1, 1)]),
            )
        )
    ]
    for load in loads:
        load.start()

    count = kets_ref.shape[2]
    spot = lax.broadcasted_iota(jnp.int32, (count, count), 0)
    from_lane = lax.broadcasted_iota(jnp.int32, (count, count), 1)

    def exchanged(high, low):
        top, bottom = (spot // high) % 2, (spot // low) % 2
        return spot + (bottom - top) * high + (top - bottom) * low

    def led(out, into):
        rest = (spot // 8) % 2 * 16 + (spot // 2) % 2 * 4 + spot % 2
        return rest + spot // 16 * out + (spot // 4) % 2 * into

    for order, ref, target in (
        (led(2, 8), kets, 0),
        (led(8, 2), kets, 1),
        (spot + (exchanged(8, 2) - spot) * late, kets_near, 0),
        (spot + (exchanged(8, 2) - spot) * late + (exchanged(4, 1) - spot), kets_near, 1),
    ):
        for at in range(local_cols):
            values = jnp.broadcast_to(kets_ref[0, at : at + 1, :], (count, count))
            tallest = jnp.sum(
                jnp.where(order == from_lane, values, 0.0), axis=1, keepdims=True
            )
            filled = jnp.broadcast_to(tallest, (count, LANES))
            if ref is kets:
                kets[target, at] = filled
            else:
                kets_near[spot_of(at), target] = filled

    chosen = lax.broadcasted_iota(jnp.int32, (width, wide), 1)
    entry = lax.broadcasted_iota(jnp.int32, (width, wide), 0)
    wanted = (chosen % LANES) * D2 + chosen // LANES
    live = (chosen % LANES) < chi
    pick[...] = jnp.where((wanted == entry) & live, 1.0, 0.0).astype(jnp.bfloat16)
    chosen = lax.broadcasted_iota(jnp.int32, (width, width), 0)
    entry = lax.broadcasted_iota(jnp.int32, (width, width), 1)
    wanted = (chosen % chi) * D2 + chosen // chi
    turn_pick[...] = jnp.where(wanted == entry, 1.0, 0.0).astype(jnp.bfloat16)
    xw[...] = jnp.zeros_like(xw)
    for load in loads:
        load.wait()
    greeted = jnp.where(has_lower, 1, 0) + jnp.where(has_upper, 1, 0)
    pl.semaphore_wait(barrier, group * col_count - 1 + greeted)

    def pass_token(way_at):
        pl.semaphore_signal(
            token.at[way_at], inc=1, device_id={"rows": place + (group, -group)[way_at]}
        )

    @pl.when(has_upper & jnp.logical_not(has_lower))
    def _():
        pass_token(0)

    @pl.when(has_lower & jnp.logical_not(has_upper))
    def _():
        pass_token(1)

    ket_copy = pltpu.make_async_remote_copy(
        kets_near.at[local_cols],
        kets_near.at[0],
        ket_send,
        ket_recv,
        device_id={"cols": cols_at + onward},
    )

    @pl.when(has_next)
    def _():
        ket_copy.start()

    def map_copies(target_way, target_col, target, local):
        made = []
        for kind, (source, buffer) in enumerate(
            ((kets, kbuf), (maps.at[0], qbuf), (maps.at[1], pbuf))
        ):
            origin, landing = source.at[target_way, target_col], buffer.at[me]
            if local:
                made.append(pltpu.make_async_copy(origin, landing, map_recv.at[kind, me]))
            else:
                made.append(
                    pltpu.make_async_remote_copy(
                        origin,
                        landing,
                        map_send.at[kind, target],
                        map_recv.at[kind, me],
                        device_id={"rows": base + target},
                    )
                )
        return made

    def each_map(target_way, cross, act):
        for target_col in range(local_cols):
            target = target_col * 2 + target_way
            wanted = (target_col != column) if cross else (target_col == column)

            @pl.when(wanted & (target != me))
            def _():
                for copy in map_copies(target_way, target_col, target, False):
                    act(copy, False)

            @pl.when(wanted & (target == me))
            def _():
                for copy in map_copies(target_way, target_col, target, True):
                    act(copy, True)

    def start(copy, local):
        copy.start()

    def finish(copy, local):
        if not local:
            copy.wait_send()

    opening_chain = jnp.logical_not(has_before)

    def start_later_maps():
        for cross in (True, False):
            each_map(late, cross, start)

    each_map(low_half, False, start)
    leading = me % 2 == low_half

    @pl.when(leading)
    def _():
        each_map(low_half, True, start)

    def clear(at, unused):
        thi[...] = jnp.zeros_like(thi)
        tlo[...] = jnp.zeros_like(tlo)
        return unused

    lax.fori_loop(0, jnp.where(leading, 1, PACE), clear, 0)

    @pl.when(jnp.logical_not(leading))
    def _():
        each_map(low_half, True, start)

    @pl.when(has_before)
    def _():
        each_map(low_half, True, finish)
        start_later_maps()

    lane_pair = lax.broadcasted_iota(jnp.int32, (count // 2, width), 1) // chi

    def folded_kets(values):
        former, latter = (
            jnp.concatenate([part] * (width // LANES), axis=1)
            for part in (values[: count // 2], values[count // 2 :])
        )
        ket = jnp.where(lane_pair // D == 0, former, latter)
        bra = jnp.where(lane_pair % D == 0, former, latter)
        legs = D**3
        for i in range(legs):
            total = ket[i : i + 1] * bra[:legs]
            for p in range(1, PHYS):
                total += ket[p * legs + i : p * legs + i + 1] * bra[p * legs : (p + 1) * legs]
            ebuf[i * legs : (i + 1) * legs] = total

    def fold_into(target):
        chunk = 16
        full = width // (2 * LANES) * 2 * LANES

        def through(at, unused):
            start = pl.multiple_of(at * chunk, chunk)
            tiles = [rbuf[pl.ds(c * chi + start, chunk), :] for c in range(D2)]
            for g in range(D2):
                for h in range(D2):
                    total = None
                    for c, tile in enumerate(tiles):
                        ket_at = (h // D) * 4 + (g // D) * 2 + c // D
                        bra_at = (h % D) * 4 + (g % D) * 2 + c % D
                        spot = ket_at * D**3 + bra_at
                        term = ebuf[spot : spot + 1, :] * tile
                        total = term if total is None else total + term
                    high, low = halves(total)
                    rows = pl.ds((g * D2 + h) * chi + start, chunk)
                    target[rows, :width] = high
                    target[rows, width : 2 * width - full] = low[:, full:]
                    target[rows, 2 * width - full :] = low[:, :full]
            return unused

        lax.fori_loop(0, chi // chunk, through, 0)

    def put_right(values):
        high, low = halves(values)
        xw[:chi, :width] = high
        xw[LANES : LANES + chi, :width] = high
        xw[:chi, width:] = low

    def joined_with(maps):
        both = dot32(maps, xw[...])
        return both[:, :width] + both[:, width:]

    def absorbed(at_step):
        full = width // (2 * LANES) * 2 * LANES
        part = D2 * chi // 2
        joined = [
            joined_with(pmap[at_step, at : at + part])
            for at in (0, part)
        ]
        total = None
        for at, piece in enumerate(joined):
            rows = [
                jnp.concatenate([half[g * chi : (g + 1) * chi] for g in range(D2 // 2)], axis=1)
                for half in halves(piece)
            ]
            depth = slice(at * D2 // 2 * width, (at + 1) * D2 // 2 * width)
            large = dot32(jnp.concatenate(rows, axis=0), fold[at_step, depth, : 2 * width - full])
            front = large[:chi, :width] + large[chi:, :width]
            rest = large[:chi, width:] + large[chi:, width:]
            small = dot32(rows[0], fold[at_step, depth, 2 * width - full :])
            value = jnp.concatenate([front[:, :full] + small, front[:, full:] + rest], axis=1)
            total = value if total is None else total + value
        return total

    def size_of(values):
        square = jnp.sum(jnp.sum(values * values, axis=1, keepdims=True), axis=0, keepdims=True)
        return square / (chi * width)

    def prepare(step, unused):
        slot = step + way * (group - 1 - 2 * step)
        for kind, buffer in enumerate((kbuf, qbuf, pbuf)):
            pltpu.make_async_copy(
                buffer.at[slot], buffer.at[slot], map_recv.at[kind, slot]
            ).wait()
        folded_kets(kbuf[slot])
        gap = jnp.zeros((LANES - chi, width), jnp.bfloat16)
        high, low = halves(qbuf[slot])
        turned = dot_last(turn_pick[...], jnp.concatenate([high, gap, low, gap], axis=0))
        turned = turned[:, :LANES] + turned[:, LANES:]
        for t, tile in enumerate(pack_lanes([turned] * D2, chi)):
            rbuf[:, t * LANES : (t + 1) * LANES] = tile
        spread_map = dot32(
            jnp.concatenate(halves(pbuf[slot]), axis=0), pick[...]
        ).astype(jnp.bfloat16)
        for at in range(2):
            for l in range(D2):
                lanes = slice(at * LANES, (at + 1) * LANES)
                pmap[step, l * chi : (l + 1) * chi, lanes] = spread_map[
                    at * chi : (at + 1) * chi, l * LANES : (l + 1) * LANES
                ]
        fold_into(fold.at[step])
        return unused

    def row_copy(source, landing, send, recv, slot):
        remote = pltpu.make_async_remote_copy(
            source, landing, send, recv, device_id={"rows": base + slot}
        )
        return remote, pltpu.make_async_copy(source, landing, recv)

    def send_row(source, landing, send, recv, slot):
        remote, local = row_copy(source, landing, send, recv, slot)

        @pl.when(slot != me)
        def _():
            remote.start()

        @pl.when(slot == me)
        def _():
            local.start()

    chain_hop = pltpu.make_async_remote_copy(
        xbuf.at[group],
        xbuf.at[0],
        chain_send,
        chain_recv,
        device_id={"rows": after * group + me},
    )

    start_slot = way * (group - 1)
    crossing = jnp.logical_not(has_before) & ((start_slot // local_cols) != (me // local_cols))
    ahead = jnp.where(has_before, group, jnp.where(crossing, group - local_cols + 1, 1))
    turned_by = jnp.where(crossing, local_cols, 0)

    def prepare_ahead(turn, unused):
        return prepare((turn + turned_by) % group, unused)


    @pl.when(has_lower & has_upper)
    def _():
        for way_at in range(2):
            pl.semaphore_wait(token.at[way_at], 1)
            pass_token(way_at)

    def side_copy(step, slot):
        return pltpu.make_async_remote_copy(
            xbuf.at[step],
            env_ref.at[way, 0],
            side_send.at[step],
            env_recv.at[way, 0],
            device_id={"rows": base + slot, "cols": cols_at + onward},
        )

    def absorb(step, carried):
        known, ratio = carried
        slot = step + way * (group - 1 - 2 * step)

        @pl.when(opening_chain & (step == local_cols))
        def _():
            start_later_maps()

        pending = (step >= 1) & jnp.logical_not(crossing & (step >= local_cols))

        @pl.when(pending & jnp.logical_not(has_before))
        def _():
            prepare(step, 0)

        send_row(
            xbuf.at[step],
            env_ref.at[way, spot_of(column)],
            env_send.at[step],
            env_recv.at[way, spot_of(column)],
            slot,
        )

        @pl.when(has_next & (column == edge_col))
        def _():
            side_copy(step, slot).start()

        renewed = absorbed(step)
        put_right(renewed * known)
        factor = ratio * lax.rsqrt(ratio * ratio * size_of(renewed) + EPSILON)
        xbuf[step + 1] = renewed * factor

        @pl.when((step == group - 1) & has_after)
        def _():
            chain_hop.start()

        return factor, factor / known

    def run_chain():
        lax.fori_loop(0, ahead, prepare_ahead, 0)

        @pl.when(has_before)
        def _():
            pltpu.make_async_copy(xbuf.at[0], xbuf.at[0], chain_recv).wait()

        @pl.when(jnp.logical_not(has_before) & (way == 0))
        def _():
            xbuf[0] = edges[0, column]

        @pl.when(jnp.logical_not(has_before) & (way == 1))
        def _():
            xbuf[0] = edges[1, column]

        put_right(xbuf[0])
        one = jnp.ones((1, 1), jnp.float32)
        lax.fori_loop(0, group, absorb, (one, one))

        for step in range(group):
            send_row(
                xbuf.at[step + 1],
                out_ref.at[way, column],
                out_send.at[step],
                out_recv.at[way, column],
                step + way * (group - 1 - 2 * step),
            )

    unit = jnp.where(
        lax.broadcasted_iota(jnp.int32, (LANES, LANES), 0)
        == lax.broadcasted_iota(jnp.int32, (LANES, LANES), 1),
        1.0,
        0.0,
    ).astype(jnp.bfloat16)
    fill = jnp.zeros((LANES - chi, LANES), jnp.bfloat16)

    def take_blocks(kind, at):
        landed = env_ref.at[kind, at]
        pltpu.make_async_copy(landed, landed, env_recv.at[kind, at]).wait()
        blocks = unpack_lanes(load_tiles(env_ref.at[kind], at, width), chi)
        for d, block in enumerate(blocks):
            lanes = slice(d * LANES, (d + 1) * LANES)
            for part, values in enumerate(halves(block)):
                tall_block = jnp.concatenate([values, fill], axis=0)
                turned = dot_last(unit, tall_block).astype(jnp.bfloat16)
                yield lanes, part, values, tall_block, turned

    def take_far(at):
        for lanes, part, values, tall_block, turned in take_blocks(early, at):
            for copy in (0, 1) if part == 0 else (2,):
                rows = slice(copy * LANES, (copy + 1) * LANES)
                far[1, at, rows, lanes] = turned
                far[0, at, rows, lanes] = tall_block

    def take_near(side, at):
        blocks = unpack_lanes(load_tiles(env_ref.at[late], at, width), chi)
        for d, block in enumerate(blocks):
            lanes = slice(d * LANES, (d + 1) * LANES)
            for part, values in enumerate(halves(block)):
                rows = slice(part * chi, (part + 1) * chi)
                if side == 0:
                    values = dot_last(unit, jnp.concatenate([values, fill], axis=0))
                    values = values.astype(jnp.bfloat16)[:chi]
                near[rows, lanes] = values

    second = jnp.where(rank >= col_count // 2, 1, 0)

    def hop(side):
        return pltpu.make_async_remote_copy(
            hop_out.at[side],
            hop_in.at[side],
            hop_send.at[side],
            hop_recv.at[side],
            device_id={"cols": cols_at + onward * (1 - 2 * side)},
        )

    def put_environ(blocks):
        for at, block in enumerate(blocks):
            vbuf[at * chi : (at + 1) * chi] = block

    def put_edge(side):
        blocks = unpack_lanes(load_tiles(sides, true_side(side), width), chi)

        @pl.when(late == 0)
        def _():
            put_environ(blocks)

        @pl.when(late == 1)
        def _():
            empty = jnp.zeros((LANES - chi, LANES), jnp.float32)
            put_environ([jnp.concatenate([block, empty], axis=0).T[:chi] for block in blocks])

    def place_of(side, order):
        return order + side * (local_cols - 2 * order)

    def join(side, at_column):
        v_high, v_low = halves(vbuf[...])
        true = true_side(side)
        jbuf[...] = dot32(
            jnp.concatenate([v_high, v_low], axis=1), far[true, at_column, : 2 * LANES]
        ) + dot32(v_high, far[true, at_column, 2 * LANES :])

    chunk = 16

    def pass_through(side, at_column, p, start):
        true = true_side(side)

        def ket(p, u, i, d, o):
            at = p * 16 + u * 8 + i * 4 + d * 2 + o
            return kets_near[at_column, true, at : at + 1, :]

        def joined(i, d):
            return jbuf[pl.ds(i * chi + start, chunk), d * LANES : (d + 1) * LANES]

        for u in range(D):
            for o in range(D):
                part = {}
                for i2 in range(D):
                    for d2 in range(D):
                        total = None
                        for i in range(D):
                            for d in range(D):
                                term = ket(p, u, i, d, o) * joined(i * D + i2, d * D + d2)
                                total = term if total is None else total + term
                        part[i2, d2] = total
                for q in range(PHYS):
                    for u2 in range(D):
                        for o2 in range(D):
                            total = None
                            for i2 in range(D):
                                for d2 in range(D):
                                    term = ket(q, u2, i2, d2, o2) * part[i2, d2]
                                    total = term if total is None else total + term
                            high, low = halves(total)
                            rows = pl.ds((u * D + u2) * LANES + start, chunk)
                            spot = (p * PHYS + q) * D2 + o * D + o2
                            lanes = slice(spot * LANES, (spot + 1) * LANES)
                            thi[rows, lanes] = high
                            tlo[rows, lanes] = low

    def open_up(side, at_column):
        join(side, at_column)

        def through(at, unused):
            for p in range(PHYS):
                pass_through(side, at_column, p, pl.multiple_of(at * chunk, chunk))
            return unused

        lax.fori_loop(0, chi // chunk, through, 0)

    def close(side, at_column, pair):
        both = near[...]
        lanes = slice(pair * wide, (pair + 1) * wide)
        large = dot32(both, thi[:, lanes])
        opens[true_side(side), at_column - side, pair] = large[:chi] + (
            large[chi:] + dot32(both[:chi], tlo[:, lanes])
        )

    def first_order(side):
        return jnp.where((side == 0) & (rank == 0), 1, 0)

    def is_edge(side):
        return ((side == 0) & (rank == 0)) | ((side == 1) & (rank == col_count - 1))

    def early_work():
        @pl.when(has_prev)
        def _():
            pltpu.make_async_copy(kets_near.at[0], kets_near.at[0], ket_recv).wait()

        for at in range(1, local_cols + 1):
            take_far(at)

        @pl.when(has_prev)
        def _():
            take_far(0)

        for side in range(2):

            @pl.when(is_edge(side))
            def _():
                put_edge(side)

        @pl.when(is_edge(second))
        def _():
            open_up(second, place_of(second, first_order(second)))

    early_first = (way != low_half) & (mine != groups // 2) & (mine != groups // 2 - 1)
    early_at = jnp.where(early_first, 0, 1)

    def phase(at, unused):
        @pl.when(at == early_at)
        def _():
            early_work()

        @pl.when(at != early_at)
        def _():
            run_chain()

        return unused

    lax.fori_loop(0, 2, phase, 0)

    spot_row = lax.broadcasted_iota(jnp.int32, (terms, terms), 0)
    spot_lane = lax.broadcasted_iota(jnp.int32, (terms, terms), 1)

    def stand(ref):
        values = jnp.broadcast_to(ref[...].astype(jnp.float32), (terms, terms))
        return jnp.sum(jnp.where(spot_row == spot_lane, values, 0.0), axis=1, keepdims=True)

    term_row = stand(rows_ref).astype(jnp.int32)
    term_bond = stand(bonds_ref).astype(jnp.int32)
    term_op = stand(ops_ref).astype(jnp.int32)
    term_weights = jnp.zeros((terms, table_ref.shape[1]), jnp.float32)
    for op in range(table_ref.shape[0]):
        term_weights = jnp.where(term_op == op, table_ref[op : op + 1, :], term_weights)

    def walk(turn, unused):
        side = (turn // local_cols + second) % 2
        order = turn % local_cols
        at_column = place_of(side, order)
        absent = (rank == 0) & (at_column == side)
        opening = order == first_order(side)
        ending = order == local_cols - 1

        fresh = (turn < local_cols) | (at_column == side * local_cols)

        @pl.when(jnp.logical_not(absent) & fresh)
        def _():
            landed = env_ref.at[late, at_column]
            pltpu.make_async_copy(landed, landed, env_recv.at[late, at_column]).wait()

        for at in range(2):

            @pl.when(jnp.logical_not(absent) & (true_side(side) == at))
            def _():
                take_near(at, at_column)

        @pl.when((order == 0) & jnp.logical_not(is_edge(side)))
        def _():
            pltpu.make_async_copy(hop_in.at[side], hop_in.at[side], hop_recv.at[side]).wait()
            put_environ(unpack_lanes(load_tiles(hop_in, side, width), chi))

        @pl.when(jnp.logical_not(absent) & opening & is_edge(side))
        def _():
            for pair in range(pairs):
                close(side, at_column, pair)

        @pl.when(jnp.logical_not(absent) & jnp.logical_not(opening & is_edge(side)))
        def _():
            join(side, at_column)
            for p in range(PHYS):
                for start in range(0, chi, chunk):
                    pass_through(side, at_column, p, start)
                for q in range(PHYS):
                    close(side, at_column, p * PHYS + q)

        asked = jnp.where(side == 0, has_next, has_prev) | jnp.logical_not(ending)

        @pl.when(jnp.logical_not(absent) & asked)
        def _():
            closed = opens[true_side(side), at_column - side, 0]
            for p in range(1, PHYS):
                closed += opens[true_side(side), at_column - side, p * PHYS + p]
            square = jnp.sum(
                jnp.sum(closed * closed, axis=1, keepdims=True), axis=0, keepdims=True
            )
            closed = closed * (1.0 / jnp.sqrt(square / (chi * width) + EPSILON))
            blocks = [closed[:, d * LANES : (d + 1) * LANES] for d in range(D2)]
            put_environ(blocks)

            @pl.when(ending)
            def _():
                for t, tile in enumerate(pack_lanes(blocks, chi)):
                    hop_out[side, :, t * LANES : (t + 1) * LANES] = tile

        @pl.when(ending & (side == 0) & has_next)
        def _():
            hop(0).start()

        @pl.when(ending & (side == 1) & has_prev)
        def _():
            hop(1).start()

        return unused

    lax.fori_loop(0, 2 * local_cols, walk, 0)

    tall = (terms, LANES)
    lane = lax.broadcasted_iota(jnp.int32, tall, 1)
    held = shared.at[0]
    held[...] = jnp.zeros(tall, jnp.float32)
    here = jnp.zeros((terms, 1), jnp.int32)
    for k in range(local_cols):
        bond = cols_at * local_cols + k - 1 + late * (local_cols - 2 * k)
        hit = (term_row == place) & (term_bond == bond)
        here = jnp.where(hit, 1, here)

        def add_bond(k=k, hit=hit):
            values = jnp.zeros(tall, jnp.float32)
            for p in range(pairs):
                former = opens[0, k, p]
                for q in range(pairs):
                    value = jnp.sum(
                        jnp.sum(former * opens[1, k, q], axis=0, keepdims=True),
                        axis=1,
                        keepdims=True,
                    )
                    values = jnp.where(lane == p * pairs + q, value, values)
            held[...] += jnp.where(hit, values, 0.0)

        if k:
            add_bond()
        else:
            pl.when(has_prev)(add_bond)

    total = held[...]
    picked = jnp.sum(total[:, : pairs * pairs] * term_weights, axis=1, keepdims=True)
    bra, ket_at = lane % pairs, lane // pairs
    diagonal = (bra // PHYS == bra % PHYS) & (ket_at // PHYS == ket_at % PHYS)
    trace = jnp.sum(
        jnp.where(diagonal & (lane < pairs * pairs), total, 0.0), axis=1, keepdims=True
    )
    size = jnp.sqrt(jnp.sum(total * total, axis=1, keepdims=True))
    energy = picked / jnp.maximum(jnp.abs(trace), 0.25 * size)
    same = lax.broadcasted_iota(jnp.int32, tall, 0) == lane
    devices = row_count * col_count
    spot_mine = place * col_count + cols_at
    own = own_share.at[0]
    own[...] = jnp.sum(jnp.where(same & (here == 1), energy, 0.0), axis=0, keepdims=True)

    @pl.when(has_lower & jnp.logical_not(has_upper))
    def _():
        pl.semaphore_wait(token.at[0], 1)

    @pl.when(has_upper & jnp.logical_not(has_lower))
    def _():
        pl.semaphore_wait(token.at[1], 1)

    def tell(turn, unused):
        row = turn + late * (row_count - 1 - 2 * turn)
        for col in range(col_count):

            @pl.when((row != place) | (col != cols_at))
            def _():
                pltpu.make_async_remote_copy(
                    own,
                    share.at[spot_mine],
                    share_send,
                    share_recv,
                    device_id={"rows": row, "cols": col},
                ).start()

        return unused

    lax.fori_loop(0, row_count, tell, 0)
    pltpu.make_async_copy(own, share.at[spot_mine], share_recv).start()
    pltpu.make_async_copy(share, share, share_recv).wait()
    others = share.at[pl.ds(0, devices - 1)]
    pltpu.make_async_copy(others, others, share_send).wait()

    @pl.when(has_next)
    def _():
        hop(0).wait_send()
        ket_copy.wait_send()

    @pl.when(has_prev)
    def _():
        hop(1).wait_send()

    for step in range(group):
        slot = step + way * (group - 1 - 2 * step)

        @pl.when(slot != me)
        def _():
            row_copy(
                xbuf.at[step],
                env_ref.at[way, spot_of(column)],
                env_send.at[step],
                env_recv.at[way, spot_of(column)],
                slot,
            )[0].wait_send()
            row_copy(
                xbuf.at[step + 1],
                out_ref.at[way, column],
                out_send.at[step],
                out_recv.at[way, column],
                slot,
            )[0].wait_send()

        @pl.when(has_next & (column == edge_col))
        def _():
            side_copy(step, slot).wait_send()

    @pl.when(opening_chain)
    def _():
        each_map(low_half, True, finish)

    each_map(low_half, False, finish)
    for cross in (True, False):
        each_map(late, cross, finish)

    @pl.when(has_after)
    def _():
        chain_hop.wait_send()

    for a in range(2):
        for b in range(local_cols):
            pltpu.make_async_copy(out_ref.at[a, b], out_ref.at[a, b], out_recv.at[a, b]).wait()


def window(row_count, col_count, args):
    local_cols = args[0].shape[1]
    chi, width = args[1].shape[-2:]
    terms = args[7].shape[0]
    group = 2 * local_cols
    wide = D2 * LANES
    pairs = PHYS * PHYS
    entries = args[0].shape[2]
    vmem = pl.BlockSpec(memory_space=pltpu.VMEM)
    stay = pl.BlockSpec(memory_space=pltpu.HBM)
    dma = pltpu.SemaphoreType.DMA

    def f32(*shape):
        return pltpu.VMEM(shape, jnp.float32)

    def bf16(*shape):
        return pltpu.VMEM(shape, jnp.bfloat16)

    return pl.pallas_call(
        functools.partial(window_kernel, row_count, col_count),
        out_shape=(
            jax.ShapeDtypeStruct((2, local_cols, chi, width), jnp.float32),
            jax.ShapeDtypeStruct((row_count * col_count, 1, LANES), jnp.float32),
        ),
        in_specs=[vmem] + [stay] * 6 + [vmem] * 4,
        out_specs=(stay, stay),
        scratch_shapes=[
            f32(2, local_cols, entries, LANES),
            f32(local_cols + 1, 2, entries, LANES),
            f32(2, 2, local_cols, chi, width),
            f32(2, local_cols, chi, width),
            f32(2, chi, width),
            f32(2, local_cols + 1, chi, width),
            f32(group, chi, width),
            f32(group, chi, width),
            f32(group, entries, LANES),
            f32(group + 1, chi, width),
            f32(D2**3, width),
            bf16(width, wide),
            bf16(width, width),
            bf16(group, width, 2 * LANES),
            f32(width, width),
            bf16(group, D2 * width, 2 * width),
            bf16(2 * LANES, 2 * width),
            f32(D2 * chi, wide),
            bf16(wide, pairs * wide),
            bf16(wide, pairs * wide),
            bf16(2 * chi, wide),
            bf16(2, local_cols + 1, 3 * LANES, wide),
            f32(D2 * chi, LANES),
            f32(2, local_cols, pairs, chi, wide),
            f32(2, chi, width),
            f32(2, chi, width),
            f32(1, 1, LANES),
            f32(1, terms, LANES),
            pltpu.SemaphoreType.REGULAR((2,)),
            dma((6,)),
            dma((3, group)),
            dma((3, group)),
            dma((group,)),
            dma((group,)),
            dma((2, local_cols + 1)),
            dma((group,)),
            dma((2, local_cols)),
            dma,
            dma,
            dma((2,)),
            dma((2,)),
            dma,
            dma,
            dma,
            dma,
        ],
        compiler_params=pltpu.CompilerParams(
            collective_id=0, has_side_effects=True, vmem_limit_bytes=56 * 1024 * 1024
        ),
        name="window",
    )(*args[:7], *(index[None] for index in args[7:10]), args[10])


def settle_kernel(
    outs_ref, share_ref, top_ref, bottom_ref, energies_ref, held, shares, line, sem
):
    gather = pltpu.make_async_copy(share_ref, shares, sem.at[0, 0])
    gather.start()
    parts = [
        (outs_ref.at[way, at], held.at[way, at], (top_ref, bottom_ref)[way].at[0, at])
        for way in range(2)
        for at in range(held.shape[1])
    ]
    for at, (source, middle, target) in enumerate(parts):
        pltpu.make_async_copy(source, middle, sem.at[0, at + 1]).start()
    gather.wait()
    line[...] = jnp.sum(shares[...], axis=0)[:, : line.shape[1]]
    put = pltpu.make_async_copy(line, energies_ref, sem.at[1, 0])
    put.start()
    for at, (source, middle, target) in enumerate(parts):
        pltpu.make_async_copy(source, middle, sem.at[0, at + 1]).wait()
        pltpu.make_async_copy(middle, target, sem.at[1, at + 1]).start()
    for at, (source, middle, target) in enumerate(parts):
        pltpu.make_async_copy(middle, target, sem.at[1, at + 1]).wait()
    put.wait()


def settle(outs, shares, terms):
    stay = pl.BlockSpec(memory_space=pltpu.HBM)
    half = jax.ShapeDtypeStruct((1,) + outs.shape[1:], outs.dtype)
    count = outs.shape[0] * outs.shape[1] + 1
    return pl.pallas_call(
        settle_kernel,
        out_shape=(half, half, jax.ShapeDtypeStruct((1, terms), shares.dtype)),
        in_specs=[stay] * 2,
        out_specs=(stay,) * 3,
        scratch_shapes=[
            pltpu.VMEM(outs.shape, outs.dtype),
            pltpu.VMEM(shares.shape, shares.dtype),
            pltpu.VMEM((1, terms), shares.dtype),
            pltpu.SemaphoreType.DMA((2, count)),
        ],
        name="settle",
    )(outs, shares)


def shards(*args):
    outs, shares = window(lax.axis_size("rows"), lax.axis_size("cols"), args)
    top, bottom, energies = settle(outs, shares, args[7].shape[0])
    return (top, bottom, energies[0])


def solution(mesh):
    placed = (
        P("rows", "cols", None),
        P(None, "rows", "cols", None, None),
        P(None, "rows", "cols", None, None),
        P("cols", None, None),
        P("cols", None, None),
        P("rows", None, None),
        P("rows", None, None),
        P(),
        P(),
        P(),
        P(),
    )
    return jax.shard_map(
        shards,
        mesh=mesh,
        in_specs=placed,
        out_specs=(P("rows", "cols", None, None), P("rows", "cols", None, None), P()),
        check_vma=False,
    )
```

```python
import functools

import jax
import jax.numpy as jnp
from jax import lax
from jax.experimental import pallas as pl
from jax.experimental.pallas import tpu as pltpu
from jax.sharding import PartitionSpec as P

D = 2
D2 = 4
PHYS = 2
EPSILON = 1e-06
LANES = 128
PACE = 9


def unpack_lanes(tiles, chi):
    rolled = {}
    lane = lax.broadcasted_iota(jnp.int32, tiles[0].shape, 1)
    blocks = []
    for block in range(D2):
        total = jnp.zeros_like(tiles[0])
        for place, tile in enumerate(tiles):
            low = max(chi * block, LANES * place)
            high = min(chi * (block + 1), LANES * (place + 1))
            if low >= high:
                continue
            shift = (LANES * place - chi * block) % LANES
            if (place, shift) not in rolled:
                rolled[place, shift] = tile if shift == 0 else pltpu.roll(tile, shift, 1)
            inside = (lane >= low - chi * block) & (lane < high - chi * block)
            total = jnp.where(inside, rolled[place, shift], total)
        blocks.append(total)
    return blocks


def pack_lanes(blocks, chi):
    lane = lax.broadcasted_iota(jnp.int32, blocks[0].shape, 1)
    rolled = {}
    tiles = []
    for place in range(chi * D2 // LANES):
        total = jnp.zeros_like(blocks[0])
        for block, values in enumerate(blocks):
            low = max(chi * block, LANES * place)
            high = min(chi * (block + 1), LANES * (place + 1))
            if low >= high:
                continue
            shift = (chi * block - LANES * place) % LANES
            if (block, shift) not in rolled:
                rolled[block, shift] = values if shift == 0 else pltpu.roll(values, shift, 1)
            inside = (lane >= low - LANES * place) & (lane < high - LANES * place)
            total = jnp.where(inside, rolled[block, shift], total)
        tiles.append(total)
    return tiles


def halves(values):
    high = values.astype(jnp.bfloat16)
    low = (values - high.astype(jnp.float32)).astype(jnp.bfloat16)
    return high, low


def dot32(former, latter):
    return jnp.dot(former, latter, preferred_element_type=jnp.float32)


def dot_last(former, latter):
    return lax.dot_general(
        former, latter, (((1,), (1,)), ((), ())), preferred_element_type=jnp.float32
    )


def load_tiles(ref, at, width):
    return [ref[at, :, LANES * t : LANES * (t + 1)] for t in range(width // LANES)]


def window_kernel(
    row_count,
    col_count,
    kets_ref,
    left_maps_ref,
    right_maps_ref,
    top_ref,
    bottom_ref,
    left_ref,
    right_ref,
    rows_ref,
    bonds_ref,
    ops_ref,
    table_ref,
    out_ref,
    share,
    kets,
    kets_near,
    maps,
    edges,
    sides,
    env_ref,
    pbuf,
    qbuf,
    kbuf,
    xbuf,
    ebuf,
    pick,
    turn_pick,
    pmap,
    rbuf,
    fold,
    xw,
    jbuf,
    thi,
    tlo,
    near,
    far,
    vbuf,
    opens,
    hop_out,
    hop_in,
    own_share,
    shared,
    token,
    load_sem,
    map_send,
    map_recv,
    env_send,
    side_send,
    env_recv,
    out_send,
    out_recv,
    chain_send,
    chain_recv,
    hop_send,
    hop_recv,
    share_send,
    share_recv,
    ket_send,
    ket_recv,
):
    local_cols = kets.shape[1]
    chi, width = maps.shape[3], maps.shape[4]
    wide = D2 * LANES
    pairs = PHYS * PHYS
    terms = rows_ref.shape[1]
    group = 2 * local_cols
    groups = row_count // group
    place = lax.axis_index("rows")
    cols_at = lax.axis_index("cols")
    mine = place // group
    me = place % group
    column = me // 2
    way = me % 2
    base = mine * group
    before = mine - 1 + 2 * way
    after = mine + 1 - 2 * way
    has_before = (before >= 0) & (before < groups)
    has_after = (after >= 0) & (after < groups)
    low_half = jnp.where(mine >= groups // 2, 1, 0)
    early, late = low_half, 1 - low_half
    onward = 1 - 2 * late
    rank = cols_at + late * (col_count - 1 - 2 * cols_at)
    has_prev = rank > 0
    has_next = rank < col_count - 1
    edge_col = low_half * (local_cols - 1)

    def spot_of(at):
        return at + 1 + late * (local_cols - 1 - 2 * at)

    def true_side(side):
        return side + late * (1 - 2 * side)
    has_lower = mine > 0
    has_upper = mine < groups - 1

    barrier = pltpu.get_barrier_semaphore()
    for at in range(col_count):
        for other in range(group):

            @pl.when((me != other) | (cols_at != at))
            def _():
                pl.semaphore_signal(
                    barrier, inc=1, device_id={"rows": base + other, "cols": at}
                )

    @pl.when(has_lower)
    def _():
        pl.semaphore_signal(barrier, inc=1, device_id={"rows": place - group})

    @pl.when(has_upper)
    def _():
        pl.semaphore_signal(barrier, inc=1, device_id={"rows": place + group})

    loads = [
        pltpu.make_async_copy(source, target, load_sem.at[at])
        for at, (source, target) in enumerate(
            (
                (right_maps_ref.at[:, 0], maps.at[0]),
                (left_maps_ref.at[:, 0], maps.at[1]),
                (top_ref, edges.at[0]),
                (bottom_ref, edges.at[1]),
                (left_ref, sides.at[pl.ds(0, 1)]),
                (right_ref, sides.at[pl.ds(1, 1)]),
            )
        )
    ]
    for load in loads:
        load.start()

    count = kets_ref.shape[2]
    spot = lax.broadcasted_iota(jnp.int32, (count, count), 0)
    from_lane = lax.broadcasted_iota(jnp.int32, (count, count), 1)

    def exchanged(high, low):
        top, bottom = (spot // high) % 2, (spot // low) % 2
        return spot + (bottom - top) * high + (top - bottom) * low

    def led(out, into):
        rest = (spot // 8) % 2 * 16 + (spot // 2) % 2 * 4 + spot % 2
        return rest + spot // 16 * out + (spot // 4) % 2 * into

    for order, ref, target in (
        (led(2, 8), kets, 0),
        (led(8, 2), kets, 1),
        (spot + (exchanged(8, 2) - spot) * late, kets_near, 0),
        (spot + (exchanged(8, 2) - spot) * late + (exchanged(4, 1) - spot), kets_near, 1),
    ):
        for at in range(local_cols):
            values = jnp.broadcast_to(kets_ref[0, at : at + 1, :], (count, count))
            tallest = jnp.sum(
                jnp.where(order == from_lane, values, 0.0), axis=1, keepdims=True
            )
            filled = jnp.broadcast_to(tallest, (count, LANES))
            if ref is kets:
                kets[target, at] = filled
            else:
                kets_near[spot_of(at), target] = filled

    chosen = lax.broadcasted_iota(jnp.int32, (width, wide), 1)
    entry = lax.broadcasted_iota(jnp.int32, (width, wide), 0)
    wanted = (chosen % LANES) * D2 + chosen // LANES
    live = (chosen % LANES) < chi
    pick[...] = jnp.where((wanted == entry) & live, 1.0, 0.0).astype(jnp.bfloat16)
    chosen = lax.broadcasted_iota(jnp.int32, (width, width), 0)
    entry = lax.broadcasted_iota(jnp.int32, (width, width), 1)
    wanted = (chosen % chi) * D2 + chosen // chi
    turn_pick[...] = jnp.where(wanted == entry, 1.0, 0.0).astype(jnp.bfloat16)
    xw[...] = jnp.zeros_like(xw)
    for load in loads:
        load.wait()
    greeted = jnp.where(has_lower, 1, 0) + jnp.where(has_upper, 1, 0)
    pl.semaphore_wait(barrier, group * col_count - 1 + greeted)

    def pass_token(way_at):
        pl.semaphore_signal(
            token.at[way_at], inc=1, device_id={"rows": place + (group, -group)[way_at]}
        )

    @pl.when(has_upper & jnp.logical_not(has_lower))
    def _():
        pass_token(0)

    @pl.when(has_lower & jnp.logical_not(has_upper))
    def _():
        pass_token(1)

    ket_copy = pltpu.make_async_remote_copy(
        kets_near.at[local_cols],
        kets_near.at[0],
        ket_send,
        ket_recv,
        device_id={"cols": cols_at + onward},
    )

    @pl.when(has_next)
    def _():
        ket_copy.start()

    def map_copies(target_way, target_col, target, local):
        made = []
        for kind, (source, buffer) in enumerate(
            ((kets, kbuf), (maps.at[0], qbuf), (maps.at[1], pbuf))
        ):
            origin, landing = source.at[target_way, target_col], buffer.at[me]
            if local:
                made.append(pltpu.make_async_copy(origin, landing, map_recv.at[kind, me]))
            else:
                made.append(
                    pltpu.make_async_remote_copy(
                        origin,
                        landing,
                        map_send.at[kind, target],
                        map_recv.at[kind, me],
                        device_id={"rows": base + target},
                    )
                )
        return made

    def each_map(target_way, cross, act):
        for target_col in range(local_cols):
            target = target_col * 2 + target_way
            wanted = (target_col != column) if cross else (target_col == column)

            @pl.when(wanted & (target != me))
            def _():
                for copy in map_copies(target_way, target_col, target, False):
                    act(copy, False)

            @pl.when(wanted & (target == me))
            def _():
                for copy in map_copies(target_way, target_col, target, True):
                    act(copy, True)

    def start(copy, local):
        copy.start()

    def finish(copy, local):
        if not local:
            copy.wait_send()

    opening_chain = jnp.logical_not(has_before)

    def start_later_maps():
        for cross in (True, False):
            each_map(late, cross, start)

    each_map(low_half, False, start)
    leading = me % 2 == low_half

    @pl.when(leading)
    def _():
        each_map(low_half, True, start)

    def clear(at, unused):
        thi[...] = jnp.zeros_like(thi)
        tlo[...] = jnp.zeros_like(tlo)
        return unused

    lax.fori_loop(0, jnp.where(leading, 1, PACE), clear, 0)

    @pl.when(jnp.logical_not(leading))
    def _():
        each_map(low_half, True, start)

    @pl.when(has_before)
    def _():
        each_map(low_half, True, finish)
        start_later_maps()

    lane_pair = lax.broadcasted_iota(jnp.int32, (count // 2, width), 1) // chi

    def folded_kets(values):
        former, latter = (
            jnp.concatenate([part] * (width // LANES), axis=1)
            for part in (values[: count // 2], values[count // 2 :])
        )
        ket = jnp.where(lane_pair // D == 0, former, latter)
        bra = jnp.where(lane_pair % D == 0, former, latter)
        legs = D**3
        for i in range(legs):
            total = ket[i : i + 1] * bra[:legs]
            for p in range(1, PHYS):
                total += ket[p * legs + i : p * legs + i + 1] * bra[p * legs : (p + 1) * legs]
            ebuf[i * legs : (i + 1) * legs] = total

    def fold_into(target):
        chunk = 16
        full = width // (2 * LANES) * 2 * LANES

        def through(at, unused):
            start = pl.multiple_of(at * chunk, chunk)
            tiles = [rbuf[pl.ds(c * chi + start, chunk), :] for c in range(D2)]
            for g in range(D2):
                for h in range(D2):
                    total = None
                    for c, tile in enumerate(tiles):
                        ket_at = (h // D) * 4 + (g // D) * 2 + c // D
                        bra_at = (h % D) * 4 + (g % D) * 2 + c % D
                        spot = ket_at * D**3 + bra_at
                        term = ebuf[spot : spot + 1, :] * tile
                        total = term if total is None else total + term
                    high, low = halves(total)
                    rows = pl.ds((g * D2 + h) * chi + start, chunk)
                    target[rows, :width] = high
                    target[rows, width : 2 * width - full] = low[:, full:]
                    target[rows, 2 * width - full :] = low[:, :full]
            return unused

        lax.fori_loop(0, chi // chunk, through, 0)

    def put_right(values):
        high, low = halves(values)
        xw[:chi, :width] = high
        xw[LANES : LANES + chi, :width] = high
        xw[:chi, width:] = low

    def joined_with(maps):
        both = dot32(maps, xw[...])
        return both[:, :width] + both[:, width:]

    def absorbed(at_step):
        full = width // (2 * LANES) * 2 * LANES
        part = D2 * chi // 2
        joined = [
            joined_with(pmap[at_step, at : at + part])
            for at in (0, part)
        ]
        total = None
        for at, piece in enumerate(joined):
            rows = [
                jnp.concatenate([half[g * chi : (g + 1) * chi] for g in range(D2 // 2)], axis=1)
                for half in halves(piece)
            ]
            depth = slice(at * D2 // 2 * width, (at + 1) * D2 // 2 * width)
            large = dot32(jnp.concatenate(rows, axis=0), fold[at_step, depth, : 2 * width - full])
            front = large[:chi, :width] + large[chi:, :width]
            rest = large[:chi, width:] + large[chi:, width:]
            small = dot32(rows[0], fold[at_step, depth, 2 * width - full :])
            value = jnp.concatenate([front[:, :full] + small, front[:, full:] + rest], axis=1)
            total = value if total is None else total + value
        return total

    def size_of(values):
        square = jnp.sum(jnp.sum(values * values, axis=1, keepdims=True), axis=0, keepdims=True)
        return square / (chi * width)

    def prepare(step, unused):
        slot = step + way * (group - 1 - 2 * step)
        for kind, buffer in enumerate((kbuf, qbuf, pbuf)):
            pltpu.make_async_copy(
                buffer.at[slot], buffer.at[slot], map_recv.at[kind, slot]
            ).wait()
        folded_kets(kbuf[slot])
        gap = jnp.zeros((LANES - chi, width), jnp.bfloat16)
        high, low = halves(qbuf[slot])
        turned = dot_last(turn_pick[...], jnp.concatenate([high, gap, low, gap], axis=0))
        turned = turned[:, :LANES] + turned[:, LANES:]
        for t, tile in enumerate(pack_lanes([turned] * D2, chi)):
            rbuf[:, t * LANES : (t + 1) * LANES] = tile
        spread_map = dot32(
            jnp.concatenate(halves(pbuf[slot]), axis=0), pick[...]
        ).astype(jnp.bfloat16)
        for at in range(2):
            for l in range(D2):
                lanes = slice(at * LANES, (at + 1) * LANES)
                pmap[step, l * chi : (l + 1) * chi, lanes] = spread_map[
                    at * chi : (at + 1) * chi, l * LANES : (l + 1) * LANES
                ]
        fold_into(fold.at[step])
        return unused

    def row_copy(source, landing, send, recv, slot):
        remote = pltpu.make_async_remote_copy(
            source, landing, send, recv, device_id={"rows": base + slot}
        )
        return remote, pltpu.make_async_copy(source, landing, recv)

    def send_row(source, landing, send, recv, slot):
        remote, local = row_copy(source, landing, send, recv, slot)

        @pl.when(slot != me)
        def _():
            remote.start()

        @pl.when(slot == me)
        def _():
            local.start()

    chain_hop = pltpu.make_async_remote_copy(
        xbuf.at[group],
        xbuf.at[0],
        chain_send,
        chain_recv,
        device_id={"rows": after * group + me},
    )

    start_slot = way * (group - 1)
    crossing = jnp.logical_not(has_before) & ((start_slot // local_cols) != (me // local_cols))
    ahead = jnp.where(has_before, group, jnp.where(crossing, group - local_cols + 1, 1))
    turned_by = jnp.where(crossing, local_cols, 0)

    def prepare_ahead(turn, unused):
        return prepare((turn + turned_by) % group, unused)


    @pl.when(has_lower & has_upper)
    def _():
        for way_at in range(2):
            pl.semaphore_wait(token.at[way_at], 1)
            pass_token(way_at)

    def side_copy(step, slot):
        return pltpu.make_async_remote_copy(
            xbuf.at[step],
            env_ref.at[way, 0],
            side_send.at[step],
            env_recv.at[way, 0],
            device_id={"rows": base + slot, "cols": cols_at + onward},
        )

    def absorb(step, carried):
        known, ratio = carried
        slot = step + way * (group - 1 - 2 * step)

        @pl.when(opening_chain & (step == local_cols))
        def _():
            start_later_maps()

        pending = (step >= 1) & jnp.logical_not(crossing & (step >= local_cols))

        @pl.when(pending & jnp.logical_not(has_before))
        def _():
            prepare(step, 0)

        @pl.when(has_next & (column == edge_col))
        def _():
            side_copy(step, slot).start()

        send_row(
            xbuf.at[step],
            env_ref.at[way, spot_of(column)],
            env_send.at[step],
            env_recv.at[way, spot_of(column)],
            slot,
        )

        renewed = absorbed(step)
        put_right(renewed * known)
        factor = ratio * lax.rsqrt(ratio * ratio * size_of(renewed) + EPSILON)
        xbuf[step + 1] = renewed * factor

        @pl.when((step == group - 1) & has_after)
        def _():
            chain_hop.start()

        return factor, factor / known

    def run_chain():
        lax.fori_loop(0, ahead, prepare_ahead, 0)

        @pl.when(has_before)
        def _():
            pltpu.make_async_copy(xbuf.at[0], xbuf.at[0], chain_recv).wait()

        @pl.when(jnp.logical_not(has_before) & (way == 0))
        def _():
            xbuf[0] = edges[0, column]

        @pl.when(jnp.logical_not(has_before) & (way == 1))
        def _():
            xbuf[0] = edges[1, column]

        put_right(xbuf[0])
        one = jnp.ones((1, 1), jnp.float32)
        lax.fori_loop(0, group, absorb, (one, one))

        for step in range(group):
            send_row(
                xbuf.at[step + 1],
                out_ref.at[way, column],
                out_send.at[step],
                out_recv.at[way, column],
                step + way * (group - 1 - 2 * step),
            )

    unit = jnp.where(
        lax.broadcasted_iota(jnp.int32, (LANES, LANES), 0)
        == lax.broadcasted_iota(jnp.int32, (LANES, LANES), 1),
        1.0,
        0.0,
    ).astype(jnp.bfloat16)
    fill = jnp.zeros((LANES - chi, LANES), jnp.bfloat16)

    def take_blocks(kind, at):
        landed = env_ref.at[kind, at]
        pltpu.make_async_copy(landed, landed, env_recv.at[kind, at]).wait()
        blocks = unpack_lanes(load_tiles(env_ref.at[kind], at, width), chi)
        for d, block in enumerate(blocks):
            lanes = slice(d * LANES, (d + 1) * LANES)
            for part, values in enumerate(halves(block)):
                tall_block = jnp.concatenate([values, fill], axis=0)
                turned = dot_last(unit, tall_block).astype(jnp.bfloat16)
                yield lanes, part, values, tall_block, turned

    def take_far(at):
        for lanes, part, values, tall_block, turned in take_blocks(early, at):
            for copy in (0, 1) if part == 0 else (2,):
                rows = slice(copy * LANES, (copy + 1) * LANES)
                far[1, at, rows, lanes] = turned
                far[0, at, rows, lanes] = tall_block

    def take_near(side, at):
        blocks = unpack_lanes(load_tiles(env_ref.at[late], at, width), chi)
        for d, block in enumerate(blocks):
            lanes = slice(d * LANES, (d + 1) * LANES)
            for part, values in enumerate(halves(block)):
                rows = slice(part * chi, (part + 1) * chi)
                if side == 0:
                    values = dot_last(unit, jnp.concatenate([values, fill], axis=0))
                    values = values.astype(jnp.bfloat16)[:chi]
                near[rows, lanes] = values

    second = jnp.where(rank >= col_count // 2, 1, 0)

    def hop(side):
        return pltpu.make_async_remote_copy(
            hop_out.at[side],
            hop_in.at[side],
            hop_send.at[side],
            hop_recv.at[side],
            device_id={"cols": cols_at + onward * (1 - 2 * side)},
        )

    def put_environ(blocks):
        for at, block in enumerate(blocks):
            vbuf[at * chi : (at + 1) * chi] = block

    def put_edge(side):
        blocks = unpack_lanes(load_tiles(sides, true_side(side), width), chi)

        @pl.when(late == 0)
        def _():
            put_environ(blocks)

        @pl.when(late == 1)
        def _():
            empty = jnp.zeros((LANES - chi, LANES), jnp.float32)
            put_environ([jnp.concatenate([block, empty], axis=0).T[:chi] for block in blocks])

    def place_of(side, order):
        return order + side * (local_cols - 2 * order)

    def join(side, at_column):
        v_high, v_low = halves(vbuf[...])
        true = true_side(side)
        jbuf[...] = dot32(
            jnp.concatenate([v_high, v_low], axis=1), far[true, at_column, : 2 * LANES]
        ) + dot32(v_high, far[true, at_column, 2 * LANES :])

    chunk = 16

    def pass_through(side, at_column, p, start):
        true = true_side(side)

        def ket(p, u, i, d, o):
            at = p * 16 + u * 8 + i * 4 + d * 2 + o
            return kets_near[at_column, true, at : at + 1, :]

        def joined(i, d):
            return jbuf[pl.ds(i * chi + start, chunk), d * LANES : (d + 1) * LANES]

        for u in range(D):
            for o in range(D):
                part = {}
                for i2 in range(D):
                    for d2 in range(D):
                        total = None
                        for i in range(D):
                            for d in range(D):
                                term = ket(p, u, i, d, o) * joined(i * D + i2, d * D + d2)
                                total = term if total is None else total + term
                        part[i2, d2] = total
                for q in range(PHYS):
                    for u2 in range(D):
                        for o2 in range(D):
                            total = None
                            for i2 in range(D):
                                for d2 in range(D):
                                    term = ket(q, u2, i2, d2, o2) * part[i2, d2]
                                    total = term if total is None else total + term
                            high, low = halves(total)
                            rows = pl.ds((u * D + u2) * LANES + start, chunk)
                            spot = (p * PHYS + q) * D2 + o * D + o2
                            lanes = slice(spot * LANES, (spot + 1) * LANES)
                            thi[rows, lanes] = high
                            tlo[rows, lanes] = low

    def open_up(side, at_column):
        join(side, at_column)

        def through(at, unused):
            for p in range(PHYS):
                pass_through(side, at_column, p, pl.multiple_of(at * chunk, chunk))
            return unused

        lax.fori_loop(0, chi // chunk, through, 0)

    def close(side, at_column, pair):
        both = near[...]
        lanes = slice(pair * wide, (pair + 1) * wide)
        large = dot32(both, thi[:, lanes])
        opens[true_side(side), at_column - side, pair] = large[:chi] + (
            large[chi:] + dot32(both[:chi], tlo[:, lanes])
        )

    def first_order(side):
        return jnp.where((side == 0) & (rank == 0), 1, 0)

    def is_edge(side):
        return ((side == 0) & (rank == 0)) | ((side == 1) & (rank == col_count - 1))

    def early_work():
        @pl.when(has_prev)
        def _():
            pltpu.make_async_copy(kets_near.at[0], kets_near.at[0], ket_recv).wait()

        for at in range(1, local_cols + 1):
            take_far(at)

        @pl.when(has_prev)
        def _():
            take_far(0)

        for side in range(2):

            @pl.when(is_edge(side))
            def _():
                put_edge(side)

        @pl.when(is_edge(second))
        def _():
            open_up(second, place_of(second, first_order(second)))

    early_first = (way != low_half) & (mine != groups // 2) & (mine != groups // 2 - 1)
    early_at = jnp.where(early_first, 0, 1)

    def phase(at, unused):
        @pl.when(at == early_at)
        def _():
            early_work()

        @pl.when(at != early_at)
        def _():
            run_chain()

        return unused

    lax.fori_loop(0, 2, phase, 0)

    spot_row = lax.broadcasted_iota(jnp.int32, (terms, terms), 0)
    spot_lane = lax.broadcasted_iota(jnp.int32, (terms, terms), 1)

    def stand(ref):
        values = jnp.broadcast_to(ref[...].astype(jnp.float32), (terms, terms))
        return jnp.sum(jnp.where(spot_row == spot_lane, values, 0.0), axis=1, keepdims=True)

    term_row = stand(rows_ref).astype(jnp.int32)
    term_bond = stand(bonds_ref).astype(jnp.int32)
    term_op = stand(ops_ref).astype(jnp.int32)
    term_weights = jnp.zeros((terms, table_ref.shape[1]), jnp.float32)
    for op in range(table_ref.shape[0]):
        term_weights = jnp.where(term_op == op, table_ref[op : op + 1, :], term_weights)

    def walk(turn, unused):
        side = (turn // local_cols + second) % 2
        order = turn % local_cols
        at_column = place_of(side, order)
        absent = (rank == 0) & (at_column == side)
        opening = order == first_order(side)
        ending = order == local_cols - 1

        fresh = (turn < local_cols) | (at_column == side * local_cols)

        @pl.when(jnp.logical_not(absent) & fresh)
        def _():
            landed = env_ref.at[late, at_column]
            pltpu.make_async_copy(landed, landed, env_recv.at[late, at_column]).wait()

        for at in range(2):

            @pl.when(jnp.logical_not(absent) & (true_side(side) == at))
            def _():
                take_near(at, at_column)

        @pl.when((order == 0) & jnp.logical_not(is_edge(side)))
        def _():
            pltpu.make_async_copy(hop_in.at[side], hop_in.at[side], hop_recv.at[side]).wait()
            put_environ(unpack_lanes(load_tiles(hop_in, side, width), chi))

        @pl.when(jnp.logical_not(absent) & opening & is_edge(side))
        def _():
            for pair in range(pairs):
                close(side, at_column, pair)

        @pl.when(jnp.logical_not(absent) & jnp.logical_not(opening & is_edge(side)))
        def _():
            join(side, at_column)
            for p in range(PHYS):
                for start in range(0, chi, chunk):
                    pass_through(side, at_column, p, start)
                for q in range(PHYS):
                    close(side, at_column, p * PHYS + q)

        asked = jnp.where(side == 0, has_next, has_prev) | jnp.logical_not(ending)

        @pl.when(jnp.logical_not(absent) & asked)
        def _():
            closed = opens[true_side(side), at_column - side, 0]
            for p in range(1, PHYS):
                closed += opens[true_side(side), at_column - side, p * PHYS + p]
            square = jnp.sum(
                jnp.sum(closed * closed, axis=1, keepdims=True), axis=0, keepdims=True
            )
            closed = closed * (1.0 / jnp.sqrt(square / (chi * width) + EPSILON))
            blocks = [closed[:, d * LANES : (d + 1) * LANES] for d in range(D2)]
            put_environ(blocks)

            @pl.when(ending)
            def _():
                for t, tile in enumerate(pack_lanes(blocks, chi)):
                    hop_out[side, :, t * LANES : (t + 1) * LANES] = tile

        @pl.when(ending & (side == 0) & has_next)
        def _():
            hop(0).start()

        @pl.when(ending & (side == 1) & has_prev)
        def _():
            hop(1).start()

        return unused

    lax.fori_loop(0, 2 * local_cols, walk, 0)

    tall = (terms, LANES)
    lane = lax.broadcasted_iota(jnp.int32, tall, 1)
    held = shared.at[0]
    held[...] = jnp.zeros(tall, jnp.float32)
    here = jnp.zeros((terms, 1), jnp.int32)
    for k in range(local_cols):
        bond = cols_at * local_cols + k - 1 + late * (local_cols - 2 * k)
        hit = (term_row == place) & (term_bond == bond)
        here = jnp.where(hit, 1, here)

        def add_bond(k=k, hit=hit):
            values = jnp.zeros(tall, jnp.float32)
            for p in range(pairs):
                former = opens[0, k, p]
                for q in range(pairs):
                    value = jnp.sum(
                        jnp.sum(former * opens[1, k, q], axis=0, keepdims=True),
                        axis=1,
                        keepdims=True,
                    )
                    values = jnp.where(lane == p * pairs + q, value, values)
            held[...] += jnp.where(hit, values, 0.0)

        if k:
            add_bond()
        else:
            pl.when(has_prev)(add_bond)

    total = held[...]
    picked = jnp.sum(total[:, : pairs * pairs] * term_weights, axis=1, keepdims=True)
    bra, ket_at = lane % pairs, lane // pairs
    diagonal = (bra // PHYS == bra % PHYS) & (ket_at // PHYS == ket_at % PHYS)
    trace = jnp.sum(
        jnp.where(diagonal & (lane < pairs * pairs), total, 0.0), axis=1, keepdims=True
    )
    size = jnp.sqrt(jnp.sum(total * total, axis=1, keepdims=True))
    energy = picked / jnp.maximum(jnp.abs(trace), 0.25 * size)
    same = lax.broadcasted_iota(jnp.int32, tall, 0) == lane
    devices = row_count * col_count
    spot_mine = place * col_count + cols_at
    own = own_share.at[0]
    own[...] = jnp.sum(jnp.where(same & (here == 1), energy, 0.0), axis=0, keepdims=True)

    @pl.when(has_lower & jnp.logical_not(has_upper))
    def _():
        pl.semaphore_wait(token.at[0], 1)

    @pl.when(has_upper & jnp.logical_not(has_lower))
    def _():
        pl.semaphore_wait(token.at[1], 1)

    def tell(turn, unused):
        row = turn + late * (row_count - 1 - 2 * turn)
        for col in range(col_count):

            @pl.when((row != place) | (col != cols_at))
            def _():
                pltpu.make_async_remote_copy(
                    own,
                    share.at[spot_mine],
                    share_send,
                    share_recv,
                    device_id={"rows": row, "cols": col},
                ).start()

        return unused

    lax.fori_loop(0, row_count, tell, 0)
    pltpu.make_async_copy(own, share.at[spot_mine], share_recv).start()
    pltpu.make_async_copy(share, share, share_recv).wait()
    others = share.at[pl.ds(0, devices - 1)]
    pltpu.make_async_copy(others, others, share_send).wait()

    @pl.when(has_next)
    def _():
        hop(0).wait_send()
        ket_copy.wait_send()

    @pl.when(has_prev)
    def _():
        hop(1).wait_send()

    for step in range(group):
        slot = step + way * (group - 1 - 2 * step)

        @pl.when(slot != me)
        def _():
            row_copy(
                xbuf.at[step],
                env_ref.at[way, spot_of(column)],
                env_send.at[step],
                env_recv.at[way, spot_of(column)],
                slot,
            )[0].wait_send()
            row_copy(
                xbuf.at[step + 1],
                out_ref.at[way, column],
                out_send.at[step],
                out_recv.at[way, column],
                slot,
            )[0].wait_send()

        @pl.when(has_next & (column == edge_col))
        def _():
            side_copy(step, slot).wait_send()

    @pl.when(opening_chain)
    def _():
        each_map(low_half, True, finish)

    each_map(low_half, False, finish)
    for cross in (True, False):
        each_map(late, cross, finish)

    @pl.when(has_after)
    def _():
        chain_hop.wait_send()

    for a in range(2):
        for b in range(local_cols):
            pltpu.make_async_copy(out_ref.at[a, b], out_ref.at[a, b], out_recv.at[a, b]).wait()


def window(row_count, col_count, args):
    local_cols = args[0].shape[1]
    chi, width = args[1].shape[-2:]
    terms = args[7].shape[0]
    group = 2 * local_cols
    wide = D2 * LANES
    pairs = PHYS * PHYS
    entries = args[0].shape[2]
    vmem = pl.BlockSpec(memory_space=pltpu.VMEM)
    stay = pl.BlockSpec(memory_space=pltpu.HBM)
    dma = pltpu.SemaphoreType.DMA

    def f32(*shape):
        return pltpu.VMEM(shape, jnp.float32)

    def bf16(*shape):
        return pltpu.VMEM(shape, jnp.bfloat16)

    return pl.pallas_call(
        functools.partial(window_kernel, row_count, col_count),
        out_shape=(
            jax.ShapeDtypeStruct((2, local_cols, chi, width), jnp.float32),
            jax.ShapeDtypeStruct((row_count * col_count, 1, LANES), jnp.float32),
        ),
        in_specs=[vmem] + [stay] * 6 + [vmem] * 4,
        out_specs=(stay, stay),
        scratch_shapes=[
            f32(2, local_cols, entries, LANES),
            f32(local_cols + 1, 2, entries, LANES),
            f32(2, 2, local_cols, chi, width),
            f32(2, local_cols, chi, width),
            f32(2, chi, width),
            f32(2, local_cols + 1, chi, width),
            f32(group, chi, width),
            f32(group, chi, width),
            f32(group, entries, LANES),
            f32(group + 1, chi, width),
            f32(D2**3, width),
            bf16(width, wide),
            bf16(width, width),
            bf16(group, width, 2 * LANES),
            f32(width, width),
            bf16(group, D2 * width, 2 * width),
            bf16(2 * LANES, 2 * width),
            f32(D2 * chi, wide),
            bf16(wide, pairs * wide),
            bf16(wide, pairs * wide),
            bf16(2 * chi, wide),
            bf16(2, local_cols + 1, 3 * LANES, wide),
            f32(D2 * chi, LANES),
            f32(2, local_cols, pairs, chi, wide),
            f32(2, chi, width),
            f32(2, chi, width),
            f32(1, 1, LANES),
            f32(1, terms, LANES),
            pltpu.SemaphoreType.REGULAR((2,)),
            dma((6,)),
            dma((3, group)),
            dma((3, group)),
            dma((group,)),
            dma((group,)),
            dma((2, local_cols + 1)),
            dma((group,)),
            dma((2, local_cols)),
            dma,
            dma,
            dma((2,)),
            dma((2,)),
            dma,
            dma,
            dma,
            dma,
        ],
        compiler_params=pltpu.CompilerParams(
            collective_id=0, has_side_effects=True, vmem_limit_bytes=56 * 1024 * 1024
        ),
        name="window",
    )(*args[:7], *(index[None] for index in args[7:10]), args[10])


def settle_kernel(
    outs_ref, share_ref, top_ref, bottom_ref, energies_ref, held, shares, line, sem
):
    gather = pltpu.make_async_copy(share_ref, shares, sem.at[0, 0])
    gather.start()
    parts = [
        (outs_ref.at[way, at], held.at[way, at], (top_ref, bottom_ref)[way].at[0, at])
        for way in range(2)
        for at in range(held.shape[1])
    ]
    for at, (source, middle, target) in enumerate(parts):
        pltpu.make_async_copy(source, middle, sem.at[0, at + 1]).start()
    gather.wait()
    line[...] = jnp.sum(shares[...], axis=0)[:, : line.shape[1]]
    put = pltpu.make_async_copy(line, energies_ref, sem.at[1, 0])
    put.start()
    for at, (source, middle, target) in enumerate(parts):
        pltpu.make_async_copy(source, middle, sem.at[0, at + 1]).wait()
        pltpu.make_async_copy(middle, target, sem.at[1, at + 1]).start()
    for at, (source, middle, target) in enumerate(parts):
        pltpu.make_async_copy(middle, target, sem.at[1, at + 1]).wait()
    put.wait()


def settle(outs, shares, terms):
    stay = pl.BlockSpec(memory_space=pltpu.HBM)
    half = jax.ShapeDtypeStruct((1,) + outs.shape[1:], outs.dtype)
    count = outs.shape[0] * outs.shape[1] + 1
    return pl.pallas_call(
        settle_kernel,
        out_shape=(half, half, jax.ShapeDtypeStruct((1, terms), shares.dtype)),
        in_specs=[stay] * 2,
        out_specs=(stay,) * 3,
        scratch_shapes=[
            pltpu.VMEM(outs.shape, outs.dtype),
            pltpu.VMEM(shares.shape, shares.dtype),
            pltpu.VMEM((1, terms), shares.dtype),
            pltpu.SemaphoreType.DMA((2, count)),
        ],
        name="settle",
    )(outs, shares)


def shards(*args):
    outs, shares = window(lax.axis_size("rows"), lax.axis_size("cols"), args)
    top, bottom, energies = settle(outs, shares, args[7].shape[0])
    return (top, bottom, energies[0])


def solution(mesh):
    placed = (
        P("rows", "cols", None),
        P(None, "rows", "cols", None, None),
        P(None, "rows", "cols", None, None),
        P("cols", None, None),
        P("cols", None, None),
        P("rows", None, None),
        P("rows", None, None),
        P(),
        P(),
        P(),
        P(),
    )
    return jax.shard_map(
        shards,
        mesh=mesh,
        in_specs=placed,
        out_specs=(P("rows", "cols", None, None), P("rows", "cols", None, None), P()),
        check_vma=False,
    )
```
